32 devices in a mesh: dp: 2 (over x), lon: 4 (over z), lat: 4 (over y, core).
Axes of the slice: x: 2, y: 2, z: 4, core: 2. Of those that a mesh axis runs over, the one named last changes fastest.
Arguments:
- grid_in: bfloat16 [32, 64, 64, 474], P('dp', 'lat', 'lon'), parts along dimension 0
- mesh_in: bfloat16 [128, 3], P(('lat', 'lon'))
- edge_in: bfloat16 [128, 48, 4], P(('lat', 'lon'))
- senders: int32 [128, 48], P(('lat', 'lon'))
- edge_mask: int32 [128, 48], P(('lat', 'lon'))
- w_grid: bfloat16 [474, 512], replicated
- w_mesh: bfloat16 [3, 512], replicated
- w_edge: bfloat16 [4, 512], replicated
- w_msg: bfloat16 [1536, 512], replicated
- w_node: bfloat16 [1024, 512], replicated
- w_gupd: bfloat16 [512, 512], replicated
- w_out: bfloat16 [6, 512, 512], replicated
- bias_gain: float32 [6, 4, 512], replicated
Outputs:
- output 1: bfloat16 [32, 128, 512], P('dp', ('lat', 'lon')), parts along dimension 0
- output 2: bfloat16 [32, 64, 64, 512], P('dp', 'lat', 'lon'), parts along dimension 0
There are 2 independent parts. The reference program is written for one: setup_inputs(seed, part) draws one part's arguments, and reference() takes and returns one part's arrays. A program takes and returns all parts, laid end to end along the dimension named above; an argument that names none is the same for every part.
All inputs are finite; a program needn't handle non-finite values.
Results may differ from the reference program's by a relative error of at most 0.00871152.
Values are sent between devices in bfloat16 or wider.
A program may use at most 1 GiB of HBM per device.

```python
import jax
import jax.numpy as jnp
from jax import lax

BATCH = 16
CIN = 474
LATENT = 512
LAT_CELLS = 4
LON_CELLS = 4
CELL = 16
GRID_PER_MESH = 32
SLOTS = 48
REACH = 3

GRID_ROWS = LAT_CELLS * CELL
GRID_COLS = LON_CELLS * CELL
MESH_CELL = CELL * CELL // GRID_PER_MESH
MESH_NODES = LAT_CELLS * LON_CELLS * MESH_CELL
LN_EPS = 1e-5


def draw_graph(graph_key):
    key_list = jax.random.split(graph_key, 11)
    node_ids = jnp.arange(MESH_NODES)
    cell_ids = node_ids // MESH_CELL
    cell_lat = cell_ids // LON_CELLS
    cell_lon = cell_ids % LON_CELLS
    in_cap = (node_ids % MESH_CELL) < MESH_CELL // 2
    top_cap = in_cap & (cell_lat == 0)
    bottom_cap = in_cap & (cell_lat == LAT_CELLS - 1)
    cap_node = top_cap | bottom_cap
    cap_offset = jax.random.randint(key_list[0], (MESH_NODES,), 0, REACH)
    recv_row = cell_lat * CELL + jax.random.randint(key_list[1], (MESH_NODES,), 0, CELL)
    recv_row = jnp.where(top_cap, cap_offset, recv_row)
    recv_row = jnp.where(bottom_cap, GRID_ROWS - 1 - cap_offset, recv_row)
    recv_col = cell_lon * CELL + jax.random.randint(key_list[2], (MESH_NODES,), 0, CELL)
    box_side = 2 * REACH + 1
    box_size = box_side * box_side
    scores = jax.random.randint(key_list[3], (MESH_NODES, box_size), 0, 1048576) * box_size + jnp.arange(box_size)
    picked = jnp.argsort(scores, axis=1)[:, :SLOTS]
    send_row = recv_row[:, None] + picked // box_side - REACH
    send_col = recv_col[:, None] + picked % box_side - REACH
    past_north = send_row < 0
    past_south = send_row >= GRID_ROWS
    send_col = jnp.where(past_north | past_south, send_col + GRID_COLS // 2, send_col)
    send_row = jnp.where(past_north, -1 - send_row, send_row)
    send_row = jnp.where(past_south, 2 * GRID_ROWS - 1 - send_row, send_row)
    cap_slot = cap_node[:, None] & (jnp.arange(SLOTS) >= SLOTS // 4)[None, :]
    cap_row = jax.random.randint(key_list[4], (MESH_NODES, SLOTS), 0, REACH)
    cap_row = jnp.where(top_cap[:, None], cap_row, GRID_ROWS - 1 - cap_row)
    cap_col = jax.random.randint(key_list[5], (MESH_NODES, SLOTS), 0, GRID_COLS)
    send_row = jnp.where(cap_slot, cap_row, send_row)
    send_col = jnp.where(cap_slot, cap_col, send_col) % GRID_COLS
    senders = (send_row * GRID_COLS + send_col).astype(jnp.int32)
    counts = jax.random.randint(key_list[6], (MESH_NODES,), 1, SLOTS + 1)
    few_count = jax.random.randint(key_list[8], (MESH_NODES,), 1, 4)
    small_node = jax.random.randint(key_list[9], (MESH_NODES,), 0, 3) == 0
    counts = jnp.where(small_node, few_count, counts)
    counts = jnp.where(cap_node, SLOTS, counts)
    slot_draw = jax.random.randint(key_list[10], (MESH_NODES, SLOTS), 0, SLOTS)
    edge_mask = ((slot_draw < counts[:, None]) | (jnp.arange(SLOTS)[None, :] == 0)).astype(jnp.int32)
    sub_pos = jax.random.uniform(key_list[7], (MESH_NODES, 2), jnp.float32)
    recv_lat = 0.5 * jnp.pi - (recv_row + sub_pos[:, 0]) * (jnp.pi / GRID_ROWS)
    recv_lon = (recv_col + sub_pos[:, 1]) * (2.0 * jnp.pi / GRID_COLS)
    send_lat = 0.5 * jnp.pi - (send_row + 0.5) * (jnp.pi / GRID_ROWS)
    send_lon = (send_col + 0.5) * (2.0 * jnp.pi / GRID_COLS)
    mesh_feat = jnp.stack([jnp.cos(recv_lat), jnp.sin(recv_lon), jnp.cos(recv_lon)], axis=-1)
    rel_lon = send_lon - recv_lon[:, None]
    sender_x = jnp.cos(send_lat) * jnp.cos(rel_lon)
    sender_y = jnp.cos(send_lat) * jnp.sin(rel_lon)
    sender_z = jnp.sin(send_lat)
    cos_lat = jnp.cos(recv_lat)[:, None]
    sin_lat = jnp.sin(recv_lat)[:, None]
    delta_x = sender_x * cos_lat + sender_z * sin_lat - 1.0
    delta_z = sender_z * cos_lat - sender_x * sin_lat
    distance = jnp.sqrt(delta_x * delta_x + sender_y * sender_y + delta_z * delta_z)
    inv_length = 1.0 / jnp.max(distance)
    edge_feat = jnp.stack([distance, delta_x, sender_y, delta_z], axis=-1) * inv_length
    return mesh_feat.astype(jnp.bfloat16), edge_feat.astype(jnp.bfloat16), senders, edge_mask


def dense_init(sub_key, fan_in, fan_out):
    values = jax.random.normal(sub_key, (fan_in, fan_out), jnp.float32) * fan_in ** -0.5
    return values.astype(jnp.bfloat16)


def setup_inputs(seed: int = 0, part: int = 0) -> dict:
    root_key = jax.random.key(seed)
    graph_key, weight_key, grid_key = jax.random.split(root_key, 3)
    mesh_in, edge_in, senders, edge_mask = draw_graph(graph_key)
    grid_keys = jax.random.split(jax.random.fold_in(grid_key, part), 2)
    row_ids = jnp.arange(GRID_ROWS)
    col_ids = jnp.arange(GRID_COLS)
    row_sign = ((row_ids // CELL) % 2) * 2.0 - 1.0
    col_sign = ((col_ids // CELL) % 2) * 2.0 - 1.0
    fronts = jax.random.normal(grid_keys[1], (2, CIN), jnp.float32)
    front_field = row_sign[:, None, None] * fronts[0] + col_sign[None, :, None] * fronts[1]
    base_field = jax.random.normal(grid_keys[0], (BATCH, GRID_ROWS, GRID_COLS, CIN), jnp.float32)
    grid_in = (base_field + 1.5 * front_field).astype(jnp.bfloat16)
    weight_keys = jax.random.split(weight_key, 8)
    w_out = (jax.random.normal(weight_keys[6], (6, LATENT, LATENT), jnp.float32) * LATENT ** -0.5).astype(jnp.bfloat16)
    spread = jnp.array([0.5, 0.5, 0.3, 0.3], jnp.float32)[None, :, None]
    offset = jnp.array([0.0, 0.0, 1.0, 0.0], jnp.float32)[None, :, None]
    bias_gain = jax.random.normal(weight_keys[7], (6, 4, LATENT), jnp.float32) * spread + offset
    return {
        'grid_in': grid_in,
        'mesh_in': mesh_in,
        'edge_in': edge_in,
        'senders': senders,
        'edge_mask': edge_mask,
        'w_grid': dense_init(weight_keys[0], CIN, LATENT),
        'w_mesh': dense_init(weight_keys[1], 3, LATENT),
        'w_edge': dense_init(weight_keys[2], 4, LATENT),
        'w_msg': dense_init(weight_keys[3], 3 * LATENT, LATENT),
        'w_node': dense_init(weight_keys[4], 2 * LATENT, LATENT),
        'w_gupd': dense_init(weight_keys[5], LATENT, LATENT),
        'w_out': w_out,
        'bias_gain': bias_gain,
    }


def mlp_apply(inputs, w_first, w_second, params):
    lead_shape = inputs.shape[:-1]
    flat_in = inputs.reshape(-1, inputs.shape[-1])
    hidden = jnp.dot(flat_in, w_first, preferred_element_type=jnp.float32) + params[0]
    hidden = jax.nn.silu(hidden).astype(jnp.bfloat16)
    result = jnp.dot(hidden, w_second, preferred_element_type=jnp.float32) + params[1]
    return result.reshape(lead_shape + (w_second.shape[1],))


def layer_norm(values, params):
    centered = values - jnp.mean(values, axis=-1, keepdims=True)
    variance = jnp.mean(centered * centered, axis=-1, keepdims=True)
    return centered * lax.rsqrt(variance + LN_EPS) * params[2] + params[3]


def embed_block(inputs, w_first, w_second, params):
    return layer_norm(mlp_apply(inputs, w_first, w_second, params), params).astype(jnp.bfloat16)


def reference(grid_in, mesh_in, edge_in, senders, edge_mask, w_grid, w_mesh, w_edge, w_msg, w_node, w_gupd, w_out, bias_gain):
    def grid_band(row_band):
        band_lat = embed_block(row_band, w_grid, w_out[0], bias_gain[0])
        band_upd = layer_norm(mlp_apply(band_lat, w_gupd, w_out[5], bias_gain[5]), bias_gain[5])
        return band_lat, (band_lat.astype(jnp.float32) + band_upd).astype(jnp.bfloat16)

    row_bands = jnp.moveaxis(grid_in.reshape(BATCH, LAT_CELLS, CELL, GRID_COLS, CIN), 1, 0)
    band_lat, band_out = lax.map(grid_band, row_bands)
    grid_flat = jnp.moveaxis(band_lat, 0, 1).reshape(BATCH, GRID_ROWS * GRID_COLS, LATENT)
    grid_out = jnp.moveaxis(band_out, 0, 1).reshape(BATCH, GRID_ROWS, GRID_COLS, LATENT)
    mesh_lat = embed_block(mesh_in, w_mesh, w_out[1], bias_gain[1])

    def cell_update(cell_block):
        cell_edges, cell_senders, cell_mask, cell_mesh = cell_block
        edge_lat = embed_block(cell_edges, w_edge, w_out[2], bias_gain[2])
        sender_lat = jnp.take(grid_flat, cell_senders.reshape(-1), axis=1).reshape(BATCH, MESH_CELL, SLOTS, LATENT)
        full_shape = (BATCH, MESH_CELL, SLOTS, LATENT)
        msg_in = jnp.concatenate([
            jnp.broadcast_to(edge_lat[None], full_shape),
            sender_lat,
            jnp.broadcast_to(cell_mesh[None, :, None, :], full_shape)], axis=-1)
        msg_upd = layer_norm(mlp_apply(msg_in, w_msg, w_out[3], bias_gain[3]), bias_gain[3])
        edge_new = (edge_lat.astype(jnp.float32) + msg_upd).astype(jnp.bfloat16)
        weights = cell_mask.astype(jnp.float32)[None, :, :, None]
        agg_sum = jnp.sum(edge_new.astype(jnp.float32) * weights, axis=2).astype(jnp.bfloat16)
        node_in = jnp.concatenate([jnp.broadcast_to(cell_mesh[None], (BATCH, MESH_CELL, LATENT)), agg_sum], axis=-1)
        node_upd = layer_norm(mlp_apply(node_in, w_node, w_out[4], bias_gain[4]), bias_gain[4])
        return (cell_mesh.astype(jnp.float32) + node_upd).astype(jnp.bfloat16)

    cell_count = LAT_CELLS * LON_CELLS
    cell_out = lax.map(cell_update, (
        edge_in.reshape(cell_count, MESH_CELL, SLOTS, 4),
        senders.reshape(cell_count, MESH_CELL, SLOTS),
        edge_mask.reshape(cell_count, MESH_CELL, SLOTS),
        mesh_lat.reshape(cell_count, MESH_CELL, LATENT)))
    mesh_out = jnp.moveaxis(cell_out, 1, 0).reshape(BATCH, MESH_NODES, LATENT)
    return mesh_out, grid_out
```

```python
import functools

import jax
import jax.numpy as jnp
from jax import lax
from jax.experimental import pallas as pl
from jax.experimental.pallas import tpu as pltpu
from jax.sharding import PartitionSpec as P

REACH = 3
LN_EPS = 1e-5
FEATS = 16
TILE = 32
F32 = jnp.float32
BF16 = jnp.bfloat16


def mm(a, b):
    return jnp.dot(a, b, preferred_element_type=F32)


def mm_nt(a, b):
    return lax.dot_general(a, b, (((1,), (1,)), ((), ())), preferred_element_type=F32)


def swish(x):
    t = x * 0.5
    return (t + t * jnp.tanh(t)).astype(BF16)


def norm(y):
    scale = 1.0 / y.shape[-1]
    centered = y - jnp.sum(y, axis=-1, keepdims=True) * scale
    var = jnp.sum(centered * centered, axis=-1, keepdims=True) * scale
    return centered * lax.rsqrt(var + LN_EPS)


def mlp_tail(pre, w2, bg):
    y = mm(swish(pre), w2) + bg[1:2]
    return norm(y) * bg[2:3] + bg[3:4]


def swap_rows(value, scr, inner, put):
    outer = value.shape[0] // inner
    pitch = scr.shape[1] // outer
    for k in range(scr.shape[0]):
        for b in range(outer):
            scr[k, pl.ds(b * pitch, inner), :] = value[b * inner:(b + 1) * inner, 128 * k:128 * (k + 1)]
    for c in range(inner):
        for k in range(scr.shape[0]):
            put(c, k, scr[k, pl.ds(c, outer, stride=pitch), :].astype(BF16))


def put_swapped(ref, c, k, part):
    ref[0, c, :, 128 * k:128 * (k + 1)] = part


def grid_kernel(x_ref, wg_ref, w0_ref, wu_ref, w5_ref, bg0_ref, bg5_ref, *rest):
    out_ref, tr_ref, scr = rest[-3:]
    batch, _, cols, chans = x_ref.shape
    latent = out_ref.shape[-1]
    rows = batch * cols
    bg0 = bg0_ref[0]
    bg5 = bg5_ref[0]
    x = x_ref[...].reshape(rows, chans)
    vg = mlp_tail(mm(x, wg_ref[...]) + bg0[0:1], w0_ref[0], bg0)
    swap_rows(vg, scr, cols, lambda c, k, part: put_swapped(tr_ref, c, k, part))
    vgb = vg.astype(BF16)
    upd = mlp_tail(mm(vgb, wu_ref[...]) + bg5[0:1], w5_ref[0], bg5)
    out = (vgb.astype(F32) + upd).astype(BF16)
    out_ref[...] = out.reshape(batch, 1, cols, latent)


def grid_call(grid_in, w_grid, w_out, w_gupd, bias_gain, row0, nrows, prev):
    batch, rows, cols, chans = grid_in.shape
    latent = w_out.shape[-1]
    whole = lambda *shape: pl.BlockSpec(shape, lambda r: (0,) * len(shape))
    pick = lambda k, *shape: pl.BlockSpec((1,) + shape, lambda r: (k,) + (0,) * len(shape))
    in_specs = [
        pl.BlockSpec((batch, 1, cols, chans), lambda r: (0, r + row0, 0, 0)),
        whole(chans, latent), pick(0, latent, latent), whole(latent, latent), pick(5, latent, latent),
        pick(0, 4, latent), pick(5, 4, latent)]
    args = [grid_in, w_grid, w_out, w_gupd, w_out, bias_gain, bias_gain]
    alias = {}
    if prev is not None:
        in_specs.append(pl.BlockSpec(memory_space=pl.ANY))
        args.append(prev)
        alias = {7: 0}
    return pl.pallas_call(
        grid_kernel,
        grid=(nrows,),
        in_specs=in_specs,
        out_specs=[
            pl.BlockSpec((batch, 1, cols, latent), lambda r: (0, r + row0, 0, 0)),
            pl.BlockSpec((1, cols, batch, latent), lambda r: (r, 0, 0, 0))],
        out_shape=[
            jax.ShapeDtypeStruct((batch, rows, cols, latent), BF16),
            jax.ShapeDtypeStruct((nrows, cols, batch, latent), BF16)],
        scratch_shapes=[pltpu.VMEM((latent // 128, batch * (cols + 8), 128), F32)],
        input_output_aliases=alias,
        cost_estimate=pl.CostEstimate(
            flops=8 * nrows * batch * cols * latent * latent, transcendentals=0,
            bytes_accessed=6 * nrows * batch * cols * latent),
        name=f'grid_rows{row0}',
    )(*args)


def edge_kernel(v_ref, we_ref, wm_ref, wmsg_ref, w1_ref, w2_ref, w3_ref, wn_ref, bg_ref,
                north_ref, top_ref, mid_ref, bot_ref, south_ref,
                own_ref, p1_ref, p2_ref, p3_ref, vm_ref, nb_ref,
                table, lp, ec, vmf, idx_v, idx_s, part, xbuf, sems, isem, *, lats, lons):
    latent = w1_ref.shape[-1]
    slots = v_ref.shape[0]
    cols, batch = table.shape[0] // (top_ref.shape[0] * 2 + mid_ref.shape[0] + 2 * REACH), table.shape[1]
    nodes = own_ref.shape[0]
    per_node = slots // (lons * nodes)
    band = lons * nodes
    lat = lax.axis_index('lat')
    lon = lax.axis_index('lon')
    copies = []
    start = 0
    for k, ref in enumerate((north_ref, top_ref, mid_ref, bot_ref, south_ref)):
        count = ref.shape[0] * cols
        src = ref.reshape(count, batch, latent)
        copy = pltpu.make_async_copy(src, table.at[pl.ds(start, count)], sems.at[k])
        copy.start()
        copies.append(copy)
        start += count
    positions = start
    cell_rows = positions // cols - 2 * REACH

    v = v_ref[...]
    pick_row = lax.broadcasted_iota(jnp.int32, (band, slots), 0) * per_node
    pick = (lax.broadcasted_iota(jnp.int32, (band, slots), 1) == pick_row)
    mesh_feat = mm(jnp.where(pick, 1.0, 0.0).astype(BF16), v).astype(BF16)
    bg1 = bg_ref[1]
    bg2 = bg_ref[2]
    bg3 = bg_ref[3]
    vm = mlp_tail(mm(mesh_feat, wm_ref[...]) + bg1[0:1], w1_ref[0], bg1).astype(BF16)
    vmf[...] = vm.astype(F32)
    own_vm = vmf[pl.ds(pl.multiple_of(lon * nodes, 8), nodes), :]
    vm_ref[...] = own_vm
    nb_ref[...] = mm(own_vm.astype(BF16), wn_ref[...]) + bg_ref[4][0:1]

    eye = (lax.broadcasted_iota(jnp.int32, (FEATS, FEATS), 0) == lax.broadcasted_iota(jnp.int32, (FEATS, FEATS), 1))
    vt = mm_nt(jnp.where(eye, 1.0, 0.0).astype(BF16), v)
    col = vt[5:6] - (lon * cols).astype(F32)
    flag = jnp.where((vt[6:7] > 0.5) & (col > -0.5) & (col < cols - 0.5), 1.0, 0.0)
    chunks = slots // 128
    pad = -chunks % 16
    rows = [flag[:, 128 * c:128 * (c + 1)] for c in range(chunks)] + [jnp.zeros((pad, 128), F32)] * (pad > 0)
    flags = jnp.concatenate(rows, axis=0)
    up = lax.broadcasted_iota(jnp.int32, (128, 128), 0) <= lax.broadcasted_iota(jnp.int32, (128, 128), 1)
    incl = mm(flags.astype(BF16), jnp.where(up, 1.0, 0.0).astype(BF16))
    n_rows = chunks + pad
    low = lax.broadcasted_iota(jnp.int32, (n_rows, n_rows), 1) < lax.broadcasted_iota(jnp.int32, (n_rows, n_rows), 0)
    row_sum = jnp.broadcast_to(incl[:, 127:128], (n_rows, 128)).astype(BF16)
    before = mm(jnp.where(low, 1.0, 0.0).astype(BF16), row_sum)
    rank = jnp.where(flags > 0.5, incl + before - 1.0, -1.0)
    total = jnp.sum(flag).astype(jnp.int32)
    vtb = vt.astype(BF16)

    def prep(t, carry):
        slot = (lax.broadcasted_iota(jnp.int32, (128, 128), 0) + t * 128).astype(F32)
        sel = jnp.concatenate(
            [jnp.where(rank[c:c + 1] == slot, 1.0, 0.0).astype(BF16) for c in range(chunks)], axis=1)
        feat = mm(sel, v).astype(BF16)
        feat_t = mm_nt(vtb, sel)
        here = pl.ds(pl.multiple_of(t * 128, 128), 128)
        live = lax.broadcasted_iota(jnp.int32, (1, 128), 1) + t * 128 < total
        win_r = feat_t[4:5] - (lat * cell_rows - REACH).astype(F32)
        win_c = feat_t[5:6] - (lon * cols).astype(F32)
        pos = jnp.where(live, (win_r * cols + win_c).astype(jnp.int32), 0)
        node = feat_t[7:8].astype(jnp.int32)
        rel = lax.rem(node + (lons - lon) * nodes, band)
        idx_v[0:1, here] = jnp.clip(pos, 0, positions - 1)
        idx_v[1:2, here] = jnp.where(live, rel, band)
        edge = mlp_tail(mm(feat, we_ref[...]) + bg2[0:1], w2_ref[0], bg2).astype(BF16)
        node_col = feat[:, 7:8].astype(F32)
        hot = lax.broadcasted_iota(jnp.int32, (128, band), 1).astype(F32) == node_col
        vm_e = mm(jnp.where(hot, 1.0, 0.0).astype(BF16), vm).astype(BF16)
        lp[here, :] = mm(edge, wmsg_ref[0:latent, :]) + mm(vm_e, wmsg_ref[2 * latent:, :]) + bg3[0:1]
        ec[here, :] = edge.astype(F32) + bg3[3:4]
        return carry

    lax.fori_loop(0, lax.div(total + 127, 128), prep, 0)
    move = pltpu.make_async_copy(idx_v, idx_s, isem)
    move.start()
    part[...] = jnp.zeros_like(part)
    move.wait()
    for copy in copies:
        copy.wait()

    def edges(t, carry):
        base = t * TILE
        for s in range(TILE):
            xbuf[pl.ds(s * batch, batch), :] = table[idx_s[0, base + s]]
        acc = mm(xbuf[...], wmsg_ref[latent:2 * latent, :]).reshape(TILE, batch, latent)
        here = pl.ds(pl.multiple_of(base, TILE), TILE)
        pre = acc + lp[here, :].reshape(TILE, 1, latent)
        hid = swish(pre).reshape(TILE * batch, latent)
        y = mm(hid, w3_ref[0]) + bg3[1:2]
        z = (norm(y) * bg3[2:3]).reshape(TILE, batch, latent) + ec[here, :].reshape(TILE, 1, latent)
        z = z.astype(BF16).astype(F32)
        for s in range(TILE):
            n = idx_s[1, base + s]
            part[n] += z[s]
        return carry

    lax.fori_loop(0, lax.div(total + TILE - 1, TILE), edges, 0)
    for k, ref in enumerate((own_ref, p1_ref, p2_ref, p3_ref)):
        ref[...] = part[k * nodes:(k + 1) * nodes]


def edge_call(v, w_edge, w_mesh, w_msg, w_out, w_node, bias_gain, strips, lats, lons, nodes):
    latent = w_out.shape[-1]
    slots = v.shape[0]
    cols, batch = strips[0].shape[1:3]
    positions = sum(s.shape[0] for s in strips) * cols
    whole = lambda a: pl.BlockSpec(a.shape, lambda r: (0,) * a.ndim)
    pick = lambda k, *shape: pl.BlockSpec((1,) + shape, lambda r: (k,) + (0,) * len(shape))
    block = jax.ShapeDtypeStruct((nodes, batch, latent), F32)
    row = jax.ShapeDtypeStruct((nodes, latent), F32)
    outs = [block] * 4 + [row] * 2
    return pl.pallas_call(
        functools.partial(edge_kernel, lats=lats, lons=lons),
        grid=(1,),
        in_specs=[whole(v), whole(w_edge), whole(w_mesh), whole(w_msg), pick(1, latent, latent), pick(2, latent, latent),
                  pick(3, latent, latent), pl.BlockSpec((latent, latent), lambda r: (0, 0)), whole(bias_gain)]
        + [pl.BlockSpec(memory_space=pl.ANY)] * 5,
        out_specs=[whole(o) for o in outs],
        out_shape=outs,
        scratch_shapes=[
            pltpu.VMEM((positions, batch, latent), BF16),
            pltpu.VMEM((slots, latent), F32),
            pltpu.VMEM((slots, latent), F32),
            pltpu.VMEM((lons * nodes, latent), F32),
            pltpu.VMEM((8, slots), jnp.int32),
            pltpu.SMEM((8, slots), jnp.int32),
            pltpu.VMEM((lons * nodes + 1, batch, latent), F32),
            pltpu.VMEM((TILE * batch, latent), BF16),
            pltpu.SemaphoreType.DMA((5,)),
            pltpu.SemaphoreType.DMA],
        cost_estimate=pl.CostEstimate(
            flops=4 * slots // 4 * batch * latent * latent, transcendentals=0, bytes_accessed=2 * positions * batch * latent),
        name='edges',
    )(v, w_edge, w_mesh, w_msg, w_out, w_out, w_out, w_node, bias_gain, *strips)


def node_kernel(own_ref, r1_ref, r2_ref, r3_ref, vm_ref, nb_ref, wn_ref, w4_ref, bg_ref, out_ref, scr):
    nodes, batch, latent = own_ref.shape
    agg = (own_ref[...] + r1_ref[...] + r2_ref[...] + r3_ref[...]).astype(BF16).reshape(nodes * batch, latent)
    acc = mm(agg, wn_ref[...]).reshape(nodes, batch, latent) + nb_ref[...].reshape(nodes, 1, latent)
    bg = bg_ref[0]
    upd = mlp_tail(acc.reshape(nodes * batch, latent), w4_ref[0], bg)
    out = (upd.reshape(nodes, batch, latent) + vm_ref[...].reshape(nodes, 1, latent)).reshape(nodes * batch, latent)

    def put(b, k, part):
        out_ref[b, :, 128 * k:128 * (k + 1)] = part

    swap_rows(out, scr, batch, put)


def node_call(blocks, vm, nb, w_node, w_out, bias_gain):
    nodes, batch, latent = blocks[0].shape
    whole = lambda a: pl.BlockSpec(a.shape, lambda r: (0,) * a.ndim)
    pick = lambda k, *shape: pl.BlockSpec((1,) + shape, lambda r: (k,) + (0,) * len(shape))
    out = jax.ShapeDtypeStruct((batch, nodes, latent), BF16)
    return pl.pallas_call(
        node_kernel,
        grid=(1,),
        in_specs=[whole(b) for b in blocks] + [whole(vm), whole(nb), pl.BlockSpec((latent, latent), lambda r: (1, 0)),
                                               pick(4, latent, latent), pick(4, 4, latent)],
        out_specs=whole(out),
        out_shape=out,
        scratch_shapes=[pltpu.VMEM((latent // 128, nodes * (batch + 8), 128), F32)],
        name='nodes',
    )(*blocks, vm, nb, w_node, w_out, bias_gain)


def solution(mesh):
    lats = mesh.shape['lat']
    lons = mesh.shape['lon']
    south_shift = [(s, s + 1) for s in range(lats - 1)]
    north_shift = [(s + 1, s) for s in range(lats - 1)]

    def cell_step(grid_in, mesh_in, edge_in, senders, edge_mask, w_grid, w_mesh, w_edge, w_msg, w_node, w_gupd, w_out, bias_gain):
        batch, rows, cols, _ = grid_in.shape
        nodes, per_node = senders.shape
        latent = w_out.shape[-1]
        grid_cols = cols * lons
        lon = lax.axis_index('lon')
        node_id = jnp.broadcast_to((jnp.arange(nodes) + lon * nodes)[:, None], (nodes, per_node))
        cols_of = [edge_in[..., k] for k in range(4)]
        cols_of += [(senders // grid_cols).astype(BF16), (senders % grid_cols).astype(BF16)]
        cols_of += [edge_mask.astype(BF16), node_id.astype(BF16)]
        cols_of += [jnp.broadcast_to(mesh_in[:, k:k + 1], (nodes, per_node)) for k in range(3)]
        cols_of += [jnp.zeros((nodes, per_node), BF16)] * (FEATS - len(cols_of))
        feats = jnp.stack(cols_of, axis=-1).reshape(nodes * per_node, FEATS)
        band = lax.all_gather(feats, 'lon', axis=0, tiled=True)
        we = jnp.zeros((FEATS, latent), BF16).at[0:4].set(w_edge)
        wm = jnp.zeros((FEATS, latent), BF16).at[8:11].set(w_mesh)
        call = functools.partial(grid_call, grid_in, w_grid, w_out, w_gupd, bias_gain)
        grid_out, top = call(0, REACH, None)
        from_south = lax.ppermute(top, 'lat', north_shift)
        grid_out, bot = call(rows - REACH, REACH, grid_out)
        from_north = lax.ppermute(bot, 'lat', south_shift)
        grid_out, mid = call(REACH, rows - 2 * REACH, grid_out)
        own, p1, p2, p3, vm, nb = edge_call(
            band, we, wm, w_msg, w_out, w_node, bias_gain, (from_north, top, mid, bot, from_south), lats, lons, nodes)
        got = [lax.ppermute(p, 'lon', [(s, (s + k) % lons) for s in range(lons)]) for k, p in ((1, p1), (2, p2), (3, p3))]
        mesh_out = node_call([own] + got, vm, nb, w_node, w_out, bias_gain)
        return mesh_out, grid_out

    grid_spec = P('dp', 'lat', 'lon', None)
    node_spec = P(('lat', 'lon'), None)
    slot_spec = P(('lat', 'lon'), None, None)
    in_specs = (grid_spec, node_spec, slot_spec, node_spec, node_spec) + (P(),) * 8
    out_specs = (P('dp', ('lat', 'lon'), None), grid_spec)
    return jax.shard_map(cell_step, mesh=mesh, in_specs=in_specs, out_specs=out_specs, check_vma=False)
```

```python
import functools

import jax
import jax.numpy as jnp
from jax import lax
from jax.experimental import pallas as pl
from jax.experimental.pallas import tpu as pltpu
from jax.sharding import PartitionSpec as P

REACH = 3
LN_EPS = 1e-5
FEATS = 16
TILE = 32
F32 = jnp.float32
BF16 = jnp.bfloat16


def mm(a, b):
    return jnp.dot(a, b, preferred_element_type=F32)


def mm_nt(a, b):
    return lax.dot_general(a, b, (((1,), (1,)), ((), ())), preferred_element_type=F32)


def swish(x):
    t = x * 0.5
    return (t + t * jnp.tanh(t)).astype(BF16)


def norm(y):
    scale = 1.0 / y.shape[-1]
    centered = y - jnp.sum(y, axis=-1, keepdims=True) * scale
    var = jnp.sum(centered * centered, axis=-1, keepdims=True) * scale
    return centered * lax.rsqrt(var + LN_EPS)


def mlp_tail(pre, w2, bg):
    y = mm(swish(pre), w2) + bg[1:2]
    return norm(y) * bg[2:3] + bg[3:4]


def swap_rows(value, scr, inner, put):
    outer = value.shape[0] // inner
    pitch = scr.shape[1] // outer
    for k in range(scr.shape[0]):
        for b in range(outer):
            scr[k, pl.ds(b * pitch, inner), :] = value[b * inner:(b + 1) * inner, 128 * k:128 * (k + 1)]
    for c in range(inner):
        for k in range(scr.shape[0]):
            put(c, k, scr[k, pl.ds(c, outer, stride=pitch), :].astype(BF16))


def embed_kernel(x_ref, wg_ref, w0_ref, bg_ref, feat_ref,
                 vg_ref, tr_ref, north_ref, south_ref, band_ref,
                 scr, up_buf, down_buf, up_sems, down_sems, feat_send, feat_recv, own_sem, *, lats, lons):
    batch, block, cols, chans = x_ref.shape
    latent = vg_ref.shape[-1]
    step = pl.program_id(0)
    last = pl.num_programs(0) - 1
    lat = lax.axis_index('lat')
    lon = lax.axis_index('lon')
    mesh_id = pl.DeviceIdType.MESH

    def strip(src, dst, sems, to):
        return pltpu.make_async_remote_copy(src, dst, sems.at[0], sems.at[1], device_id={'lat': to}, device_id_type=mesh_id)

    north_send = strip(up_buf, south_ref, up_sems, lat - 1)
    south_send = strip(down_buf, north_ref, down_sems, lat + 1)
    feats = [pltpu.make_async_remote_copy(
        feat_ref, band_ref.at[lon], feat_send.at[k - 1], feat_recv.at[k - 1],
        device_id={'lon': lax.rem(lon + k, lons)}, device_id_type=mesh_id) for k in range(1, lons)]
    own = pltpu.make_async_copy(feat_ref, band_ref.at[lon], own_sem)

    @pl.when(step == 0)
    def _():
        barrier = pltpu.get_barrier_semaphore()
        for k in range(1, lons):
            pl.semaphore_signal(barrier, 1, device_id={'lon': lax.rem(lon + k, lons)}, device_id_type=mesh_id)

        @pl.when(lat > 0)
        def _():
            pl.semaphore_signal(barrier, 1, device_id={'lat': lat - 1}, device_id_type=mesh_id)

        @pl.when(lat < lats - 1)
        def _():
            pl.semaphore_signal(barrier, 1, device_id={'lat': lat + 1}, device_id_type=mesh_id)

        own.start()

    @pl.when(step == 1)
    def _():
        barrier = pltpu.get_barrier_semaphore()
        inner = (lat > 0).astype(jnp.int32) + (lat < lats - 1).astype(jnp.int32)
        pl.semaphore_wait(barrier, lons - 1 + inner)

        @pl.when(lat > 0)
        def _():
            north_send.start()

        for copy in feats:
            copy.start()

    @pl.when((step == 2) & (lat < lats - 1))
    def _():
        south_send.start()

    rows = batch * cols
    bg = bg_ref[0]
    for r in range(block):
        x = x_ref[:, r].reshape(rows, chans)
        vg = mlp_tail(mm(x, wg_ref[...]) + bg[0:1], w0_ref[0], bg)
        vg_ref[:, r] = vg.astype(BF16).reshape(batch, cols, latent)

        def put(c, k, part):
            tr_ref[r, c, :, 128 * k:128 * (k + 1)] = part

        swap_rows(vg, scr.at[r], cols, put)

    @pl.when(step == 0)
    def _():
        up_buf[...] = tr_ref[0:REACH]

    @pl.when(step == 1)
    def _():
        down_buf[...] = tr_ref[block - REACH:]

    @pl.when(step == last)
    def _():
        own.wait()
        for copy in feats:
            copy.wait()

        @pl.when(lat > 0)
        def _():
            north_send.wait_send()
            south_send.wait_recv()

        @pl.when(lat < lats - 1)
        def _():
            south_send.wait_send()
            north_send.wait_recv()


def embed_call(grid_in, w_grid, w_out, bias_gain, feats, lats, lons, block):
    batch, rows, cols, chans = grid_in.shape
    latent = w_out.shape[-1]
    steps = rows // block
    whole = lambda *shape: pl.BlockSpec(shape, lambda r: (0,) * len(shape))
    pick = lambda k, *shape: pl.BlockSpec((1,) + shape, lambda r: (k,) + (0,) * len(shape))
    at = lambda r: lax.rem(r * (steps - 1), steps)
    strip = jax.ShapeDtypeStruct((REACH, cols, batch, latent), BF16)
    anywhere = pl.BlockSpec(memory_space=pl.ANY)
    return pl.pallas_call(
        functools.partial(embed_kernel, lats=lats, lons=lons),
        grid=(steps,),
        in_specs=[
            pl.BlockSpec((batch, block, cols, chans), lambda r: (0, at(r), 0, 0)),
            whole(chans, latent), pick(0, latent, latent), pick(0, 4, latent), whole(*feats.shape)],
        out_specs=[
            pl.BlockSpec((batch, block, cols, latent), lambda r: (0, at(r), 0, 0)),
            pl.BlockSpec((block, cols, batch, latent), lambda r: (at(r), 0, 0, 0)),
            anywhere, anywhere, anywhere],
        out_shape=[
            jax.ShapeDtypeStruct((batch, rows, cols, latent), BF16),
            jax.ShapeDtypeStruct((rows, cols, batch, latent), BF16),
            strip, strip, jax.ShapeDtypeStruct((lons,) + feats.shape, BF16)],
        scratch_shapes=[
            pltpu.VMEM((block, latent // 128, batch * (cols + 8), 128), F32),
            pltpu.VMEM(strip.shape, BF16), pltpu.VMEM(strip.shape, BF16),
            pltpu.SemaphoreType.DMA((2,)), pltpu.SemaphoreType.DMA((2,)),
            pltpu.SemaphoreType.DMA((lons - 1,)), pltpu.SemaphoreType.DMA((lons - 1,)), pltpu.SemaphoreType.DMA],
        compiler_params=pltpu.CompilerParams(collective_id=0, has_side_effects=True),
        cost_estimate=pl.CostEstimate(
            flops=4 * rows * batch * cols * latent * latent, transcendentals=0,
            bytes_accessed=6 * rows * batch * cols * latent),
        name='embed',
    )(grid_in, w_grid, w_out, bias_gain, feats)


def update_kernel(vg_ref, wu_ref, w5_ref, bg_ref, dep_ref, out_ref):
    bg = bg_ref[0]
    vg = vg_ref[...]
    upd = mlp_tail(mm(vg, wu_ref[...]) + bg[0:1], w5_ref[0], bg)
    out_ref[...] = (vg.astype(F32) + upd).astype(BF16)


def update_call(vg, w_gupd, w_out, bias_gain, dep, block):
    rows, latent = vg.shape
    pick = lambda k, *shape: pl.BlockSpec((1,) + shape, lambda r: (k,) + (0,) * len(shape))
    tile = pl.BlockSpec((block, latent), lambda r: (r, 0))
    return pl.pallas_call(
        update_kernel,
        grid=(rows // block,),
        in_specs=[tile, pl.BlockSpec((latent, latent), lambda r: (0, 0)), pick(5, latent, latent), pick(5, 4, latent),
                  pl.BlockSpec(memory_space=pl.ANY)],
        out_specs=tile,
        out_shape=jax.ShapeDtypeStruct(vg.shape, BF16),
        cost_estimate=pl.CostEstimate(flops=4 * rows * latent * latent, transcendentals=0, bytes_accessed=4 * rows * latent),
        name='update',
    )(vg, w_gupd, w_out, bias_gain, dep)


def edge_kernel(v_ref, we_ref, wm_ref, wmsg_ref, w1_ref, w2_ref, w3_ref, wn_ref, bg_ref,
                north_ref, mid_ref, south_ref,
                own_ref, p1_ref, p2_ref, p3_ref, vm_ref, nb_ref,
                table, lp, ec, vmf, idx_v, idx_s, part, xbuf, sems, isem, *, lats, lons):
    latent = w1_ref.shape[-1]
    slots = lons * v_ref.shape[-1]
    cols, batch = mid_ref.shape[1:3]
    nodes = own_ref.shape[0]
    per_node = slots // (lons * nodes)
    band = lons * nodes
    lat = lax.axis_index('lat')
    lon = lax.axis_index('lon')
    copies = []
    start = 0
    for k, ref in enumerate((north_ref, mid_ref, south_ref)):
        count = ref.shape[0] * cols
        src = ref.reshape(count, batch, latent)
        copy = pltpu.make_async_copy(src, table.at[pl.ds(start, count)], sems.at[k])
        copy.start()
        copies.append(copy)
        start += count
    positions = start
    cell_rows = positions // cols - 2 * REACH

    vtb = jnp.concatenate([v_ref[k] for k in range(lons)], axis=1)
    vt = vtb.astype(F32)
    pick_row = lax.broadcasted_iota(jnp.int32, (band, slots), 0) * per_node
    pick = (lax.broadcasted_iota(jnp.int32, (band, slots), 1) == pick_row)
    mesh_feat = mm_nt(jnp.where(pick, 1.0, 0.0).astype(BF16), vtb).astype(BF16)
    bg1 = bg_ref[1]
    bg2 = bg_ref[2]
    bg3 = bg_ref[3]
    vm = mlp_tail(mm(mesh_feat, wm_ref[...]) + bg1[0:1], w1_ref[0], bg1).astype(BF16)
    vmf[...] = vm.astype(F32)
    own_vm = vmf[pl.ds(pl.multiple_of(lon * nodes, 8), nodes), :]
    vm_ref[...] = own_vm
    nb_ref[...] = mm(own_vm.astype(BF16), wn_ref[...]) + bg_ref[4][0:1]

    col = vt[5:6] - (lon * cols).astype(F32)
    flag = jnp.where((vt[6:7] > 0.5) & (col > -0.5) & (col < cols - 0.5), 1.0, 0.0)
    chunks = slots // 128
    pad = -chunks % 16
    rows = [flag[:, 128 * c:128 * (c + 1)] for c in range(chunks)] + [jnp.zeros((pad, 128), F32)] * (pad > 0)
    flags = jnp.concatenate(rows, axis=0)
    up = lax.broadcasted_iota(jnp.int32, (128, 128), 0) <= lax.broadcasted_iota(jnp.int32, (128, 128), 1)
    incl = mm(flags.astype(BF16), jnp.where(up, 1.0, 0.0).astype(BF16))
    n_rows = chunks + pad
    low = lax.broadcasted_iota(jnp.int32, (n_rows, n_rows), 1) < lax.broadcasted_iota(jnp.int32, (n_rows, n_rows), 0)
    row_sum = jnp.broadcast_to(incl[:, 127:128], (n_rows, 128)).astype(BF16)
    before = mm(jnp.where(low, 1.0, 0.0).astype(BF16), row_sum)
    rank = jnp.where(flags > 0.5, incl + before - 1.0, -1.0)
    total = jnp.sum(flag).astype(jnp.int32)

    def prep(t, carry):
        slot = (lax.broadcasted_iota(jnp.int32, (128, 128), 0) + t * 128).astype(F32)
        sel = jnp.concatenate(
            [jnp.where(rank[c:c + 1] == slot, 1.0, 0.0).astype(BF16) for c in range(chunks)], axis=1)
        feat = mm_nt(sel, vtb).astype(BF16)
        feat_t = mm_nt(vtb, sel)
        here = pl.ds(pl.multiple_of(t * 128, 128), 128)
        live = lax.broadcasted_iota(jnp.int32, (1, 128), 1) + t * 128 < total
        win_r = feat_t[4:5] - (lat * cell_rows - REACH).astype(F32)
        win_c = feat_t[5:6] - (lon * cols).astype(F32)
        pos = jnp.where(live, (win_r * cols + win_c).astype(jnp.int32), REACH * cols)
        node = feat_t[7:8].astype(jnp.int32)
        rel = lax.rem(node + (lons - lon) * nodes, band)
        idx_v[0:1, here] = jnp.clip(pos, 0, positions - 1)
        idx_v[1:2, here] = jnp.where(live, rel, band)
        edge = mlp_tail(mm(feat, we_ref[...]) + bg2[0:1], w2_ref[0], bg2).astype(BF16)
        node_col = feat[:, 7:8].astype(F32)
        hot = lax.broadcasted_iota(jnp.int32, (128, band), 1).astype(F32) == node_col
        vm_e = mm(jnp.where(hot, 1.0, 0.0).astype(BF16), vm).astype(BF16)
        lp[here, :] = mm(edge, wmsg_ref[0:latent, :]) + mm(vm_e, wmsg_ref[2 * latent:, :]) + bg3[0:1]
        ec[here, :] = edge.astype(F32) + bg3[3:4]
        return carry

    lax.fori_loop(0, lax.div(total + 127, 128), prep, 0)
    move = pltpu.make_async_copy(idx_v, idx_s, isem)
    move.start()
    part[...] = jnp.zeros_like(part)
    move.wait()
    for copy in copies:
        copy.wait()

    def edges(t, carry):
        base = t * TILE
        for s in range(TILE):
            xbuf[pl.ds(s * batch, batch), :] = table[idx_s[0, base + s]]
        acc = mm(xbuf[...], wmsg_ref[latent:2 * latent, :]).reshape(TILE, batch, latent)
        here = pl.ds(pl.multiple_of(base, TILE), TILE)
        pre = acc + lp[here, :].reshape(TILE, 1, latent)
        hid = swish(pre).reshape(TILE * batch, latent)
        y = mm(hid, w3_ref[0]) + bg3[1:2]
        z = (norm(y) * bg3[2:3]).reshape(TILE, batch, latent) + ec[here, :].reshape(TILE, 1, latent)
        z = z.astype(BF16).astype(F32)
        for s in range(TILE):
            n = idx_s[1, base + s]
            part[n] += z[s]
        return carry

    lax.fori_loop(0, lax.div(total + TILE - 1, TILE), edges, 0)
    for k, ref in enumerate((own_ref, p1_ref, p2_ref, p3_ref)):
        ref[...] = part[k * nodes:(k + 1) * nodes]


def edge_call(v, w_edge, w_mesh, w_msg, w_out, w_node, bias_gain, strips, lats, lons, nodes):
    latent = w_out.shape[-1]
    slots = lons * v.shape[-1]
    cols, batch = strips[0].shape[1:3]
    positions = sum(s.shape[0] for s in strips) * cols
    whole = lambda a: pl.BlockSpec(a.shape, lambda r: (0,) * a.ndim)
    pick = lambda k, *shape: pl.BlockSpec((1,) + shape, lambda r: (k,) + (0,) * len(shape))
    block = jax.ShapeDtypeStruct((nodes, batch, latent), F32)
    row = jax.ShapeDtypeStruct((nodes, latent), F32)
    outs = [block] * 4 + [row] * 2
    return pl.pallas_call(
        functools.partial(edge_kernel, lats=lats, lons=lons),
        grid=(1,),
        in_specs=[whole(v), whole(w_edge), whole(w_mesh), whole(w_msg), pick(1, latent, latent), pick(2, latent, latent),
                  pick(3, latent, latent), pl.BlockSpec((latent, latent), lambda r: (0, 0)), whole(bias_gain)]
        + [pl.BlockSpec(memory_space=pl.ANY)] * 3,
        out_specs=[whole(o) for o in outs],
        out_shape=outs,
        scratch_shapes=[
            pltpu.VMEM((positions, batch, latent), BF16),
            pltpu.VMEM((slots, latent), F32),
            pltpu.VMEM((slots, latent), F32),
            pltpu.VMEM((lons * nodes, latent), F32),
            pltpu.VMEM((8, slots), jnp.int32),
            pltpu.SMEM((8, slots), jnp.int32),
            pltpu.VMEM((lons * nodes + 1, batch, latent), F32),
            pltpu.VMEM((TILE * batch, latent), BF16),
            pltpu.SemaphoreType.DMA((3,)),
            pltpu.SemaphoreType.DMA],
        cost_estimate=pl.CostEstimate(
            flops=4 * slots // 4 * batch * latent * latent, transcendentals=0, bytes_accessed=2 * positions * batch * latent),
        name='edges',
    )(v, w_edge, w_mesh, w_msg, w_out, w_out, w_out, w_node, bias_gain, *strips)


def node_kernel(own_ref, r1_ref, r2_ref, r3_ref, vm_ref, nb_ref, wn_ref, w4_ref, bg_ref, out_ref, scr):
    nodes, batch, latent = own_ref.shape
    agg = (own_ref[...] + r1_ref[...] + r2_ref[...] + r3_ref[...]).astype(BF16).reshape(nodes * batch, latent)
    acc = mm(agg, wn_ref[...]).reshape(nodes, batch, latent) + nb_ref[...].reshape(nodes, 1, latent)
    bg = bg_ref[0]
    upd = mlp_tail(acc.reshape(nodes * batch, latent), w4_ref[0], bg)
    out = (upd.reshape(nodes, batch, latent) + vm_ref[...].reshape(nodes, 1, latent)).reshape(nodes * batch, latent)

    def put(b, k, part):
        out_ref[b, :, 128 * k:128 * (k + 1)] = part

    swap_rows(out, scr, batch, put)


def node_call(blocks, vm, nb, w_node, w_out, bias_gain):
    nodes, batch, latent = blocks[0].shape
    whole = lambda a: pl.BlockSpec(a.shape, lambda r: (0,) * a.ndim)
    pick = lambda k, *shape: pl.BlockSpec((1,) + shape, lambda r: (k,) + (0,) * len(shape))
    out = jax.ShapeDtypeStruct((batch, nodes, latent), BF16)
    return pl.pallas_call(
        node_kernel,
        grid=(1,),
        in_specs=[whole(b) for b in blocks] + [whole(vm), whole(nb), pl.BlockSpec((latent, latent), lambda r: (1, 0)),
                                               pick(4, latent, latent), pick(4, 4, latent)],
        out_specs=whole(out),
        out_shape=out,
        scratch_shapes=[pltpu.VMEM((latent // 128, nodes * (batch + 8), 128), F32)],
        name='nodes',
    )(*blocks, vm, nb, w_node, w_out, bias_gain)


def solution(mesh):
    lats = mesh.shape['lat']
    lons = mesh.shape['lon']
    south_shift = [(s, s + 1) for s in range(lats - 1)]
    north_shift = [(s + 1, s) for s in range(lats - 1)]

    def cell_step(grid_in, mesh_in, edge_in, senders, edge_mask, w_grid, w_mesh, w_edge, w_msg, w_node, w_gupd, w_out, bias_gain):
        batch, rows, cols, _ = grid_in.shape
        nodes, per_node = senders.shape
        latent = w_out.shape[-1]
        grid_cols = cols * lons
        lon = lax.axis_index('lon')
        node_id = jnp.broadcast_to((jnp.arange(nodes) + lon * nodes)[:, None], (nodes, per_node))
        cols_of = [edge_in[..., k] for k in range(4)]
        cols_of += [(senders // grid_cols).astype(BF16), (senders % grid_cols).astype(BF16)]
        cols_of += [edge_mask.astype(BF16), node_id.astype(BF16)]
        cols_of += [jnp.broadcast_to(mesh_in[:, k:k + 1], (nodes, per_node)) for k in range(3)]
        cols_of += [jnp.zeros((nodes, per_node), BF16)] * (FEATS - len(cols_of))
        feats = jnp.stack(cols_of, axis=0).reshape(FEATS, nodes * per_node)
        we = jnp.zeros((FEATS, latent), BF16).at[0:4].set(w_edge)
        wm = jnp.zeros((FEATS, latent), BF16).at[8:11].set(w_mesh)
        vg, tr, north, south, band = embed_call(grid_in, w_grid, w_out, bias_gain, feats, lats, lons, 4)
        own, p1, p2, p3, vm, nb = edge_call(
            band, we, wm, w_msg, w_out, w_node, bias_gain, (north, tr, south), lats, lons, nodes)
        pairs = lambda k, polar: [
            (j * lats + i, (j + k) % lons * lats + i) for i in range(lats) for j in range(lons)
            if not polar or i in (0, lats - 1)]
        got = [lax.ppermute(p, ('lon', 'lat'), pairs(k, 1 < k < lons - 1)) for k, p in ((2, p2), (1, p1), (3, p3))]
        flat = update_call(vg.reshape(batch * rows * cols, latent), w_gupd, w_out, bias_gain, nb, 1024)
        grid_out = flat.reshape(batch, rows, cols, latent)
        mesh_out = node_call([own] + got, vm, nb, w_node, w_out, bias_gain)
        return mesh_out, grid_out

    grid_spec = P('dp', 'lat', 'lon', None)
    node_spec = P(('lat', 'lon'), None)
    slot_spec = P(('lat', 'lon'), None, None)
    in_specs = (grid_spec, node_spec, slot_spec, node_spec, node_spec) + (P(),) * 8
    out_specs = (P('dp', ('lat', 'lon'), None), grid_spec)
    return jax.shard_map(cell_step, mesh=mesh, in_specs=in_specs, out_specs=out_specs, check_vma=False)
```

```python
import functools

import jax
import jax.numpy as jnp
from jax import lax
from jax.experimental import pallas as pl
from jax.experimental.pallas import tpu as pltpu
from jax.sharding import PartitionSpec as P

REACH = 3
LN_EPS = 1e-5
FEATS = 16
TILE = 32
SUB = 256
F32 = jnp.float32
BF16 = jnp.bfloat16


def mm(a, b):
    return jnp.dot(a, b, preferred_element_type=F32)


def mm_nt(a, b):
    return lax.dot_general(a, b, (((1,), (1,)), ((), ())), preferred_element_type=F32)


def gate(t):
    return (t + t * jnp.tanh(t)).astype(BF16)


def swish(x):
    return gate(x * 0.5)


def norm(y):
    scale = 1.0 / y.shape[-1]
    centered = y - jnp.sum(y, axis=-1, keepdims=True) * scale
    var = jnp.sum(centered * centered, axis=-1, keepdims=True) * scale
    return centered * lax.rsqrt(var + LN_EPS)


def mlp_tail(pre, w2, bg):
    y = mm(swish(pre), w2) + bg[1:2]
    return norm(y) * bg[2:3] + bg[3:4]


def swap_rows(value, scr, inner, put):
    outer = value.shape[0] // inner
    pitch = scr.shape[1] // outer
    for k in range(scr.shape[0]):
        for b in range(outer):
            scr[k, pl.ds(b * pitch, inner), :] = value[b * inner:(b + 1) * inner, 128 * k:128 * (k + 1)]
    for c in range(inner):
        for k in range(scr.shape[0]):
            put(c, k, scr[k, pl.ds(c, outer, stride=pitch), :].astype(BF16))


def pack_slots(send_ref, mask_ref, edge_ref, mesh_ref, lanes, table, lon, grid_cols):
    nodes, per_node = send_ref.shape
    bits = grid_cols.bit_length() - 1
    send = send_ref[...]
    row = lax.shift_right_logical(send, bits).astype(F32)
    col = (send & (grid_cols - 1)).astype(F32)
    mask = mask_ref[...].astype(F32)
    mesh = mesh_ref[...].astype(F32)
    pieces = []
    for n in range(nodes):
        here = slice(n, n + 1)
        lanes[...] = jnp.zeros_like(lanes)
        lanes[0:4, 0:per_node] = edge_ref[n].astype(F32)
        lanes[4:5, 0:per_node] = row[here]
        lanes[5:6, 0:per_node] = col[here]
        lanes[6:7, 0:per_node] = mask[here]
        lanes[7:8, 0:per_node] = jnp.full((1, per_node), n, F32) + (lon * nodes).astype(F32)
        lanes[8:11, 0:per_node] = jnp.broadcast_to(mesh[:, here], (3, per_node))
        pieces.append(lanes[...])
    for p in range(nodes // 2):
        table[:, 128 * p:128 * (p + 1)] = pieces[p] + pltpu.roll(pieces[p + nodes // 2], 64, 1)


def embed_kernel(x_ref, wg_ref, w0_ref, bg_ref, send_ref, mask_ref, edge_ref, mesh_ref,
                 vg_ref, tr_ref, north_ref, south_ref, band_ref,
                 scr, half, lanes, table, feat_ref, up_buf, down_buf, up_sems, down_sems, feat_send, feat_recv, own_sem, *, lats, lons):
    batch, block, cols, chans = x_ref.shape
    latent = vg_ref.shape[-1]
    step = pl.program_id(0)
    last = pl.num_programs(0) - 1
    lat = lax.axis_index('lat')
    lon = lax.axis_index('lon')
    mesh_id = pl.DeviceIdType.MESH

    def strip(src, dst, sems, to):
        return pltpu.make_async_remote_copy(src, dst, sems.at[0], sems.at[1], device_id={'lat': to}, device_id_type=mesh_id)

    north_send = strip(up_buf, south_ref, up_sems, lat - 1)
    south_send = strip(down_buf, north_ref, down_sems, lat + 1)
    feats = [pltpu.make_async_remote_copy(
        feat_ref, band_ref.at[lon], feat_send.at[k - 1], feat_recv.at[k - 1],
        device_id={'lon': lax.rem(lon + k, lons)}, device_id_type=mesh_id) for k in range(1, lons)]
    own = pltpu.make_async_copy(feat_ref, band_ref.at[lon], own_sem)

    @pl.when(step == 0)
    def _():
        barrier = pltpu.get_barrier_semaphore()
        for k in range(1, lons):
            pl.semaphore_signal(barrier, 1, device_id={'lon': lax.rem(lon + k, lons)}, device_id_type=mesh_id)

        @pl.when(lat > 0)
        def _():
            pl.semaphore_signal(barrier, 1, device_id={'lat': lat - 1}, device_id_type=mesh_id)

        @pl.when(lat < lats - 1)
        def _():
            pl.semaphore_signal(barrier, 1, device_id={'lat': lat + 1}, device_id_type=mesh_id)

        pack_slots(send_ref, mask_ref, edge_ref, mesh_ref, lanes, table, lon, cols * lons)
        feat_ref[...] = table[...].astype(BF16)

    @pl.when(step == 1)
    def _():
        barrier = pltpu.get_barrier_semaphore()
        inner = (lat > 0).astype(jnp.int32) + (lat < lats - 1).astype(jnp.int32)
        pl.semaphore_wait(barrier, lons - 1 + inner)

        @pl.when(lat > 0)
        def _():
            north_send.start()

        own.start()
        for copy in feats:
            copy.start()

    @pl.when((step == 2) & (lat < lats - 1))
    def _():
        south_send.start()

    rows = batch * cols
    halve(half, wg_ref)
    bg = bg_ref[0]
    b1 = bg[0:1] * 0.5

    def first(r):
        return gate(mm(x_ref[:, r].reshape(rows, chans), half[...]) + b1)

    def second(r, hid):
        vg = norm(mm(hid, w0_ref[0]) + bg[1:2]) * bg[2:3] + bg[3:4]
        vg_ref[:, r] = vg.astype(BF16).reshape(batch, cols, latent)

        def put(c, k, part):
            tr_ref[r, c, :, 128 * k:128 * (k + 1)] = part

        swap_rows(vg, scr.at[r], cols, put)

    staged(block, first, second)

    @pl.when(step == 0)
    def _():
        up_buf[...] = tr_ref[0:REACH]

    @pl.when(step == 1)
    def _():
        down_buf[...] = tr_ref[block - REACH:]

    @pl.when(step == last)
    def _():
        own.wait()
        for copy in feats:
            copy.wait()

        @pl.when(lat > 0)
        def _():
            north_send.wait_send()
            south_send.wait_recv()

        @pl.when(lat < lats - 1)
        def _():
            south_send.wait_send()
            north_send.wait_recv()


def embed_call(grid_in, w_grid, w_out, bias_gain, senders, edge_mask, edge_t, mesh_t, lats, lons, block):
    batch, rows, cols, chans = grid_in.shape
    latent = w_out.shape[-1]
    steps = rows // block
    nodes = senders.shape[0]
    feats = jax.ShapeDtypeStruct((FEATS, nodes // 2 * 128), BF16)
    whole = lambda *shape: pl.BlockSpec(shape, lambda r: (0,) * len(shape))
    pick = lambda k, *shape: pl.BlockSpec((1,) + shape, lambda r: (k,) + (0,) * len(shape))
    at = lambda r: lax.rem(r * (steps - 1), steps)
    strip = jax.ShapeDtypeStruct((REACH, cols, batch, latent), BF16)
    anywhere = pl.BlockSpec(memory_space=pl.ANY)
    return pl.pallas_call(
        functools.partial(embed_kernel, lats=lats, lons=lons),
        grid=(steps,),
        in_specs=[
            pl.BlockSpec((batch, block, cols, chans), lambda r: (0, at(r), 0, 0)),
            whole(chans, latent), pick(0, latent, latent), pick(0, 4, latent), whole(*senders.shape),
            whole(*edge_mask.shape), whole(*edge_t.shape), whole(*mesh_t.shape)],
        out_specs=[
            pl.BlockSpec((batch, block, cols, latent), lambda r: (0, at(r), 0, 0)),
            pl.BlockSpec((block, cols, batch, latent), lambda r: (at(r), 0, 0, 0)),
            anywhere, anywhere, anywhere],
        out_shape=[
            jax.ShapeDtypeStruct((batch, rows, cols, latent), BF16),
            jax.ShapeDtypeStruct((rows, cols, batch, latent), BF16),
            strip, strip, jax.ShapeDtypeStruct((lons,) + feats.shape, BF16)],
        scratch_shapes=[
            pltpu.VMEM((block, latent // 128, batch * (cols + 8), 128), F32),
            pltpu.VMEM((chans, latent), BF16), pltpu.VMEM((FEATS, 128), F32), pltpu.VMEM(feats.shape, F32),
            pltpu.VMEM(feats.shape, BF16), pltpu.VMEM(strip.shape, BF16), pltpu.VMEM(strip.shape, BF16),
            pltpu.SemaphoreType.DMA((2,)), pltpu.SemaphoreType.DMA((2,)),
            pltpu.SemaphoreType.DMA((lons - 1,)), pltpu.SemaphoreType.DMA((lons - 1,)), pltpu.SemaphoreType.DMA],
        compiler_params=pltpu.CompilerParams(collective_id=0, has_side_effects=True),
        cost_estimate=pl.CostEstimate(
            flops=4 * rows * batch * cols * latent * latent, transcendentals=0,
            bytes_accessed=6 * rows * batch * cols * latent),
        name='embed',
    )(grid_in, w_grid, w_out, bias_gain, senders, edge_mask, edge_t, mesh_t)


def halve(dst, src):
    @pl.when(pl.program_id(0) == 0)
    def _():
        dst[...] = src[...] * jnp.asarray(0.5, BF16)


def staged(count, first, second):
    hid = first(0)
    for i in range(count):
        nxt = first(i + 1) if i + 1 < count else None
        second(i, hid)
        hid = nxt


def update_kernel(vg_ref, wu_ref, w5_ref, bg_ref, dep_ref, out_ref, half):
    halve(half, wu_ref)
    bg = bg_ref[0]
    b1 = bg[0:1] * 0.5

    def first(i):
        return gate(mm(vg_ref[i * SUB:(i + 1) * SUB], half[...]) + b1)

    def second(i, hid):
        upd = norm(mm(hid, w5_ref[0]) + bg[1:2]) * bg[2:3] + bg[3:4]
        out_ref[i * SUB:(i + 1) * SUB] = (vg_ref[i * SUB:(i + 1) * SUB].astype(F32) + upd).astype(BF16)

    staged(out_ref.shape[0] // SUB, first, second)


def update_call(vg, w_gupd, w_out, bias_gain, dep, block):
    rows, latent = vg.shape
    pick = lambda k, *shape: pl.BlockSpec((1,) + shape, lambda r: (k,) + (0,) * len(shape))
    tile = pl.BlockSpec((block, latent), lambda r: (r, 0))
    return pl.pallas_call(
        update_kernel,
        grid=(rows // block,),
        in_specs=[tile, pl.BlockSpec((latent, latent), lambda r: (0, 0)), pick(5, latent, latent), pick(5, 4, latent),
                  pl.BlockSpec(memory_space=pl.ANY)],
        out_specs=tile,
        out_shape=jax.ShapeDtypeStruct(vg.shape, BF16),
        scratch_shapes=[pltpu.VMEM((latent, latent), BF16)],
        cost_estimate=pl.CostEstimate(flops=4 * rows * latent * latent, transcendentals=0, bytes_accessed=4 * rows * latent),
        name='update',
    )(vg, w_gupd, w_out, bias_gain, dep)


def edge_kernel(v_ref, we_ref, wm_ref, wmsg_ref, w1_ref, w2_ref, w3_ref, wn_ref, bg_ref,
                north_ref, mid_ref, south_ref,
                own_ref, p1_ref, p2_ref, p3_ref, vm_ref, nb_ref,
                table, lp, ec, vmf, idx_v, idx_s, part, half, hid_a, hid_b, xbuf, sems, isem, *, lats, lons):
    latent = w1_ref.shape[-1]
    slots = lons * v_ref.shape[-1]
    cols, batch = mid_ref.shape[1:3]
    nodes = own_ref.shape[0]
    band = lons * nodes
    lat = lax.axis_index('lat')
    lon = lax.axis_index('lon')
    copies = []
    start = 0
    for k, ref in enumerate((north_ref, mid_ref, south_ref)):
        count = ref.shape[0] * cols
        src = ref.reshape(count, batch, latent)
        copy = pltpu.make_async_copy(src, table.at[pl.ds(start, count)], sems.at[k])
        copy.start()
        copies.append(copy)
        start += count
    positions = start
    cell_rows = positions // cols - 2 * REACH

    vtb = jnp.concatenate([v_ref[k] for k in range(lons)], axis=1)
    vt = vtb.astype(F32)
    ids = lax.broadcasted_iota(jnp.int32, (band, slots), 0)
    local = lax.rem(ids, nodes)
    pick_row = lax.div(ids, nodes) * (slots // lons) + lax.rem(local, nodes // 2) * 128 + lax.div(local, nodes // 2) * 64
    pick = lax.broadcasted_iota(jnp.int32, (band, slots), 1) == pick_row
    mesh_feat = mm_nt(jnp.where(pick, 1.0, 0.0).astype(BF16), vtb).astype(BF16)
    we = jnp.concatenate([we_ref[...].astype(F32), jnp.zeros((FEATS - 4, latent), F32)], axis=0).astype(BF16)
    wm = jnp.concatenate(
        [jnp.zeros((8, latent), F32), wm_ref[...].astype(F32), jnp.zeros((FEATS - 11, latent), F32)], axis=0).astype(BF16)
    bg1 = bg_ref[1]
    bg2 = bg_ref[2]
    bg3 = bg_ref[3]
    vm = mlp_tail(mm(mesh_feat, wm) + bg1[0:1], w1_ref[0], bg1).astype(BF16)
    vmf[...] = vm.astype(F32)
    own_vm = vmf[pl.ds(pl.multiple_of(lon * nodes, 8), nodes), :]
    vm_ref[...] = own_vm
    nb_ref[...] = mm(own_vm.astype(BF16), wn_ref[...]) + bg_ref[4][0:1]

    col = vt[5:6] - (lon * cols).astype(F32)
    flag = jnp.where((vt[6:7] > 0.5) & (col > -0.5) & (col < cols - 0.5), 1.0, 0.0)
    chunks = slots // 128
    pad = -chunks % 16
    rows = [flag[:, 128 * c:128 * (c + 1)] for c in range(chunks)] + [jnp.zeros((pad, 128), F32)] * (pad > 0)
    flags = jnp.concatenate(rows, axis=0)
    up = lax.broadcasted_iota(jnp.int32, (128, 128), 0) <= lax.broadcasted_iota(jnp.int32, (128, 128), 1)
    incl = mm(flags.astype(BF16), jnp.where(up, 1.0, 0.0).astype(BF16))
    n_rows = chunks + pad
    low = lax.broadcasted_iota(jnp.int32, (n_rows, n_rows), 1) < lax.broadcasted_iota(jnp.int32, (n_rows, n_rows), 0)
    row_sum = jnp.broadcast_to(incl[:, 127:128], (n_rows, 128)).astype(BF16)
    before = mm(jnp.where(low, 1.0, 0.0).astype(BF16), row_sum)
    rank = jnp.where(flags > 0.5, incl + before - 1.0, -1.0)
    total = jnp.sum(flag).astype(jnp.int32)

    def prep(t, carry):
        slot = (lax.broadcasted_iota(jnp.int32, (128, 128), 0) + t * 128).astype(F32)
        sel = jnp.concatenate(
            [jnp.where(rank[c:c + 1] == slot, 1.0, 0.0).astype(BF16) for c in range(chunks)], axis=1)
        feat = mm_nt(sel, vtb).astype(BF16)
        feat_t = mm_nt(vtb, sel)
        here = pl.ds(pl.multiple_of(t * 128, 128), 128)
        live = lax.broadcasted_iota(jnp.int32, (1, 128), 1) + t * 128 < total
        win_r = feat_t[4:5] - (lat * cell_rows - REACH).astype(F32)
        win_c = feat_t[5:6] - (lon * cols).astype(F32)
        pos = jnp.where(live, (win_r * cols + win_c).astype(jnp.int32), REACH * cols)
        node = feat_t[7:8].astype(jnp.int32)
        rel = lax.rem(node + (lons - lon) * nodes, band)
        idx_v[0:1, here] = jnp.clip(pos, 0, positions - 1)
        idx_v[1:2, here] = jnp.where(live, rel, band)
        edge = mlp_tail(mm(feat, we) + bg2[0:1], w2_ref[0], bg2).astype(BF16)
        node_col = feat[:, 7:8].astype(F32)
        hot = lax.broadcasted_iota(jnp.int32, (128, band), 1).astype(F32) == node_col
        vm_e = mm(jnp.where(hot, 1.0, 0.0).astype(BF16), vm).astype(BF16)
        lp[here, :] = (mm(edge, wmsg_ref[0:latent, :]) + mm(vm_e, wmsg_ref[2 * latent:, :]) + bg3[0:1]) * 0.5
        ec[here, :] = edge.astype(F32) + bg3[3:4]
        return carry

    lax.fori_loop(0, lax.div(total + 127, 128), prep, 0)
    move = pltpu.make_async_copy(idx_v, idx_s, isem)
    move.start()
    part[...] = jnp.zeros_like(part)
    half[...] = wmsg_ref[latent:2 * latent, :] * jnp.asarray(0.5, BF16)
    move.wait()
    for copy in copies:
        copy.wait()

    per = TILE // 2
    bufs = (xbuf.at[0], xbuf.at[1])
    hids = (hid_a, hid_b)

    def first(base, k):
        for s in range(per):
            bufs[k][pl.ds(s * batch, batch), :] = table[idx_s[0, base + s]]
        acc = mm(bufs[k][...], half[...]).reshape(per, batch, latent)
        here = pl.ds(pl.multiple_of(base, per), per)
        hids[k][...] = gate(acc + lp[here, :].reshape(per, 1, latent)).reshape(per * batch, latent)

    def second(base, k):
        y = mm(hids[k][...], w3_ref[0]) + bg3[1:2]
        here = pl.ds(pl.multiple_of(base, per), per)
        z = (norm(y) * bg3[2:3]).reshape(per, batch, latent) + ec[here, :].reshape(per, 1, latent)
        z = z.astype(BF16).astype(F32)
        for s in range(per):
            n = idx_s[1, base + s]
            part[n] += z[s]

    tiles = lax.div(total + TILE - 1, TILE)

    @pl.when(tiles > 0)
    def _():
        first(0, 0)

    def edges(t, carry):
        base = t * TILE
        first(base + per, 1)
        second(base, 0)
        first(jnp.minimum(t + 1, tiles - 1) * TILE, 0)
        second(base + per, 1)
        return carry

    lax.fori_loop(0, tiles, edges, 0)
    for k, ref in enumerate((own_ref, p1_ref, p2_ref, p3_ref)):
        ref[...] = part[k * nodes:(k + 1) * nodes]


def edge_call(v, w_edge, w_mesh, w_msg, w_out, w_node, bias_gain, strips, lats, lons, nodes):
    latent = w_out.shape[-1]
    slots = lons * v.shape[-1]
    cols, batch = strips[0].shape[1:3]
    positions = sum(s.shape[0] for s in strips) * cols
    whole = lambda a: pl.BlockSpec(a.shape, lambda r: (0,) * a.ndim)
    pick = lambda k, *shape: pl.BlockSpec((1,) + shape, lambda r: (k,) + (0,) * len(shape))
    block = jax.ShapeDtypeStruct((nodes, batch, latent), F32)
    row = jax.ShapeDtypeStruct((nodes, latent), F32)
    outs = [block] * 4 + [row] * 2
    return pl.pallas_call(
        functools.partial(edge_kernel, lats=lats, lons=lons),
        grid=(1,),
        in_specs=[whole(v), whole(w_edge), whole(w_mesh), whole(w_msg), pick(1, latent, latent), pick(2, latent, latent),
                  pick(3, latent, latent), pl.BlockSpec((latent, latent), lambda r: (0, 0)), whole(bias_gain)]
        + [pl.BlockSpec(memory_space=pl.ANY)] * 3,
        out_specs=[whole(o) for o in outs],
        out_shape=outs,
        scratch_shapes=[
            pltpu.VMEM((positions, batch, latent), BF16),
            pltpu.VMEM((slots, latent), F32),
            pltpu.VMEM((slots, latent), F32),
            pltpu.VMEM((lons * nodes, latent), F32),
            pltpu.VMEM((8, slots), jnp.int32),
            pltpu.SMEM((8, slots), jnp.int32),
            pltpu.VMEM((lons * nodes + 1, batch, latent), F32),
            pltpu.VMEM((latent, latent), BF16),
            pltpu.VMEM((TILE // 2 * batch, latent), BF16),
            pltpu.VMEM((TILE // 2 * batch, latent), BF16),
            pltpu.VMEM((2, TILE // 2 * batch, latent), BF16),
            pltpu.SemaphoreType.DMA((3,)),
            pltpu.SemaphoreType.DMA],
        cost_estimate=pl.CostEstimate(
            flops=4 * slots // 4 * batch * latent * latent, transcendentals=0, bytes_accessed=2 * positions * batch * latent),
        name='edges',
    )(v, w_edge, w_mesh, w_msg, w_out, w_out, w_out, w_node, bias_gain, *strips)


def node_kernel(own_ref, r1_ref, r2_ref, r3_ref, vm_ref, nb_ref, wn_ref, w4_ref, bg_ref, out_ref, scr):
    nodes, batch, latent = own_ref.shape
    agg = (own_ref[...] + r1_ref[...] + r2_ref[...] + r3_ref[...]).astype(BF16).reshape(nodes * batch, latent)
    acc = mm(agg, wn_ref[...]).reshape(nodes, batch, latent) + nb_ref[...].reshape(nodes, 1, latent)
    bg = bg_ref[0]
    upd = mlp_tail(acc.reshape(nodes * batch, latent), w4_ref[0], bg)
    out = (upd.reshape(nodes, batch, latent) + vm_ref[...].reshape(nodes, 1, latent)).reshape(nodes * batch, latent)

    def put(b, k, part):
        out_ref[b, :, 128 * k:128 * (k + 1)] = part

    swap_rows(out, scr, batch, put)


def node_call(blocks, vm, nb, w_node, w_out, bias_gain):
    nodes, batch, latent = blocks[0].shape
    whole = lambda a: pl.BlockSpec(a.shape, lambda r: (0,) * a.ndim)
    pick = lambda k, *shape: pl.BlockSpec((1,) + shape, lambda r: (k,) + (0,) * len(shape))
    out = jax.ShapeDtypeStruct((batch, nodes, latent), BF16)
    return pl.pallas_call(
        node_kernel,
        grid=(1,),
        in_specs=[whole(b) for b in blocks] + [whole(vm), whole(nb), pl.BlockSpec((latent, latent), lambda r: (1, 0)),
                                               pick(4, latent, latent), pick(4, 4, latent)],
        out_specs=whole(out),
        out_shape=out,
        scratch_shapes=[pltpu.VMEM((latent // 128, nodes * (batch + 8), 128), F32)],
        name='nodes',
    )(*blocks, vm, nb, w_node, w_out, bias_gain)


def solution(mesh):
    lats = mesh.shape['lat']
    lons = mesh.shape['lon']
    south_shift = [(s, s + 1) for s in range(lats - 1)]
    north_shift = [(s + 1, s) for s in range(lats - 1)]

    def cell_step(grid_in, mesh_in, edge_in, senders, edge_mask, w_grid, w_mesh, w_edge, w_msg, w_node, w_gupd, w_out, bias_gain):
        batch, rows, cols, _ = grid_in.shape
        nodes = senders.shape[0]
        latent = w_out.shape[-1]
        vg, tr, north, south, band = embed_call(
            grid_in, w_grid, w_out, bias_gain, senders, edge_mask, jnp.swapaxes(edge_in, 1, 2), mesh_in.T, lats, lons, 4)
        own, p1, p2, p3, vm, nb = edge_call(
            band, w_edge, w_mesh, w_msg, w_out, w_node, bias_gain, (north, tr, south), lats, lons, nodes)
        pairs = lambda k, polar: [
            (j * lats + i, (j + k) % lons * lats + i) for i in range(lats) for j in range(lons)
            if not polar or i in (0, lats - 1)]
        got = [lax.ppermute(p, ('lon', 'lat'), pairs(k, 1 < k < lons - 1)) for k, p in ((2, p2), (1, p1), (3, p3))]
        flat = update_call(vg.reshape(batch * rows * cols, latent), w_gupd, w_out, bias_gain, nb, 2048)
        grid_out = flat.reshape(batch, rows, cols, latent)
        mesh_out = node_call([own] + got, vm, nb, w_node, w_out, bias_gain)
        return mesh_out, grid_out

    grid_spec = P('dp', 'lat', 'lon', None)
    node_spec = P(('lat', 'lon'), None)
    slot_spec = P(('lat', 'lon'), None, None)
    in_specs = (grid_spec, node_spec, slot_spec, node_spec, node_spec) + (P(),) * 8
    out_specs = (P('dp', ('lat', 'lon'), None), grid_spec)
    return jax.shard_map(cell_step, mesh=mesh, in_specs=in_specs, out_specs=out_specs, check_vma=False)
```

```python
import functools

import jax
import jax.numpy as jnp
from jax import lax
from jax.experimental import pallas as pl
from jax.experimental.pallas import tpu as pltpu
from jax.sharding import PartitionSpec as P

REACH = 3
LN_EPS = 1e-5
FEATS = 16
TILE = 32
SUB = 256
EDGE_VMEM = 20 * 2 ** 20
NODE_VMEM = 6 * 2 ** 20
GRID_VMEM = 24 * 2 ** 20
UPDATE_VMEM = 10 * 2 ** 20
F32 = jnp.float32
BF16 = jnp.bfloat16


def mm(a, b):
    return jnp.dot(a, b, preferred_element_type=F32)


def mm_nt(a, b):
    return lax.dot_general(a, b, (((1,), (1,)), ((), ())), preferred_element_type=F32)


def gate(t):
    return (t + t * jnp.tanh(t)).astype(BF16)


def swish(x):
    return gate(x * 0.5)


def norm(y):
    scale = 1.0 / y.shape[-1]
    centered = y - jnp.sum(y, axis=-1, keepdims=True) * scale
    var = jnp.sum(centered * centered, axis=-1, keepdims=True) * scale
    return centered * lax.rsqrt(var + LN_EPS)


def mlp_tail(pre, w2, bg):
    y = mm(swish(pre), w2) + bg[1:2]
    return norm(y) * bg[2:3] + bg[3:4]


def swap_rows(value, scr, inner, put):
    outer = value.shape[0] // inner
    pitch = scr.shape[1] // outer
    for k in range(scr.shape[0]):
        for b in range(outer):
            scr[k, pl.ds(b * pitch, inner), :] = value[b * inner:(b + 1) * inner, 128 * k:128 * (k + 1)]
    for c in range(inner):
        for k in range(scr.shape[0]):
            put(c, k, scr[k, pl.ds(c, outer, stride=pitch), :].astype(BF16))


def pack_slots(send_ref, mask_ref, edge_ref, mesh_ref, lanes, table, lon, grid_cols):
    nodes, per_node = send_ref.shape
    bits = grid_cols.bit_length() - 1
    send = send_ref[...]
    row = lax.shift_right_logical(send, bits).astype(F32)
    col = (send & (grid_cols - 1)).astype(F32)
    mask = mask_ref[...].astype(F32)
    mesh = mesh_ref[...].astype(F32)
    pieces = []
    for n in range(nodes):
        here = slice(n, n + 1)
        lanes[...] = jnp.zeros_like(lanes)
        lanes[0:4, 0:per_node] = edge_ref[n].astype(F32)
        lanes[4:5, 0:per_node] = row[here]
        lanes[5:6, 0:per_node] = col[here]
        lanes[6:7, 0:per_node] = mask[here]
        lanes[7:8, 0:per_node] = jnp.full((1, per_node), n, F32) + (lon * nodes).astype(F32)
        lanes[8:11, 0:per_node] = jnp.broadcast_to(mesh[:, here], (3, per_node))
        pieces.append(lanes[...])
    for p in range(nodes // 2):
        table[:, 128 * p:128 * (p + 1)] = pieces[p] + pltpu.roll(pieces[p + nodes // 2], 64, 1)


def embed_kernel(x_ref, wg_ref, w0_ref, bg_ref, send_ref, mask_ref, edge_ref, mesh_ref,
                 vg_ref, tab_ref, band_ref,
                 scr, half, lanes, table, feat_ref, up_buf, down_buf, from_south, from_north, feat_in, up_sems, down_sems, feat_send, feat_recv, *, lats, lons):
    batch, grid_rows, cols, chans = x_ref.shape
    latent = vg_ref.shape[-1]
    step = pl.program_id(0)
    last = pl.num_programs(0) - 1
    block = scr.shape[0]
    base = lax.rem(step * last, last + 1) * block

    lat = lax.axis_index('lat')
    lon = lax.axis_index('lon')
    mesh_id = pl.DeviceIdType.MESH

    def strip(src, dst, sems, to):
        return pltpu.make_async_remote_copy(src, dst, sems.at[0], sems.at[1], device_id={'lat': to}, device_id_type=mesh_id)

    north_send = strip(up_buf, from_south, up_sems, lat - 1)
    south_send = strip(down_buf, from_north, down_sems, lat + 1)
    feats = [pltpu.make_async_remote_copy(
        feat_ref, feat_in.at[lon], feat_send.at[k - 1], feat_recv.at[k - 1],
        device_id={'lon': lax.rem(lon + k, lons)}, device_id_type=mesh_id) for k in range(1, lons)]

    @pl.when(step == 0)
    def _():
        barrier = pltpu.get_barrier_semaphore()
        for k in range(1, lons):
            pl.semaphore_signal(barrier, 1, device_id={'lon': lax.rem(lon + k, lons)}, device_id_type=mesh_id)

        @pl.when(lat > 0)
        def _():
            pl.semaphore_signal(barrier, 1, device_id={'lat': lat - 1}, device_id_type=mesh_id)

        @pl.when(lat < lats - 1)
        def _():
            pl.semaphore_signal(barrier, 1, device_id={'lat': lat + 1}, device_id_type=mesh_id)

        pack_slots(send_ref, mask_ref, edge_ref, mesh_ref, lanes, table, lon, cols * lons)
        feat_ref[...] = table[...].astype(BF16)

    @pl.when(step == 1)
    def _():
        barrier = pltpu.get_barrier_semaphore()
        inner = (lat > 0).astype(jnp.int32) + (lat < lats - 1).astype(jnp.int32)
        pl.semaphore_wait(barrier, lons - 1 + inner)

        @pl.when(lat > 0)
        def _():
            north_send.start()

        feat_in[lon] = feat_ref[...]
        for copy in feats:
            copy.start()

    @pl.when((step == 2) & (lat < lats - 1))
    def _():
        south_send.start()

    rows = batch * cols
    halve(half, wg_ref)
    bg = bg_ref[0]
    b1 = bg[0:1] * 0.5

    def first(r):
        return gate(mm(x_ref[:, base + r].reshape(rows, chans), half[...]) + b1)

    def second(r, hid):
        vg = norm(mm(hid, w0_ref[0]) + bg[1:2]) * bg[2:3] + bg[3:4]
        vg_ref[:, base + r] = vg.astype(BF16).reshape(batch, cols, latent)

        def put(c, k, part):
            tab_ref[REACH + base + r, c, :, 128 * k:128 * (k + 1)] = part

        swap_rows(vg, scr.at[r], cols, put)

    staged(block, first, second)

    @pl.when(step == 0)
    def _():
        up_buf[...] = tab_ref[REACH:2 * REACH]

    @pl.when(step == 1)
    def _():
        down_buf[...] = tab_ref[grid_rows:grid_rows + REACH]

    @pl.when(step == last)
    def _():
        for copy in feats:
            copy.wait()
        band_ref[...] = feat_in[...]

        @pl.when(lat > 0)
        def _():
            north_send.wait_send()
            south_send.wait_recv()
            tab_ref[0:REACH] = from_north[...]

        @pl.when(lat < lats - 1)
        def _():
            south_send.wait_send()
            north_send.wait_recv()
            tab_ref[grid_rows + REACH:grid_rows + 2 * REACH] = from_south[...]


def embed_call(grid_in, w_grid, w_out, bias_gain, senders, edge_mask, edge_t, mesh_t, lats, lons, block):
    batch, rows, cols, chans = grid_in.shape
    latent = w_out.shape[-1]
    steps = rows // block
    nodes = senders.shape[0]
    feats = jax.ShapeDtypeStruct((FEATS, nodes // 2 * 128), BF16)
    whole = lambda *shape: pl.BlockSpec(shape, lambda r: (0,) * len(shape))
    pick = lambda k, *shape: pl.BlockSpec((1,) + shape, lambda r: (k,) + (0,) * len(shape))
    strip = (REACH, cols, batch, latent)
    local = pl.BlockSpec(memory_space=pltpu.VMEM)
    return pl.pallas_call(
        functools.partial(embed_kernel, lats=lats, lons=lons),
        grid=(steps,),
        in_specs=[
            local,
            whole(chans, latent), pick(0, latent, latent), pick(0, 4, latent), whole(*senders.shape),
            whole(*edge_mask.shape), whole(*edge_t.shape), whole(*mesh_t.shape)],
        out_specs=[local, local, local],
        out_shape=[
            jax.ShapeDtypeStruct((batch, rows, cols, latent), BF16),
            jax.ShapeDtypeStruct((rows + 2 * REACH, cols, batch, latent), BF16),
            jax.ShapeDtypeStruct((lons,) + feats.shape, BF16)],
        scratch_shapes=[
            pltpu.VMEM((block, latent // 128, batch * (cols + 8), 128), F32),
            pltpu.VMEM((chans, latent), BF16), pltpu.VMEM((FEATS, 128), F32), pltpu.VMEM(feats.shape, F32),
            pltpu.VMEM(feats.shape, BF16),
            pltpu.VMEM(strip, BF16), pltpu.VMEM(strip, BF16), pltpu.VMEM(strip, BF16), pltpu.VMEM(strip, BF16),
            pltpu.VMEM((lons,) + feats.shape, BF16),
            pltpu.SemaphoreType.DMA((2,)), pltpu.SemaphoreType.DMA((2,)),
            pltpu.SemaphoreType.DMA((lons - 1,)), pltpu.SemaphoreType.DMA((lons - 1,))],
        compiler_params=pltpu.CompilerParams(collective_id=0, has_side_effects=True, vmem_limit_bytes=GRID_VMEM),
        cost_estimate=pl.CostEstimate(
            flops=4 * rows * batch * cols * latent * latent, transcendentals=0,
            bytes_accessed=6 * rows * batch * cols * latent),
        name='embed',
    )(grid_in, w_grid, w_out, bias_gain, senders, edge_mask, edge_t, mesh_t)


def halve(dst, src):
    @pl.when(pl.program_id(0) == 0)
    def _():
        dst[...] = src[...] * jnp.asarray(0.5, BF16)


def staged(count, first, second):
    hid = first(0)
    for i in range(count):
        nxt = first(i + 1) if i + 1 < count else None
        second(i, hid)
        hid = nxt


def update_kernel(vg_ref, wu_ref, w5_ref, bg_ref, dep_ref, out_ref, half):
    halve(half, wu_ref)
    bg = bg_ref[0]
    b1 = bg[0:1] * 0.5
    base = pl.program_id(0) * out_ref.shape[0]

    def rows(i):
        return pl.ds(pl.multiple_of(base + i * SUB, SUB), SUB)

    def first(i):
        return gate(mm(vg_ref[rows(i), :], half[...]) + b1)

    def second(i, hid):
        upd = norm(mm(hid, w5_ref[0]) + bg[1:2]) * bg[2:3] + bg[3:4]
        out_ref[i * SUB:(i + 1) * SUB] = (vg_ref[rows(i), :].astype(F32) + upd).astype(BF16)

    staged(out_ref.shape[0] // SUB, first, second)


def update_call(vg, w_gupd, w_out, bias_gain, dep, block):
    rows, latent = vg.shape
    pick = lambda k, *shape: pl.BlockSpec((1,) + shape, lambda r: (k,) + (0,) * len(shape))
    tile = pl.BlockSpec((block, latent), lambda r: (r, 0))
    return pl.pallas_call(
        update_kernel,
        grid=(rows // block,),
        in_specs=[pl.BlockSpec(memory_space=pltpu.VMEM), pl.BlockSpec((latent, latent), lambda r: (0, 0)), pick(5, latent, latent), pick(5, 4, latent),
                  pl.BlockSpec(memory_space=pl.ANY)],
        out_specs=tile,
        out_shape=jax.ShapeDtypeStruct(vg.shape, BF16),
        scratch_shapes=[pltpu.VMEM((latent, latent), BF16)],
        cost_estimate=pl.CostEstimate(flops=4 * rows * latent * latent, transcendentals=0, bytes_accessed=4 * rows * latent),
        compiler_params=pltpu.CompilerParams(vmem_limit_bytes=UPDATE_VMEM),
        name='update',
    )(vg, w_gupd, w_out, bias_gain, dep)


def edge_kernel(v_ref, we_ref, wm_ref, wmsg_ref, wo_ref, wn_ref, bg_ref,
                tab_ref, *rest, lats, lons, near):
    lp, ec, vmf, idx_v, idx_s, part, half, hid_a, hid_b, xbuf, isem = rest[-11:]
    outs = rest[:-11]
    latent = wo_ref.shape[-1]
    slots = lons * v_ref.shape[-1]
    grid_rows, cols, batch = tab_ref.shape[:3]
    positions = grid_rows * cols
    cell_rows = grid_rows - 2 * REACH
    table = tab_ref.reshape(positions, batch, latent)
    nodes = outs[0].shape[0]
    band = lons * nodes
    lat = lax.axis_index('lat')
    lon = lax.axis_index('lon')
    vtb = jnp.concatenate([v_ref[k] for k in range(lons)], axis=1)
    vt = vtb.astype(F32)
    ids = lax.broadcasted_iota(jnp.int32, (band, slots), 0)
    local = lax.rem(ids, nodes)
    pick_row = lax.div(ids, nodes) * (slots // lons) + lax.rem(local, nodes // 2) * 128 + lax.div(local, nodes // 2) * 64
    pick = lax.broadcasted_iota(jnp.int32, (band, slots), 1) == pick_row
    mesh_feat = mm_nt(jnp.where(pick, 1.0, 0.0).astype(BF16), vtb).astype(BF16)
    we = jnp.concatenate([we_ref[...].astype(F32), jnp.zeros((FEATS - 4, latent), F32)], axis=0).astype(BF16)
    wm = jnp.concatenate(
        [jnp.zeros((8, latent), F32), wm_ref[...].astype(F32), jnp.zeros((FEATS - 11, latent), F32)], axis=0).astype(BF16)
    bg1 = bg_ref[1]
    bg2 = bg_ref[2]
    bg3 = bg_ref[3]
    vm = mlp_tail(mm(mesh_feat, wm) + bg1[0:1], wo_ref[1], bg1).astype(BF16)
    if near:
        vmf[...] = vm.astype(F32)
        own_vm = vmf[pl.ds(pl.multiple_of(lon * nodes, 8), nodes), :]
        outs[1][...] = own_vm
        outs[2][...] = mm(own_vm.astype(BF16), wn_ref[0:latent, :]) + bg_ref[4][0:1]

    col = vt[5:6] - (lon * cols).astype(F32)
    cell = vt[7:8] - (lon * nodes).astype(F32)
    inner = (cell > -0.5) & (cell < nodes - 0.5)
    wanted = inner if near else jnp.logical_not(inner)
    flag = jnp.where((vt[6:7] > 0.5) & (col > -0.5) & (col < cols - 0.5) & wanted, 1.0, 0.0)
    chunks = slots // 128
    pad = -chunks % 16
    rows = [flag[:, 128 * c:128 * (c + 1)] for c in range(chunks)] + [jnp.zeros((pad, 128), F32)] * (pad > 0)
    flags = jnp.concatenate(rows, axis=0)
    up = lax.broadcasted_iota(jnp.int32, (128, 128), 0) <= lax.broadcasted_iota(jnp.int32, (128, 128), 1)
    incl = mm(flags.astype(BF16), jnp.where(up, 1.0, 0.0).astype(BF16))
    n_rows = chunks + pad
    low = lax.broadcasted_iota(jnp.int32, (n_rows, n_rows), 1) < lax.broadcasted_iota(jnp.int32, (n_rows, n_rows), 0)
    row_sum = jnp.broadcast_to(incl[:, 127:128], (n_rows, 128)).astype(BF16)
    before = mm(jnp.where(low, 1.0, 0.0).astype(BF16), row_sum)
    rank = jnp.where(flags > 0.5, incl + before - 1.0, -1.0)
    total = jnp.sum(flag).astype(jnp.int32)

    def prep(t, carry):
        slot = (lax.broadcasted_iota(jnp.int32, (128, 128), 0) + t * 128).astype(F32)
        sel = jnp.concatenate(
            [jnp.where(rank[c:c + 1] == slot, 1.0, 0.0).astype(BF16) for c in range(chunks)], axis=1)
        feat = mm_nt(sel, vtb).astype(BF16)
        feat_t = mm_nt(vtb, sel)
        here = pl.ds(pl.multiple_of(t * 128, 128), 128)
        live = lax.broadcasted_iota(jnp.int32, (1, 128), 1) + t * 128 < total
        win_r = feat_t[4:5] - (lat * cell_rows - REACH).astype(F32)
        win_c = feat_t[5:6] - (lon * cols).astype(F32)
        pos = jnp.where(live, (win_r * cols + win_c).astype(jnp.int32), REACH * cols)
        node = feat_t[7:8].astype(jnp.int32)
        rel = lax.rem(node + (lons - lon) * nodes, band)
        idx_v[0:1, here] = jnp.clip(pos, 0, positions - 1)
        idx_v[1:2, here] = jnp.where(live, rel, band)
        edge = mlp_tail(mm(feat, we) + bg2[0:1], wo_ref[2], bg2).astype(BF16)
        node_col = feat[:, 7:8].astype(F32)
        hot = lax.broadcasted_iota(jnp.int32, (128, band), 1).astype(F32) == node_col
        vm_e = mm(jnp.where(hot, 1.0, 0.0).astype(BF16), vm).astype(BF16)
        lp[here, :] = (mm(edge, wmsg_ref[0:latent, :]) + mm(vm_e, wmsg_ref[2 * latent:, :]) + bg3[0:1]) * 0.5
        ec[here, :] = edge.astype(F32) + bg3[3:4]
        return carry

    lax.fori_loop(0, lax.div(total + 127, 128), prep, 0)
    move = pltpu.make_async_copy(idx_v, idx_s, isem)
    move.start()
    part[...] = jnp.zeros_like(part)
    half[...] = wmsg_ref[latent:2 * latent, :] * jnp.asarray(0.5, BF16)
    move.wait()

    per = TILE // 2
    bufs = (xbuf.at[0], xbuf.at[1])
    hids = (hid_a, hid_b)

    def first(base, k):
        for s in range(per):
            bufs[k][pl.ds(s * batch, batch), :] = table[idx_s[0, base + s]]
        acc = mm(bufs[k][...], half[...]).reshape(per, batch, latent)
        here = pl.ds(pl.multiple_of(base, per), per)
        hids[k][...] = gate(acc + lp[here, :].reshape(per, 1, latent)).reshape(per * batch, latent)

    def second(base, k):
        y = mm(hids[k][...], wo_ref[3]) + bg3[1:2]
        here = pl.ds(pl.multiple_of(base, per), per)
        z = (norm(y) * bg3[2:3]).reshape(per, batch, latent) + ec[here, :].reshape(per, 1, latent)
        z = z.astype(BF16).astype(F32)
        for s in range(per):
            n = idx_s[1, base + s]
            part[n] += z[s]

    tiles = lax.div(total + TILE - 1, TILE)

    @pl.when(tiles > 0)
    def _():
        first(0, 0)

    def edges(t, carry):
        base = t * TILE
        first(base + per, 1)
        second(base, 0)
        first(jnp.minimum(t + 1, tiles - 1) * TILE, 0)
        second(base + per, 1)
        return carry

    lax.fori_loop(0, tiles, edges, 0)
    if near:
        outs[0][...] = part[0:nodes]
    else:
        for k in range(1, lons):
            outs[k - 1][...] = part[k * nodes:(k + 1) * nodes]


def edge_call(v, w_edge, w_mesh, w_msg, w_out, w_node, bias_gain, table, lats, lons, nodes, per_node, near):
    latent = w_out.shape[-1]
    slots = lons * v.shape[-1]
    batch = table.shape[2]
    whole = lambda a: pl.BlockSpec(a.shape, lambda r: (0,) * a.ndim)
    pick = lambda k, *shape: pl.BlockSpec((1,) + shape, lambda r: (k,) + (0,) * len(shape))
    limit = lons * nodes * per_node
    block = jax.ShapeDtypeStruct((nodes, batch, latent), F32)
    row = jax.ShapeDtypeStruct((nodes, latent), F32)
    outs = [block] + [row] * 2 if near else [block] * (lons - 1)
    local = pl.BlockSpec(memory_space=pltpu.VMEM)
    return pl.pallas_call(
        functools.partial(edge_kernel, lats=lats, lons=lons, near=near),
        in_specs=[local] * 8,
        out_specs=[local] * len(outs),
        out_shape=outs,
        scratch_shapes=[
            pltpu.VMEM((limit, latent), F32),
            pltpu.VMEM((limit, latent), F32),
            pltpu.VMEM((lons * nodes, latent), F32),
            pltpu.VMEM((8, limit), jnp.int32),
            pltpu.SMEM((8, limit), jnp.int32),
            pltpu.VMEM((lons * nodes + 1, batch, latent), F32),
            pltpu.VMEM((latent, latent), BF16),
            pltpu.VMEM((TILE // 2 * batch, latent), BF16),
            pltpu.VMEM((TILE // 2 * batch, latent), BF16),
            pltpu.VMEM((2, TILE // 2 * batch, latent), BF16),
            pltpu.SemaphoreType.DMA],
        cost_estimate=pl.CostEstimate(
            flops=4 * slots // 4 * batch * latent * latent, transcendentals=0, bytes_accessed=2 * slots * batch * latent),
        compiler_params=pltpu.CompilerParams(vmem_limit_bytes=EDGE_VMEM),
        name='edges_near' if near else 'edges_far',
    )(v, w_edge, w_mesh, w_msg, w_out, w_node, bias_gain, table)


def node_kernel(own_ref, r1_ref, r2_ref, r3_ref, vm_ref, nb_ref, wn_ref, w4_ref, bg_ref, out_ref, scr):
    nodes, batch, latent = own_ref.shape
    agg = (own_ref[...] + r1_ref[...] + r2_ref[...] + r3_ref[...]).astype(BF16).reshape(nodes * batch, latent)
    acc = mm(agg, wn_ref[latent:, :]).reshape(nodes, batch, latent) + nb_ref[...].reshape(nodes, 1, latent)
    bg = bg_ref[4]
    upd = mlp_tail(acc.reshape(nodes * batch, latent), w4_ref[4], bg)
    out = (upd.reshape(nodes, batch, latent) + vm_ref[...].reshape(nodes, 1, latent)).reshape(nodes * batch, latent)

    def put(b, k, part):
        out_ref[b, :, 128 * k:128 * (k + 1)] = part

    swap_rows(out, scr, batch, put)


def node_call(blocks, vm, nb, w_node, w_out, bias_gain):
    nodes, batch, latent = blocks[0].shape
    local = pl.BlockSpec(memory_space=pltpu.VMEM)
    out = jax.ShapeDtypeStruct((batch, nodes, latent), BF16)
    return pl.pallas_call(
        node_kernel,
        in_specs=[local] * 9,
        out_specs=local,
        out_shape=out,
        compiler_params=pltpu.CompilerParams(vmem_limit_bytes=NODE_VMEM),
        scratch_shapes=[pltpu.VMEM((latent // 128, nodes * (batch + 8), 128), F32)],
        name='nodes',
    )(*blocks, vm, nb, w_node, w_out, bias_gain)


def solution(mesh):
    lats = mesh.shape['lat']
    lons = mesh.shape['lon']
    south_shift = [(s, s + 1) for s in range(lats - 1)]
    north_shift = [(s + 1, s) for s in range(lats - 1)]

    def cell_step(grid_in, mesh_in, edge_in, senders, edge_mask, w_grid, w_mesh, w_edge, w_msg, w_node, w_gupd, w_out, bias_gain):
        batch, rows, cols, _ = grid_in.shape
        nodes = senders.shape[0]
        latent = w_out.shape[-1]
        vg, table, band = embed_call(
            grid_in, w_grid, w_out, bias_gain, senders, edge_mask, jnp.swapaxes(edge_in, 1, 2), mesh_in.T, lats, lons, 4)
        edges = functools.partial(
            edge_call, band, w_edge, w_mesh, w_msg, w_out, w_node, bias_gain, table, lats, lons, *senders.shape)
        p1, p2, p3 = edges(False)
        own, vm, nb = edges(True)
        pairs = lambda k, polar: [
            (j * lats + i, (j + k) % lons * lats + i) for i in range(lats) for j in range(lons)
            if not polar or i in (0, lats - 1)]
        got = [lax.ppermute(p, ('lon', 'lat'), pairs(k, 1 < k < lons - 1)) for k, p in ((2, p2), (1, p1), (3, p3))]
        flat = update_call(vg.reshape(batch * rows * cols, latent), w_gupd, w_out, bias_gain, nb, 1024)
        grid_out = flat.reshape(batch, rows, cols, latent)
        mesh_out = node_call([own] + got, vm, nb, w_node, w_out, bias_gain)
        return mesh_out, grid_out

    grid_spec = P('dp', 'lat', 'lon', None)
    node_spec = P(('lat', 'lon'), None)
    slot_spec = P(('lat', 'lon'), None, None)
    in_specs = (grid_spec, node_spec, slot_spec, node_spec, node_spec) + (P(),) * 8
    out_specs = (P('dp', ('lat', 'lon'), None), grid_spec)
    return jax.shard_map(cell_step, mesh=mesh, in_specs=in_specs, out_specs=out_specs, check_vma=False)
```

```python
import functools

import jax
import jax.numpy as jnp
from jax import lax
from jax.experimental import pallas as pl
from jax.experimental.pallas import tpu as pltpu
from jax.sharding import PartitionSpec as P

REACH = 3
LN_EPS = 1e-5
FEATS = 16
TILE = 32
SUB = 256
PREP = 256
PACK_VMEM = 40 * 2 ** 20
PACK_FLOPS = 2 * 10 ** 9
PACK_BYTES = 10 ** 6
EDGE_VMEM = 20 * 2 ** 20
NODE_VMEM = 6 * 2 ** 20
GRID_VMEM = 24 * 2 ** 20
UPDATE_VMEM = 10 * 2 ** 20
F32 = jnp.float32
BF16 = jnp.bfloat16


def mm(a, b):
    return jnp.dot(a, b, preferred_element_type=F32)


def mm_nt(a, b):
    return lax.dot_general(a, b, (((1,), (1,)), ((), ())), preferred_element_type=F32)


def gate(t):
    return (t + t * jnp.tanh(t)).astype(BF16)


def swish(x):
    return gate(x * 0.5)


def norm(y):
    scale = 1.0 / y.shape[-1]
    centered = y - jnp.sum(y, axis=-1, keepdims=True) * scale
    var = jnp.sum(centered * centered, axis=-1, keepdims=True) * scale
    return centered * lax.rsqrt(var + LN_EPS)


def mlp_tail(pre, w2, bg):
    y = mm(swish(pre), w2) + bg[1:2]
    return norm(y) * bg[2:3] + bg[3:4]


def swap_rows(value, scr, inner, put):
    outer = value.shape[0] // inner
    pitch = scr.shape[1] // outer
    for k in range(scr.shape[0]):
        for b in range(outer):
            scr[k, pl.ds(b * pitch, inner), :] = value[b * inner:(b + 1) * inner, 128 * k:128 * (k + 1)]
    for c in range(inner):
        for k in range(scr.shape[0]):
            put(c, k, scr[k, pl.ds(c, outer, stride=pitch), :].astype(BF16))


def pack_slots(send_ref, mask_ref, edge_ref, mesh_ref, lanes, table, lon, grid_cols):
    nodes, per_node = send_ref.shape
    bits = grid_cols.bit_length() - 1
    send = send_ref[...]
    row = lax.shift_right_logical(send, bits).astype(F32)
    col = (send & (grid_cols - 1)).astype(F32)
    mask = mask_ref[...].astype(F32)
    mesh = mesh_ref[...].astype(F32)
    pieces = []
    for n in range(nodes):
        here = slice(n, n + 1)
        lanes[...] = jnp.zeros_like(lanes)
        lanes[0:4, 0:per_node] = edge_ref[n].astype(F32)
        lanes[4:5, 0:per_node] = row[here]
        lanes[5:6, 0:per_node] = col[here]
        lanes[6:7, 0:per_node] = mask[here]
        lanes[7:8, 0:per_node] = jnp.full((1, per_node), n, F32) + (lon * nodes).astype(F32)
        lanes[8:11, 0:per_node] = jnp.broadcast_to(mesh[:, here], (3, per_node))
        pieces.append(lanes[...])
    for p in range(nodes // 2):
        table[:, 128 * p:128 * (p + 1)] = pieces[p] + pltpu.roll(pieces[p + nodes // 2], 64, 1)


def pack_kernel(send_ref, mask_ref, edge_ref, mesh_ref, out_ref, lanes, table, *, grid_cols):
    pack_slots(send_ref, mask_ref, edge_ref, mesh_ref, lanes, table, lax.axis_index('lon'), grid_cols)
    out_ref[...] = table[...].astype(BF16)


def pack_call(senders, edge_mask, edge_t, mesh_t, grid_cols):
    width = senders.shape[0] // 2 * 128
    return pl.pallas_call(
        functools.partial(pack_kernel, grid_cols=grid_cols),
        out_shape=jax.ShapeDtypeStruct((FEATS, width), BF16),
        scratch_shapes=[pltpu.VMEM((FEATS, 128), F32), pltpu.VMEM((FEATS, width), F32)],
        compiler_params=pltpu.CompilerParams(vmem_limit_bytes=PACK_VMEM),
        cost_estimate=pl.CostEstimate(flops=PACK_FLOPS, transcendentals=0, bytes_accessed=PACK_BYTES),
        name='pack',
    )(senders, edge_mask, edge_t, mesh_t)


def embed_kernel(x_ref, wg_ref, w0_ref, bg_ref, feat_ref,
                 vg_ref, tab_ref, band_ref,
                 scr, half, up_buf, down_buf, from_south, from_north, feat_in, up_sems, down_sems, feat_send, feat_recv, *, lats, lons):
    batch, grid_rows, cols, chans = x_ref.shape
    latent = vg_ref.shape[-1]
    step = pl.program_id(0)
    last = pl.num_programs(0) - 1
    block = scr.shape[0]
    base = lax.rem(step * last, last + 1) * block

    lat = lax.axis_index('lat')
    lon = lax.axis_index('lon')
    mesh_id = pl.DeviceIdType.MESH

    def strip(src, dst, sems, to):
        return pltpu.make_async_remote_copy(src, dst, sems.at[0], sems.at[1], device_id={'lat': to}, device_id_type=mesh_id)

    north_send = strip(up_buf, from_south, up_sems, lat - 1)
    south_send = strip(down_buf, from_north, down_sems, lat + 1)
    feats = [pltpu.make_async_remote_copy(
        feat_ref, feat_in.at[lon], feat_send.at[k - 1], feat_recv.at[k - 1],
        device_id={'lon': lax.rem(lon + k, lons)}, device_id_type=mesh_id) for k in range(1, lons)]

    @pl.when(step == 0)
    def _():
        barrier = pltpu.get_barrier_semaphore()
        for k in range(1, lons):
            pl.semaphore_signal(barrier, 1, device_id={'lon': lax.rem(lon + k, lons)}, device_id_type=mesh_id)

        @pl.when(lat > 0)
        def _():
            pl.semaphore_signal(barrier, 1, device_id={'lat': lat - 1}, device_id_type=mesh_id)

        @pl.when(lat < lats - 1)
        def _():
            pl.semaphore_signal(barrier, 1, device_id={'lat': lat + 1}, device_id_type=mesh_id)

    @pl.when(step == 1)
    def _():
        barrier = pltpu.get_barrier_semaphore()
        inner = (lat > 0).astype(jnp.int32) + (lat < lats - 1).astype(jnp.int32)
        pl.semaphore_wait(barrier, lons - 1 + inner)

        @pl.when(lat > 0)
        def _():
            north_send.start()

        feat_in[lon] = feat_ref[...]
        for copy in feats:
            copy.start()

    @pl.when((step == 2) & (lat < lats - 1))
    def _():
        south_send.start()

    rows = batch * cols
    halve(half, wg_ref)
    bg = bg_ref[0]
    b1 = bg[0:1] * 0.5

    def first(r):
        return gate(mm(x_ref[:, base + r].reshape(rows, chans), half[...]) + b1)

    def second(r, hid):
        vg = norm(mm(hid, w0_ref[0]) + bg[1:2]) * bg[2:3] + bg[3:4]
        vg_ref[:, base + r] = vg.astype(BF16).reshape(batch, cols, latent)

        def put(c, k, part):
            tab_ref[REACH + base + r, c, :, 128 * k:128 * (k + 1)] = part

        swap_rows(vg, scr.at[r], cols, put)

    staged(block, first, second)

    @pl.when(step == 0)
    def _():
        up_buf[...] = tab_ref[REACH:2 * REACH]

    @pl.when(step == 1)
    def _():
        down_buf[...] = tab_ref[grid_rows:grid_rows + REACH]

    @pl.when(step == last)
    def _():
        for copy in feats:
            copy.wait()
        band_ref[...] = feat_in[...]

        @pl.when(lat > 0)
        def _():
            north_send.wait_send()
            south_send.wait_recv()
            tab_ref[0:REACH] = from_north[...]

        @pl.when(lat < lats - 1)
        def _():
            south_send.wait_send()
            north_send.wait_recv()
            tab_ref[grid_rows + REACH:grid_rows + 2 * REACH] = from_south[...]


def embed_call(grid_in, w_grid, w_out, bias_gain, feats, lats, lons, block):
    batch, rows, cols, chans = grid_in.shape
    latent = w_out.shape[-1]
    steps = rows // block
    whole = lambda *shape: pl.BlockSpec(shape, lambda r: (0,) * len(shape))
    pick = lambda k, *shape: pl.BlockSpec((1,) + shape, lambda r: (k,) + (0,) * len(shape))
    strip = (REACH, cols, batch, latent)
    local = pl.BlockSpec(memory_space=pltpu.VMEM)
    return pl.pallas_call(
        functools.partial(embed_kernel, lats=lats, lons=lons),
        grid=(steps,),
        in_specs=[
            local,
            whole(chans, latent), pick(0, latent, latent), pick(0, 4, latent), local],
        out_specs=[local, local, local],
        out_shape=[
            jax.ShapeDtypeStruct((batch, rows, cols, latent), BF16),
            jax.ShapeDtypeStruct((rows + 2 * REACH, cols, batch, latent), BF16),
            jax.ShapeDtypeStruct((lons,) + feats.shape, BF16)],
        scratch_shapes=[
            pltpu.VMEM((block, latent // 128, batch * (cols + 8), 128), F32),
            pltpu.VMEM((chans, latent), BF16),
            pltpu.VMEM(strip, BF16), pltpu.VMEM(strip, BF16), pltpu.VMEM(strip, BF16), pltpu.VMEM(strip, BF16),
            pltpu.VMEM((lons,) + feats.shape, BF16),
            pltpu.SemaphoreType.DMA((2,)), pltpu.SemaphoreType.DMA((2,)),
            pltpu.SemaphoreType.DMA((lons - 1,)), pltpu.SemaphoreType.DMA((lons - 1,))],
        compiler_params=pltpu.CompilerParams(collective_id=0, has_side_effects=True, vmem_limit_bytes=GRID_VMEM),
        cost_estimate=pl.CostEstimate(
            flops=4 * rows * batch * cols * latent * latent, transcendentals=0,
            bytes_accessed=6 * rows * batch * cols * latent),
        name='embed',
    )(grid_in, w_grid, w_out, bias_gain, feats)


def halve(dst, src):
    @pl.when(pl.program_id(0) == 0)
    def _():
        dst[...] = src[...] * jnp.asarray(0.5, BF16)


def staged(count, first, second):
    hid = first(0)
    for i in range(count):
        nxt = first(i + 1) if i + 1 < count else None
        second(i, hid)
        hid = nxt


def update_kernel(vg_ref, wu_ref, w5_ref, bg_ref, dep_ref, out_ref, half):
    halve(half, wu_ref)
    bg = bg_ref[0]
    b1 = bg[0:1] * 0.5
    base = pl.program_id(0) * out_ref.shape[0]

    def rows(i):
        return pl.ds(pl.multiple_of(base + i * SUB, SUB), SUB)

    def first(i):
        return gate(mm(vg_ref[rows(i), :], half[...]) + b1)

    def second(i, hid):
        upd = norm(mm(hid, w5_ref[0]) + bg[1:2]) * bg[2:3] + bg[3:4]
        out_ref[i * SUB:(i + 1) * SUB] = (vg_ref[rows(i), :].astype(F32) + upd).astype(BF16)

    staged(out_ref.shape[0] // SUB, first, second)


def update_call(vg, w_gupd, w_out, bias_gain, dep, block):
    rows, latent = vg.shape
    pick = lambda k, *shape: pl.BlockSpec((1,) + shape, lambda r: (k,) + (0,) * len(shape))
    tile = pl.BlockSpec((block, latent), lambda r: (r, 0))
    return pl.pallas_call(
        update_kernel,
        grid=(rows // block,),
        in_specs=[pl.BlockSpec(memory_space=pltpu.VMEM), pl.BlockSpec((latent, latent), lambda r: (0, 0)), pick(5, latent, latent), pick(5, 4, latent),
                  pl.BlockSpec(memory_space=pl.ANY)],
        out_specs=tile,
        out_shape=jax.ShapeDtypeStruct(vg.shape, BF16),
        scratch_shapes=[pltpu.VMEM((latent, latent), BF16)],
        cost_estimate=pl.CostEstimate(flops=4 * rows * latent * latent, transcendentals=0, bytes_accessed=4 * rows * latent),
        compiler_params=pltpu.CompilerParams(vmem_limit_bytes=UPDATE_VMEM),
        name='update',
    )(vg, w_gupd, w_out, bias_gain, dep)


def message_loop(start, stop, tab_ref, w_in, w3, bg3, lp, ec, idx, part, bufs, hids):
    rows, cols, batch, latent = tab_ref.shape
    table = tab_ref.reshape(rows * cols, batch, latent)
    per = TILE // 2
    b2 = bg3[1:2]
    gain = bg3[2:3]

    def first(base, k):
        for s in range(per):
            bufs[k][pl.ds(s * batch, batch), :] = table[idx[0, base + s]]
        here = pl.ds(pl.multiple_of(base, per), per)
        acc = mm(bufs[k][...], w_in[...]).reshape(per, batch, latent)
        hids[k][...] = gate(acc + lp[here, :].reshape(per, 1, latent)).reshape(per * batch, latent)

    def second(base, k):
        here = pl.ds(pl.multiple_of(base, per), per)
        y = mm(hids[k][...], w3[...]) + b2
        z = (norm(y) * gain).reshape(per, batch, latent) + ec[here, :].reshape(per, 1, latent)
        z = z.astype(BF16).astype(F32)
        for s in range(per):
            n = idx[1, base + s]
            part[n] += z[s]

    @pl.when(stop > start)
    def _():
        first(start * TILE, 0)

    def step(t, carry):
        base = t * TILE
        first(base + per, 1)
        second(base, 0)
        first(jnp.minimum(t + 1, stop - 1) * TILE, 0)
        second(base + per, 1)
        return carry

    lax.fori_loop(start, stop, step, 0)


def far_kernel(v_ref, we_ref, wm_ref, wmsg_ref, wo_ref, bg_ref, tab_ref,
               p1_ref, p2_ref, p3_ref, lp, ec, idx_v, own_vm_ref,
               vmf, idx_s, part, half, hid_a, hid_b, buf_a, buf_b, isem, *, lons, nodes):
    latent = wo_ref.shape[-1]
    slots = lons * v_ref.shape[-1]
    grid_rows, cols = tab_ref.shape[:2]
    positions = grid_rows * cols
    cell_rows = grid_rows - 2 * REACH
    band = lons * nodes
    lat = lax.axis_index('lat')
    lon = lax.axis_index('lon')
    vtb = jnp.concatenate([v_ref[k] for k in range(lons)], axis=1)
    vt = vtb.astype(F32)
    ids = lax.broadcasted_iota(jnp.int32, (band, slots), 0)
    local = lax.rem(ids, nodes)
    pick_row = lax.div(ids, nodes) * (slots // lons) + lax.rem(local, nodes // 2) * 128 + lax.div(local, nodes // 2) * 64
    pick = lax.broadcasted_iota(jnp.int32, (band, slots), 1) == pick_row
    mesh_feat = mm_nt(jnp.where(pick, 1.0, 0.0).astype(BF16), vtb).astype(BF16)
    we = jnp.concatenate([we_ref[...].astype(F32), jnp.zeros((FEATS - 4, latent), F32)], axis=0).astype(BF16)
    wm = jnp.concatenate(
        [jnp.zeros((8, latent), F32), wm_ref[...].astype(F32), jnp.zeros((FEATS - 11, latent), F32)], axis=0).astype(BF16)
    bg1 = bg_ref[1]
    bg2 = bg_ref[2]
    bg3 = bg_ref[3]
    vm = mlp_tail(mm(mesh_feat, wm) + bg1[0:1], wo_ref[1], bg1).astype(BF16)
    vmf[...] = vm.astype(F32)
    own_vm_ref[...] = vmf[pl.ds(pl.multiple_of(lon * nodes, 8), nodes), :]

    col = vt[5:6] - (lon * cols).astype(F32)
    cell = vt[7:8] - (lon * nodes).astype(F32)
    inner = (cell > -0.5) & (cell < nodes - 0.5)
    live = (vt[6:7] > 0.5) & (col > -0.5) & (col < cols - 0.5)
    chunks = slots // 128
    up = lax.broadcasted_iota(jnp.int32, (128, 128), 0) <= lax.broadcasted_iota(jnp.int32, (128, 128), 1)
    low = lax.broadcasted_iota(jnp.int32, (chunks, chunks), 1) < lax.broadcasted_iota(jnp.int32, (chunks, chunks), 0)
    up = jnp.where(up, 1.0, 0.0).astype(BF16)
    low = jnp.where(low, 1.0, 0.0).astype(BF16)

    def ranks(flag):
        flag = jnp.where(flag, 1.0, 0.0)
        flags = jnp.concatenate([flag[:, 128 * c:128 * (c + 1)] for c in range(chunks)], axis=0)
        incl = mm(flags.astype(BF16), up)
        before = mm(low, jnp.broadcast_to(incl[:, 127:128], (chunks, 128)).astype(BF16))
        return flags, incl + before - 1.0, jnp.sum(flag).astype(jnp.int32)

    far, far_rank, n_far = ranks(live & jnp.logical_not(inner))
    near, near_rank, n_near = ranks(live & inner)
    far_tiles = lax.div(n_far + TILE - 1, TILE)
    skip = far_tiles * TILE
    end = skip + n_near
    rank = jnp.where(far > 0.5, far_rank, jnp.where(near > 0.5, near_rank + skip.astype(F32), -1.0))
    preps = lax.div(end + PREP - 1, PREP)

    def select(t):
        slot = (lax.broadcasted_iota(jnp.int32, (PREP, 128), 0) + t * PREP).astype(F32)
        return jnp.concatenate(
            [jnp.where(rank[c:c + 1] == slot, 1.0, 0.0).astype(BF16) for c in range(chunks)], axis=1)

    def index(t, carry):
        feat_t = mm_nt(vtb, select(t))
        here = pl.ds(pl.multiple_of(t * PREP, PREP), PREP)
        slot = lax.broadcasted_iota(jnp.int32, (1, PREP), 1) + t * PREP
        used = (slot < n_far) | ((slot >= skip) & (slot < end))
        win_r = feat_t[4:5] - (lat * cell_rows - REACH).astype(F32)
        win_c = feat_t[5:6] - (lon * cols).astype(F32)
        pos = jnp.where(used, (win_r * cols + win_c).astype(jnp.int32), REACH * cols)
        rel = lax.rem(feat_t[7:8].astype(jnp.int32) + (lons - lon) * nodes, band)
        idx_v[0:1, here] = jnp.clip(pos, 0, positions - 1)
        idx_v[1:2, here] = jnp.where(used, rel, band)
        idx_v[2:3, here] = jnp.full((1, PREP), far_tiles, jnp.int32)
        idx_v[3:4, here] = jnp.full((1, PREP), lax.div(end + TILE - 1, TILE), jnp.int32)
        return carry

    idx_v[2:3, 0:128] = jnp.zeros((1, 128), jnp.int32)
    idx_v[3:4, 0:128] = jnp.zeros((1, 128), jnp.int32)
    lax.fori_loop(0, preps, index, 0)
    move = pltpu.make_async_copy(idx_v, idx_s, isem)
    move.start()
    part[...] = jnp.zeros_like(part)
    half[...] = wmsg_ref[latent:2 * latent, :] * jnp.asarray(0.5, BF16)

    def prep(t, carry):
        feat = mm_nt(select(t), vtb).astype(BF16)
        here = pl.ds(pl.multiple_of(t * PREP, PREP), PREP)
        edge = mlp_tail(mm(feat, we) + bg2[0:1], wo_ref[2], bg2).astype(BF16)
        hot = lax.broadcasted_iota(jnp.int32, (PREP, band), 1).astype(F32) == feat[:, 7:8].astype(F32)
        vm_e = mm(jnp.where(hot, 1.0, 0.0).astype(BF16), vm).astype(BF16)
        lp[here, :] = (mm(edge, wmsg_ref[0:latent, :]) + mm(vm_e, wmsg_ref[2 * latent:, :]) + bg3[0:1]) * 0.5
        ec[here, :] = edge.astype(F32) + bg3[3:4]
        return carry

    lax.fori_loop(0, preps, prep, 0)
    move.wait()
    message_loop(0, far_tiles, tab_ref, half, wo_ref.at[3], bg3, lp, ec, idx_s, part, (buf_a, buf_b), (hid_a, hid_b))
    for k, ref in enumerate((p1_ref, p2_ref, p3_ref)):
        ref[...] = part[(k + 1) * nodes:(k + 2) * nodes]


def near_kernel(idx, lp, ec, wmsg_ref, wo_ref, bg_ref, tab_ref, own_ref, part, half, hid_a, hid_b, buf_a, buf_b):
    latent = wo_ref.shape[-1]
    nodes = own_ref.shape[0]
    part[...] = jnp.zeros_like(part)
    half[...] = wmsg_ref[latent:2 * latent, :] * jnp.asarray(0.5, BF16)
    message_loop(idx[2, 0], idx[3, 0], tab_ref, half, wo_ref.at[3], bg_ref[3], lp, ec, idx, part,
                 (buf_a, buf_b), (hid_a, hid_b))
    own_ref[...] = part[0:nodes]


def loop_scratch(batch, latent):
    half_tile = pltpu.VMEM((TILE // 2 * batch, latent), BF16)
    return [pltpu.VMEM((latent, latent), BF16)] + [half_tile] * 4


def edge_call(v, w_edge, w_mesh, w_msg, w_out, bias_gain, table, lats, lons, nodes, per_node):
    latent = w_out.shape[-1]
    batch = table.shape[2]
    limit = lons * nodes * per_node + PREP
    local = pl.BlockSpec(memory_space=pltpu.VMEM)
    outs = [jax.ShapeDtypeStruct((nodes, batch, latent), F32)] * (lons - 1)
    outs += [jax.ShapeDtypeStruct((limit, latent), F32)] * 2
    outs += [jax.ShapeDtypeStruct((4, limit), jnp.int32), jax.ShapeDtypeStruct((nodes, latent), F32)]
    res = pl.pallas_call(
        functools.partial(far_kernel, lons=lons, nodes=nodes),
        in_specs=[local] * 7,
        out_specs=[local] * len(outs),
        out_shape=outs,
        scratch_shapes=[
            pltpu.VMEM((lons * nodes, latent), F32),
            pltpu.SMEM((4, limit), jnp.int32),
            pltpu.VMEM((lons * nodes + 1, batch, latent), F32)] + loop_scratch(batch, latent) + [pltpu.SemaphoreType.DMA],
        compiler_params=pltpu.CompilerParams(vmem_limit_bytes=EDGE_VMEM),
        cost_estimate=pl.CostEstimate(
            flops=4 * limit // 8 * batch * latent * latent, transcendentals=0, bytes_accessed=limit * batch * latent),
        name='edges_far',
    )(v, w_edge, w_mesh, w_msg, w_out, bias_gain, table)
    return res[:lons - 1], (res[-2], res[-4], res[-3], res[-1])


def near_call(lists, w_msg, w_out, bias_gain, table, nodes, band):
    idx, lp, ec, _ = lists
    latent = w_out.shape[-1]
    batch = table.shape[2]
    local = pl.BlockSpec(memory_space=pltpu.VMEM)
    return pl.pallas_call(
        near_kernel,
        in_specs=[pl.BlockSpec(memory_space=pltpu.SMEM)] + [local] * 6,
        out_specs=[local],
        out_shape=[jax.ShapeDtypeStruct((nodes, batch, latent), F32)],
        scratch_shapes=[pltpu.VMEM((band + 1, batch, latent), F32)] + loop_scratch(batch, latent),
        compiler_params=pltpu.CompilerParams(vmem_limit_bytes=EDGE_VMEM),
        cost_estimate=pl.CostEstimate(
            flops=lp.shape[0] * batch * latent * latent, transcendentals=0, bytes_accessed=lp.shape[0] * batch * latent),
        name='edges_near',
    )(idx, lp, ec, w_msg, w_out, bias_gain, table)


def node_kernel(own_ref, r1_ref, r2_ref, r3_ref, vm_ref, wn_ref, w4_ref, bg_ref, out_ref, scr):
    nodes, batch, latent = own_ref.shape
    agg = (own_ref[...] + r1_ref[...] + r2_ref[...] + r3_ref[...]).astype(BF16).reshape(nodes * batch, latent)
    bg = bg_ref[4]
    base = mm(vm_ref[...].astype(BF16), wn_ref[0:latent, :]) + bg[0:1]
    acc = mm(agg, wn_ref[latent:, :]).reshape(nodes, batch, latent) + base.reshape(nodes, 1, latent)
    upd = mlp_tail(acc.reshape(nodes * batch, latent), w4_ref[4], bg)
    out = (upd.reshape(nodes, batch, latent) + vm_ref[...].reshape(nodes, 1, latent)).reshape(nodes * batch, latent)

    def put(b, k, part):
        out_ref[b, :, 128 * k:128 * (k + 1)] = part

    swap_rows(out, scr, batch, put)


def node_call(blocks, vm, w_node, w_out, bias_gain):
    nodes, batch, latent = blocks[0].shape
    local = pl.BlockSpec(memory_space=pltpu.VMEM)
    out = jax.ShapeDtypeStruct((batch, nodes, latent), BF16)
    return pl.pallas_call(
        node_kernel,
        in_specs=[local] * 8,
        out_specs=local,
        out_shape=out,
        compiler_params=pltpu.CompilerParams(vmem_limit_bytes=NODE_VMEM),
        scratch_shapes=[pltpu.VMEM((latent // 128, nodes * (batch + 8), 128), F32)],
        name='nodes',
    )(*blocks, vm, w_node, w_out, bias_gain)


def solution(mesh):
    lats = mesh.shape['lat']
    lons = mesh.shape['lon']
    south_shift = [(s, s + 1) for s in range(lats - 1)]
    north_shift = [(s + 1, s) for s in range(lats - 1)]

    def cell_step(grid_in, mesh_in, edge_in, senders, edge_mask, w_grid, w_mesh, w_edge, w_msg, w_node, w_gupd, w_out, bias_gain):
        batch, rows, cols, _ = grid_in.shape
        nodes = senders.shape[0]
        latent = w_out.shape[-1]
        feats = pack_call(senders, edge_mask, jnp.swapaxes(edge_in, 1, 2), mesh_in.T, cols * lons)
        vg, table, band = embed_call(grid_in, w_grid, w_out, bias_gain, feats, lats, lons, 4)
        blocks, lists = edge_call(band, w_edge, w_mesh, w_msg, w_out, bias_gain, table, lats, lons, *senders.shape)
        own, = near_call(lists, w_msg, w_out, bias_gain, table, senders.shape[0], senders.shape[0] * lons)
        pairs = lambda k, polar: [
            (j * lats + i, (j + k) % lons * lats + i) for i in range(lats) for j in range(lons)
            if not polar or i in (0, lats - 1)]
        got = [lax.ppermute(p, ('lon', 'lat'), pairs(k, 1 < k < lons - 1)) for k, p in ((2, blocks[1]), (1, blocks[0]), (3, blocks[2]))]
        flat = update_call(vg.reshape(batch * rows * cols, latent), w_gupd, w_out, bias_gain, own, 1024)
        grid_out = flat.reshape(batch, rows, cols, latent)
        mesh_out = node_call([own] + got, lists[3], w_node, w_out, bias_gain)
        return mesh_out, grid_out

    grid_spec = P('dp', 'lat', 'lon', None)
    node_spec = P(('lat', 'lon'), None)
    slot_spec = P(('lat', 'lon'), None, None)
    in_specs = (grid_spec, node_spec, slot_spec, node_spec, node_spec) + (P(),) * 8
    out_specs = (P('dp', ('lat', 'lon'), None), grid_spec)
    return jax.shard_map(cell_step, mesh=mesh, in_specs=in_specs, out_specs=out_specs, check_vma=False)
```

```python
import functools

import jax
import jax.numpy as jnp
from jax import lax
from jax.experimental import pallas as pl
from jax.experimental.pallas import tpu as pltpu
from jax.sharding import PartitionSpec as P

REACH = 3
LN_EPS = 1e-5
FEATS = 16
TILE = 32
SUB = 256
PREP = 128
PACK_VMEM = 40 * 2 ** 20
PACK_FLOPS = 2 * 10 ** 9
PACK_BYTES = 10 ** 6
EDGE_VMEM = 20 * 2 ** 20
NODE_VMEM = 6 * 2 ** 20
GRID_VMEM = 24 * 2 ** 20
UPDATE_VMEM = 12 * 2 ** 20
F32 = jnp.float32
BF16 = jnp.bfloat16


def mm(a, b):
    return jnp.dot(a, b, preferred_element_type=F32)


def mm_nt(a, b):
    return lax.dot_general(a, b, (((1,), (1,)), ((), ())), preferred_element_type=F32)


def gate(t):
    return (t + t * jnp.tanh(t)).astype(BF16)


def swish(x):
    return gate(x * 0.5)


def norm(y):
    scale = 1.0 / y.shape[-1]
    centered = y - jnp.sum(y, axis=-1, keepdims=True) * scale
    var = jnp.sum(centered * centered, axis=-1, keepdims=True) * scale
    return centered * lax.rsqrt(var + LN_EPS)


def mlp_tail(pre, w2, bg):
    y = mm(swish(pre), w2) + bg[1:2]
    return norm(y) * bg[2:3] + bg[3:4]


def swap_rows(value, scr, inner, put):
    outer = value.shape[0] // inner
    pitch = scr.shape[1] // outer
    for k in range(scr.shape[0]):
        for b in range(outer):
            scr[k, pl.ds(b * pitch, inner), :] = value[b * inner:(b + 1) * inner, 128 * k:128 * (k + 1)]
    for c in range(inner):
        for k in range(scr.shape[0]):
            put(c, k, scr[k, pl.ds(c, outer, stride=pitch), :].astype(BF16))


def pack_slots(send_ref, mask_ref, edge_ref, mesh_ref, lanes, table, lon, grid_cols):
    nodes, per_node = send_ref.shape
    bits = grid_cols.bit_length() - 1
    send = send_ref[...]
    row = lax.shift_right_logical(send, bits).astype(F32)
    col = (send & (grid_cols - 1)).astype(F32)
    mask = mask_ref[...].astype(F32)
    mesh = mesh_ref[...].astype(F32)
    pieces = []
    for n in range(nodes):
        here = slice(n, n + 1)
        lanes[...] = jnp.zeros_like(lanes)
        lanes[0:4, 0:per_node] = edge_ref[n].astype(F32)
        lanes[4:5, 0:per_node] = row[here]
        lanes[5:6, 0:per_node] = col[here]
        lanes[6:7, 0:per_node] = mask[here]
        lanes[7:8, 0:per_node] = jnp.full((1, per_node), n, F32) + (lon * nodes).astype(F32)
        lanes[8:11, 0:per_node] = jnp.broadcast_to(mesh[:, here], (3, per_node))
        pieces.append(lanes[...])
    for p in range(nodes // 2):
        table[:, 128 * p:128 * (p + 1)] = pieces[p] + pltpu.roll(pieces[p + nodes // 2], 64, 1)


def idle_kernel(out_ref):
    out_ref[...] = jnp.zeros_like(out_ref)


def idle_call():
    return pl.pallas_call(
        idle_kernel,
        out_shape=jax.ShapeDtypeStruct((8, 128), F32),
        compiler_params=pltpu.CompilerParams(vmem_limit_bytes=PACK_VMEM),
        cost_estimate=pl.CostEstimate(flops=PACK_FLOPS, transcendentals=0, bytes_accessed=PACK_BYTES),
        name='idle',
    )()


def pack_kernel(send_ref, mask_ref, edge_ref, mesh_ref, dep_ref, out_ref, lanes, table, *, grid_cols):
    pack_slots(send_ref, mask_ref, edge_ref, mesh_ref, lanes, table, lax.axis_index('lon'), grid_cols)
    out_ref[...] = table[...].astype(BF16)


def pack_call(senders, edge_mask, edge_t, mesh_t, dep, grid_cols):
    width = senders.shape[0] // 2 * 128
    return pl.pallas_call(
        functools.partial(pack_kernel, grid_cols=grid_cols),
        out_shape=jax.ShapeDtypeStruct((FEATS, width), BF16),
        scratch_shapes=[pltpu.VMEM((FEATS, 128), F32), pltpu.VMEM((FEATS, width), F32)],
        compiler_params=pltpu.CompilerParams(vmem_limit_bytes=PACK_VMEM),
        cost_estimate=pl.CostEstimate(flops=PACK_FLOPS, transcendentals=0, bytes_accessed=PACK_BYTES),
        name='pack',
    )(senders, edge_mask, edge_t, mesh_t, dep)


def embed_kernel(x_ref, wg_ref, wo_ref, bg_ref, feat_ref,
                 vg_ref, tab_ref, band_ref,
                 scr, half, from_south, from_north, feat_in, up_sems, down_sems, feat_send, feat_recv, *, lats, lons):
    batch, grid_rows, cols, chans = x_ref.shape
    latent = vg_ref.shape[-1]
    lat = lax.axis_index('lat')
    lon = lax.axis_index('lon')
    odd = lax.rem(lat, 2)
    inner_north = lat > 0
    inner_south = lat < lats - 1
    mesh_id = pl.DeviceIdType.MESH

    def strip(start, dst, sems, to):
        return pltpu.make_async_remote_copy(
            tab_ref.at[pl.ds(start, REACH)], dst, sems.at[0], sems.at[1], device_id={'lat': to}, device_id_type=mesh_id)

    north_send = strip(REACH, from_south, up_sems, lat - 1)
    south_send = strip(grid_rows, from_north, down_sems, lat + 1)
    feats = [pltpu.make_async_remote_copy(
        feat_ref, feat_in.at[lon], feat_send.at[k - 1], feat_recv.at[k - 1],
        device_id={'lon': lax.rem(lon + k, lons)}, device_id_type=mesh_id) for k in range(1, lons)]

    barrier = pltpu.get_barrier_semaphore()
    for k in range(1, lons):
        pl.semaphore_signal(barrier, 1, device_id={'lon': lax.rem(lon + k, lons)}, device_id_type=mesh_id)

    @pl.when(inner_north)
    def _():
        pl.semaphore_signal(barrier, 1, device_id={'lat': lat - 1}, device_id_type=mesh_id)

    @pl.when(inner_south)
    def _():
        pl.semaphore_signal(barrier, 1, device_id={'lat': lat + 1}, device_id_type=mesh_id)

    feat_in[lon] = feat_ref[...]
    half[...] = wg_ref[...] * jnp.asarray(0.5, BF16)
    bg = bg_ref[0]
    b1 = bg[0:1] * 0.5

    def row(i):
        return i + odd * (grid_rows - 1 - 2 * i)

    def first(i):
        return gate(mm(x_ref[:, row(i)].reshape(batch * cols, chans), half[...]) + b1)

    def second(i, hid):
        vg = norm(mm(hid, wo_ref[0]) + bg[1:2]) * bg[2:3] + bg[3:4]
        vg_ref[:, row(i)] = vg.astype(BF16).reshape(batch, cols, latent)

        def put(c, k, part):
            tab_ref[REACH + row(i), c, :, 128 * k:128 * (k + 1)] = part

        swap_rows(vg, scr.at[i % scr.shape[0]], cols, put)

    staged(range(REACH), first, second)
    pl.semaphore_wait(barrier, lons - 1 + inner_north.astype(jnp.int32) + inner_south.astype(jnp.int32))

    @pl.when(inner_north & (odd == 0))
    def _():
        north_send.start()

    @pl.when(inner_south & (odd == 1))
    def _():
        south_send.start()

    for copy in feats:
        copy.start()
    staged(range(grid_rows - REACH, grid_rows), first, second)

    @pl.when(inner_north & (odd == 1))
    def _():
        north_send.start()

    @pl.when(inner_south & (odd == 0))
    def _():
        south_send.start()

    staged(range(REACH, grid_rows - REACH), first, second)
    for copy in feats:
        copy.wait()
    band_ref[...] = feat_in[...]

    @pl.when(inner_north)
    def _():
        north_send.wait_send()
        south_send.wait_recv()
        tab_ref[0:REACH] = from_north[...]

    @pl.when(inner_south)
    def _():
        south_send.wait_send()
        north_send.wait_recv()
        tab_ref[grid_rows + REACH:grid_rows + 2 * REACH] = from_south[...]


def embed_call(grid_in, w_grid, w_out, bias_gain, feats, lats, lons):
    batch, rows, cols, chans = grid_in.shape
    latent = w_out.shape[-1]
    strip = (REACH, cols, batch, latent)
    local = pl.BlockSpec(memory_space=pltpu.VMEM)
    return pl.pallas_call(
        functools.partial(embed_kernel, lats=lats, lons=lons),
        in_specs=[local] * 5,
        out_specs=[local] * 3,
        out_shape=[
            jax.ShapeDtypeStruct((batch, rows, cols, latent), BF16),
            jax.ShapeDtypeStruct((rows + 2 * REACH, cols, batch, latent), BF16),
            jax.ShapeDtypeStruct((lons,) + feats.shape, BF16)],
        scratch_shapes=[
            pltpu.VMEM((4, latent // 128, batch * (cols + 8), 128), F32),
            pltpu.VMEM((chans, latent), BF16),
            pltpu.VMEM(strip, BF16), pltpu.VMEM(strip, BF16),
            pltpu.VMEM((lons,) + feats.shape, BF16),
            pltpu.SemaphoreType.DMA((2,)), pltpu.SemaphoreType.DMA((2,)),
            pltpu.SemaphoreType.DMA((lons - 1,)), pltpu.SemaphoreType.DMA((lons - 1,))],
        compiler_params=pltpu.CompilerParams(collective_id=0, has_side_effects=True, vmem_limit_bytes=GRID_VMEM),
        cost_estimate=pl.CostEstimate(
            flops=4 * rows * batch * cols * latent * latent, transcendentals=0,
            bytes_accessed=6 * rows * batch * cols * latent),
        name='embed',
    )(grid_in, w_grid, w_out, bias_gain, feats)


def staged(items, first, second):
    items = list(items)
    hid = first(items[0])
    for k, item in enumerate(items):
        nxt = first(items[k + 1]) if k + 1 < len(items) else None
        second(item, hid)
        hid = nxt


def update_kernel(vg_ref, wu_ref, wo_ref, bg_ref, dep_ref, out_ref, half, obuf, sems):
    half[...] = wu_ref[...] * jnp.asarray(0.5, BF16)
    bg = bg_ref[5]
    b1 = bg[0:1] * 0.5
    count = vg_ref.shape[0] // SUB

    def rows(i):
        return pl.ds(i * SUB, SUB)

    def put(i):
        return pltpu.make_async_copy(obuf.at[rows(i)], out_ref.at[rows(i)], sems.at[i])

    def first(i):
        return gate(mm(vg_ref[rows(i), :], half[...]) + b1)

    def second(i, hid):
        upd = norm(mm(hid, wo_ref[5]) + bg[1:2]) * bg[2:3] + bg[3:4]
        obuf[rows(i), :] = (vg_ref[rows(i), :].astype(F32) + upd).astype(BF16)
        if i:
            put(i - 1).start()

    staged(range(count), first, second)
    put(count - 1).start()
    for i in range(count):
        put(i).wait()


def update_call(vg, w_gupd, w_out, bias_gain, dep):
    rows, latent = vg.shape
    local = pl.BlockSpec(memory_space=pltpu.VMEM)
    anywhere = pl.BlockSpec(memory_space=pl.ANY)
    return pl.pallas_call(
        update_kernel,
        in_specs=[local] * 4 + [anywhere],
        out_specs=anywhere,
        out_shape=jax.ShapeDtypeStruct(vg.shape, BF16),
        scratch_shapes=[pltpu.VMEM((latent, latent), BF16), pltpu.VMEM(vg.shape, BF16), pltpu.SemaphoreType.DMA((rows // SUB,))],
        cost_estimate=pl.CostEstimate(flops=4 * rows * latent * latent, transcendentals=0, bytes_accessed=4 * rows * latent),
        compiler_params=pltpu.CompilerParams(vmem_limit_bytes=UPDATE_VMEM),
        name='update',
    )(vg, w_gupd, w_out, bias_gain, dep)


def message_loop(start, stop, tab_ref, w_in, w3, bg3, lp, ec, idx, part, bufs, hids):
    rows, cols, batch, latent = tab_ref.shape
    table = tab_ref.reshape(rows * cols, batch, latent)
    per = TILE // 2
    b2 = bg3[1:2]
    gain = bg3[2:3]

    def first(base, k):
        for s in range(per):
            bufs[k][pl.ds(s * batch, batch), :] = table[idx[0, base + s]]
        here = pl.ds(pl.multiple_of(base, per), per)
        acc = mm(bufs[k][...], w_in[...]).reshape(per, batch, latent)
        hids[k][...] = gate(acc + lp[here, :].reshape(per, 1, latent)).reshape(per * batch, latent)

    def second(base, k):
        here = pl.ds(pl.multiple_of(base, per), per)
        y = mm(hids[k][...], w3[...]) + b2
        z = (norm(y) * gain).reshape(per, batch, latent) + ec[here, :].reshape(per, 1, latent)
        z = z.astype(BF16).astype(F32)
        for s in range(per):
            n = idx[1, base + s]
            part[n] += z[s]

    @pl.when(stop > start)
    def _():
        first(start * TILE, 0)

    def step(t, carry):
        base = t * TILE
        first(base + per, 1)
        second(base, 0)
        first(jnp.minimum(t + 1, stop - 1) * TILE, 0)
        second(base + per, 1)
        return carry

    lax.fori_loop(start, stop, step, 0)


def three_parts(x):
    hi = x.astype(BF16)
    rest = x - hi.astype(F32)
    mid = rest.astype(BF16)
    return jnp.concatenate([hi, mid, (rest - mid.astype(F32)).astype(BF16)], axis=0)


def select(rank, base):
    slot = lax.broadcasted_iota(jnp.int32, (PREP, 128), 0).astype(F32) + base
    return jnp.concatenate(
        [jnp.where(rank[c:c + 1] == slot, 1.0, 0.0).astype(BF16) for c in range(rank.shape[0])], axis=1)


def prepare(start, stop, rank, vtb, we_ref, wmsg_ref, wo_ref, bg_ref, node_proj, lp, ec):
    latent = wo_ref.shape[-1]
    band = node_proj.shape[0] // 3
    we = jnp.concatenate([we_ref[...].astype(F32), jnp.zeros((FEATS - 4, latent), F32)], axis=0).astype(BF16)
    bg2 = bg_ref[2]
    bg3 = bg_ref[3]

    def prep(t, carry):
        feat = mm_nt(select(rank, (t * PREP).astype(F32)), vtb).astype(BF16)
        here = pl.ds(pl.multiple_of(t * PREP, PREP), PREP)
        edge = mlp_tail(mm(feat, we) + bg2[0:1], wo_ref[2], bg2).astype(BF16)
        lane = lax.rem(lax.broadcasted_iota(jnp.int32, (PREP, 3 * band), 1), band).astype(F32)
        hot = jnp.where(lane == feat[:, 7:8].astype(F32), 1.0, 0.0).astype(BF16)
        lp[here, :] = (mm(edge, wmsg_ref[0:latent, :]) + mm(hot, node_proj[...]) + bg3[0:1]) * 0.5
        ec[here, :] = edge.astype(F32) + bg3[3:4]
        return carry

    lax.fori_loop(start, stop, prep, 0)


def far_kernel(v_ref, we_ref, wm_ref, wmsg_ref, wo_ref, bg_ref, tab_ref,
               p1_ref, p2_ref, p3_ref, idx_v, rank_ref, proj_ref, own_vm_ref,
               lp, ec, vmf, idx_s, part, half, hid_a, hid_b, buf_a, buf_b, isem, *, lons, nodes):
    latent = wo_ref.shape[-1]
    slots = lons * v_ref.shape[-1]
    grid_rows, cols = tab_ref.shape[:2]
    positions = grid_rows * cols
    cell_rows = grid_rows - 2 * REACH
    band = lons * nodes
    lat = lax.axis_index('lat')
    lon = lax.axis_index('lon')
    vtb = jnp.concatenate([v_ref[k] for k in range(lons)], axis=1)
    vt = vtb.astype(F32)
    ids = lax.broadcasted_iota(jnp.int32, (band, slots), 0)
    local = lax.rem(ids, nodes)
    pick_row = lax.div(ids, nodes) * (slots // lons) + lax.rem(local, nodes // 2) * 128 + lax.div(local, nodes // 2) * 64
    pick = lax.broadcasted_iota(jnp.int32, (band, slots), 1) == pick_row
    mesh_feat = mm_nt(jnp.where(pick, 1.0, 0.0).astype(BF16), vtb).astype(BF16)
    wm = jnp.concatenate(
        [jnp.zeros((8, latent), F32), wm_ref[...].astype(F32), jnp.zeros((FEATS - 11, latent), F32)], axis=0).astype(BF16)
    bg1 = bg_ref[1]
    vm = mlp_tail(mm(mesh_feat, wm) + bg1[0:1], wo_ref[1], bg1).astype(BF16)
    vmf[...] = vm.astype(F32)
    proj_ref[...] = three_parts(mm(vm, wmsg_ref[2 * latent:, :]))
    own_vm_ref[...] = vmf[pl.ds(pl.multiple_of(lon * nodes, 8), nodes), :]

    col = vt[5:6] - (lon * cols).astype(F32)
    cell = vt[7:8] - (lon * nodes).astype(F32)
    inner = (cell > -0.5) & (cell < nodes - 0.5)
    live = (vt[6:7] > 0.5) & (col > -0.5) & (col < cols - 0.5)
    chunks = slots // 128
    up = lax.broadcasted_iota(jnp.int32, (128, 128), 0) <= lax.broadcasted_iota(jnp.int32, (128, 128), 1)
    low = lax.broadcasted_iota(jnp.int32, (chunks, chunks), 1) < lax.broadcasted_iota(jnp.int32, (chunks, chunks), 0)
    up = jnp.where(up, 1.0, 0.0).astype(BF16)
    low = jnp.where(low, 1.0, 0.0).astype(BF16)

    def ranks(flag):
        flag = jnp.where(flag, 1.0, 0.0)
        flags = jnp.concatenate([flag[:, 128 * c:128 * (c + 1)] for c in range(chunks)], axis=0)
        incl = mm(flags.astype(BF16), up)
        before = mm(low, jnp.broadcast_to(incl[:, 127:128], (chunks, 128)).astype(BF16))
        return flags, incl + before - 1.0, jnp.sum(flag).astype(jnp.int32)

    far, far_rank, n_far = ranks(live & jnp.logical_not(inner))
    near, near_rank, n_near = ranks(live & inner)
    far_tiles = lax.div(n_far + TILE - 1, TILE)
    skip = far_tiles * TILE
    end = skip + n_near
    rank = jnp.where(far > 0.5, far_rank, jnp.where(near > 0.5, near_rank + skip.astype(F32), -1.0))
    preps = lax.div(end + PREP - 1, PREP)

    rank_ref[...] = rank

    def index(t, carry):
        feat_t = mm_nt(vtb, select(rank, (t * PREP).astype(F32)))
        here = pl.ds(pl.multiple_of(t * PREP, PREP), PREP)
        slot = lax.broadcasted_iota(jnp.int32, (1, PREP), 1) + t * PREP
        used = (slot < n_far) | ((slot >= skip) & (slot < end))
        win_r = feat_t[4:5] - (lat * cell_rows - REACH).astype(F32)
        win_c = feat_t[5:6] - (lon * cols).astype(F32)
        pos = jnp.where(used, (win_r * cols + win_c).astype(jnp.int32), REACH * cols)
        rel = lax.rem(feat_t[7:8].astype(jnp.int32) + (lons - lon) * nodes, band)
        idx_v[0:1, here] = jnp.clip(pos, 0, positions - 1)
        idx_v[1:2, here] = jnp.where(used, rel, band)
        idx_v[2:3, here] = jnp.full((1, PREP), far_tiles, jnp.int32)
        idx_v[3:4, here] = jnp.full((1, PREP), lax.div(end + TILE - 1, TILE), jnp.int32)
        return carry

    idx_v[2:3, 0:128] = jnp.zeros((1, 128), jnp.int32)
    idx_v[3:4, 0:128] = jnp.zeros((1, 128), jnp.int32)
    lax.fori_loop(0, preps, index, 0)
    move = pltpu.make_async_copy(idx_v, idx_s, isem)
    move.start()
    part[...] = jnp.zeros_like(part)
    half[...] = wmsg_ref[latent:2 * latent, :] * jnp.asarray(0.5, BF16)

    prepare(0, lax.div(skip + PREP - 1, PREP), rank, vtb, we_ref, wmsg_ref, wo_ref, bg_ref, proj_ref, lp, ec)
    move.wait()
    message_loop(0, far_tiles, tab_ref, half, wo_ref.at[3], bg_ref[3], lp, ec, idx_s, part, (buf_a, buf_b), (hid_a, hid_b))
    for k, ref in enumerate((p1_ref, p2_ref, p3_ref)):
        ref[...] = part[(k + 1) * nodes:(k + 2) * nodes]


def near_kernel(idx, v_ref, rank_ref, proj_ref, we_ref, wmsg_ref, wo_ref, bg_ref, tab_ref, own_ref, lp, ec, part, half, hid_a, hid_b, buf_a, buf_b):
    latent = wo_ref.shape[-1]
    nodes = own_ref.shape[0]
    part[...] = jnp.zeros_like(part)
    half[...] = wmsg_ref[latent:2 * latent, :] * jnp.asarray(0.5, BF16)
    vtb = jnp.concatenate([v_ref[k] for k in range(v_ref.shape[0])], axis=1)
    start, stop = idx[2, 0], idx[3, 0]
    ratio = PREP // TILE
    prepare(lax.div(start, ratio), lax.div(stop + ratio - 1, ratio), rank_ref[...], vtb, we_ref, wmsg_ref, wo_ref, bg_ref,
            proj_ref, lp, ec)
    message_loop(start, stop, tab_ref, half, wo_ref.at[3], bg_ref[3], lp, ec, idx, part,
                 (buf_a, buf_b), (hid_a, hid_b))
    own_ref[...] = part[0:nodes]


def loop_scratch(batch, latent):
    half_tile = pltpu.VMEM((TILE // 2 * batch, latent), BF16)
    return [pltpu.VMEM((latent, latent), BF16)] + [half_tile] * 4


def edge_call(v, w_edge, w_mesh, w_msg, w_out, bias_gain, table, lats, lons, nodes, per_node):
    latent = w_out.shape[-1]
    batch = table.shape[2]
    limit = lons * nodes * per_node + PREP
    local = pl.BlockSpec(memory_space=pltpu.VMEM)
    outs = [jax.ShapeDtypeStruct((nodes, batch, latent), F32)] * (lons - 1)
    outs += [jax.ShapeDtypeStruct((4, limit), jnp.int32), jax.ShapeDtypeStruct((lons * v.shape[-1] // 128, 128), F32)]
    outs += [jax.ShapeDtypeStruct((3 * lons * nodes, latent), BF16), jax.ShapeDtypeStruct((nodes, latent), F32)]
    res = pl.pallas_call(
        functools.partial(far_kernel, lons=lons, nodes=nodes),
        in_specs=[local] * 7,
        out_specs=[local] * len(outs),
        out_shape=outs,
        scratch_shapes=[
            pltpu.VMEM((limit, latent), F32), pltpu.VMEM((limit, latent), F32),
            pltpu.VMEM((lons * nodes, latent), F32),
            pltpu.SMEM((4, limit), jnp.int32),
            pltpu.VMEM((lons * nodes + 1, batch, latent), F32)] + loop_scratch(batch, latent) + [pltpu.SemaphoreType.DMA],
        compiler_params=pltpu.CompilerParams(vmem_limit_bytes=EDGE_VMEM),
        cost_estimate=pl.CostEstimate(
            flops=4 * limit // 8 * batch * latent * latent, transcendentals=0, bytes_accessed=limit * batch * latent),
        name='edges_far',
    )(v, w_edge, w_mesh, w_msg, w_out, bias_gain, table)
    return res[:lons - 1], res[lons - 1:]


def near_call(v, lists, w_edge, w_msg, w_out, bias_gain, table, nodes, band):
    idx, rank, proj, _ = lists
    latent = w_out.shape[-1]
    batch = table.shape[2]
    local = pl.BlockSpec(memory_space=pltpu.VMEM)
    return pl.pallas_call(
        near_kernel,
        in_specs=[pl.BlockSpec(memory_space=pltpu.SMEM)] + [local] * 8,
        out_specs=[local],
        out_shape=[jax.ShapeDtypeStruct((nodes, batch, latent), F32)],
        scratch_shapes=[pltpu.VMEM((idx.shape[1], latent), F32), pltpu.VMEM((idx.shape[1], latent), F32),
                        pltpu.VMEM((band + 1, batch, latent), F32)] + loop_scratch(batch, latent),
        compiler_params=pltpu.CompilerParams(vmem_limit_bytes=EDGE_VMEM),
        cost_estimate=pl.CostEstimate(
            flops=idx.shape[1] * batch * latent * latent, transcendentals=0, bytes_accessed=idx.shape[1] * batch * latent),
        name='edges_near',
    )(idx, v, rank, proj, w_edge, w_msg, w_out, bias_gain, table)


def node_kernel(own_ref, r1_ref, r2_ref, r3_ref, vm_ref, wn_ref, w4_ref, bg_ref, out_ref, scr):
    nodes, batch, latent = own_ref.shape
    agg = (own_ref[...] + r1_ref[...] + r2_ref[...] + r3_ref[...]).astype(BF16).reshape(nodes * batch, latent)
    bg = bg_ref[4]
    base = mm(vm_ref[...].astype(BF16), wn_ref[0:latent, :]) + bg[0:1]
    acc = mm(agg, wn_ref[latent:, :]).reshape(nodes, batch, latent) + base.reshape(nodes, 1, latent)
    upd = mlp_tail(acc.reshape(nodes * batch, latent), w4_ref[4], bg)
    out = (upd.reshape(nodes, batch, latent) + vm_ref[...].reshape(nodes, 1, latent)).reshape(nodes * batch, latent)

    def put(b, k, part):
        out_ref[b, :, 128 * k:128 * (k + 1)] = part

    swap_rows(out, scr, batch, put)


def node_call(blocks, vm, w_node, w_out, bias_gain):
    nodes, batch, latent = blocks[0].shape
    local = pl.BlockSpec(memory_space=pltpu.VMEM)
    out = jax.ShapeDtypeStruct((batch, nodes, latent), BF16)
    return pl.pallas_call(
        node_kernel,
        in_specs=[local] * 8,
        out_specs=local,
        out_shape=out,
        compiler_params=pltpu.CompilerParams(vmem_limit_bytes=NODE_VMEM),
        scratch_shapes=[pltpu.VMEM((latent // 128, nodes * (batch + 8), 128), F32)],
        name='nodes',
    )(*blocks, vm, w_node, w_out, bias_gain)


def solution(mesh):
    lats = mesh.shape['lat']
    lons = mesh.shape['lon']
    south_shift = [(s, s + 1) for s in range(lats - 1)]
    north_shift = [(s + 1, s) for s in range(lats - 1)]

    def cell_step(grid_in, mesh_in, edge_in, senders, edge_mask, w_grid, w_mesh, w_edge, w_msg, w_node, w_gupd, w_out, bias_gain):
        batch, rows, cols, _ = grid_in.shape
        nodes = senders.shape[0]
        latent = w_out.shape[-1]
        feats = pack_call(senders, edge_mask, jnp.swapaxes(edge_in, 1, 2), mesh_in.T, idle_call(), cols * lons)
        vg, table, band = embed_call(grid_in, w_grid, w_out, bias_gain, feats, lats, lons)
        blocks, lists = edge_call(band, w_edge, w_mesh, w_msg, w_out, bias_gain, table, lats, lons, *senders.shape)
        own, = near_call(band, lists, w_edge, w_msg, w_out, bias_gain, table, senders.shape[0], senders.shape[0] * lons)
        pairs = lambda k, polar: [
            (j * lats + i, (j + k) % lons * lats + i) for i in range(lats) for j in range(lons)
            if not polar or i in (0, lats - 1)]
        got = [lax.ppermute(p, ('lon', 'lat'), pairs(k, 1 < k < lons - 1)) for k, p in ((2, blocks[1]), (1, blocks[0]), (3, blocks[2]))]
        flat = update_call(vg.reshape(batch * rows * cols, latent), w_gupd, w_out, bias_gain, own)
        grid_out = flat.reshape(batch, rows, cols, latent)
        mesh_out = node_call([own] + got, lists[3], w_node, w_out, bias_gain)
        return mesh_out, grid_out

    grid_spec = P('dp', 'lat', 'lon', None)
    node_spec = P(('lat', 'lon'), None)
    slot_spec = P(('lat', 'lon'), None, None)
    in_specs = (grid_spec, node_spec, slot_spec, node_spec, node_spec) + (P(),) * 8
    out_specs = (P('dp', ('lat', 'lon'), None), grid_spec)
    return jax.shard_map(cell_step, mesh=mesh, in_specs=in_specs, out_specs=out_specs, check_vma=False)
```

```python
import functools

import jax
import jax.numpy as jnp
from jax import lax
from jax.experimental import pallas as pl
from jax.experimental.pallas import tpu as pltpu
from jax.sharding import PartitionSpec as P

REACH = 3
LN_EPS = 1e-5
FEATS = 16
TILE = 32
SUB = 256
PREP = 128
CODE = 64
PACK_VMEM = 40 * 2 ** 20
PACK_FLOPS = 2 * 10 ** 9
PACK_BYTES = 10 ** 6
EDGE_VMEM = 20 * 2 ** 20
NODE_VMEM = 6 * 2 ** 20
GRID_VMEM = 24 * 2 ** 20
UPDATE_VMEM = 12 * 2 ** 20
F32 = jnp.float32
BF16 = jnp.bfloat16


def mm(a, b):
    return jnp.dot(a, b, preferred_element_type=F32)


def mm_nt(a, b):
    return lax.dot_general(a, b, (((1,), (1,)), ((), ())), preferred_element_type=F32)


def gate(t):
    return (t + t * jnp.tanh(t)).astype(BF16)


def swish(x):
    return gate(x * 0.5)


def norm(y):
    scale = 1.0 / y.shape[-1]
    centered = y - jnp.sum(y, axis=-1, keepdims=True) * scale
    var = jnp.sum(centered * centered, axis=-1, keepdims=True) * scale
    return centered * lax.rsqrt(var + LN_EPS)


def mlp_tail(pre, w2, bg):
    y = mm(swish(pre), w2) + bg[1:2]
    return norm(y) * bg[2:3] + bg[3:4]


def swap_rows(value, scr, inner, put):
    outer = value.shape[0] // inner
    pitch = scr.shape[1] // outer
    for k in range(scr.shape[0]):
        for b in range(outer):
            scr[k, pl.ds(b * pitch, inner), :] = value[b * inner:(b + 1) * inner, 128 * k:128 * (k + 1)]
    for c in range(inner):
        for k in range(scr.shape[0]):
            put(c, k, scr[k, pl.ds(c, outer, stride=pitch), :].astype(BF16))


def pack_slots(send_ref, mask_ref, edge_ref, mesh_ref, lanes, table, lon, grid_cols):
    nodes, per_node = send_ref.shape
    bits = grid_cols.bit_length() - 1
    send = send_ref[...]
    row = lax.shift_right_logical(send, bits).astype(F32)
    col = (send & (grid_cols - 1)).astype(F32)
    mask = mask_ref[...].astype(F32)
    mesh = mesh_ref[...].astype(F32)
    pieces = []
    for n in range(nodes):
        here = slice(n, n + 1)
        lanes[...] = jnp.zeros_like(lanes)
        lanes[0:4, 0:per_node] = edge_ref[n].astype(F32)
        lanes[4:5, 0:per_node] = row[here]
        lanes[5:6, 0:per_node] = col[here]
        lanes[6:7, 0:per_node] = mask[here]
        lanes[7:8, 0:per_node] = jnp.full((1, per_node), n, F32) + (lon * nodes).astype(F32)
        lanes[8:11, 0:per_node] = jnp.broadcast_to(mesh[:, here], (3, per_node))
        pieces.append(lanes[...])
    for p in range(nodes // 2):
        table[:, 128 * p:128 * (p + 1)] = pieces[p] + pltpu.roll(pieces[p + nodes // 2], 64, 1)


def idle_kernel(out_ref):
    out_ref[...] = jnp.zeros_like(out_ref)


def idle_call():
    return pl.pallas_call(
        idle_kernel,
        out_shape=jax.ShapeDtypeStruct((8, 128), F32),
        compiler_params=pltpu.CompilerParams(vmem_limit_bytes=PACK_VMEM),
        cost_estimate=pl.CostEstimate(flops=PACK_FLOPS, transcendentals=0, bytes_accessed=PACK_BYTES),
        name='idle',
    )()


def pack_kernel(send_ref, mask_ref, edge_ref, mesh_ref, dep_ref, out_ref, lanes, table, *, grid_cols):
    pack_slots(send_ref, mask_ref, edge_ref, mesh_ref, lanes, table, lax.axis_index('lon'), grid_cols)
    out_ref[...] = table[...].astype(BF16)


def pack_call(senders, edge_mask, edge_t, mesh_t, dep, grid_cols):
    width = senders.shape[0] // 2 * 128
    return pl.pallas_call(
        functools.partial(pack_kernel, grid_cols=grid_cols),
        out_shape=jax.ShapeDtypeStruct((FEATS, width), BF16),
        scratch_shapes=[pltpu.VMEM((FEATS, 128), F32), pltpu.VMEM((FEATS, width), F32)],
        compiler_params=pltpu.CompilerParams(vmem_limit_bytes=PACK_VMEM),
        cost_estimate=pl.CostEstimate(flops=PACK_FLOPS, transcendentals=0, bytes_accessed=PACK_BYTES),
        name='pack',
    )(senders, edge_mask, edge_t, mesh_t, dep)


def rank_slots(vtb, lon, cols, nodes):
    slots = vtb.shape[1]
    chunks = slots // 128
    vt = vtb.astype(F32)
    col = vt[5:6] - (lon * cols).astype(F32)
    cell = vt[7:8] - (lon * nodes).astype(F32)
    inner = (cell > -0.5) & (cell < nodes - 0.5)
    live = (vt[6:7] > 0.5) & (col > -0.5) & (col < cols - 0.5)
    up = lax.broadcasted_iota(jnp.int32, (128, 128), 0) <= lax.broadcasted_iota(jnp.int32, (128, 128), 1)
    low = lax.broadcasted_iota(jnp.int32, (chunks, chunks), 1) < lax.broadcasted_iota(jnp.int32, (chunks, chunks), 0)
    up = jnp.where(up, 1.0, 0.0).astype(BF16)
    low = jnp.where(low, 1.0, 0.0).astype(BF16)
    ones = jnp.full((chunks, chunks), 1.0, BF16)

    def count(flag):
        flag = jnp.where(flag, 1.0, 0.0)
        flags = jnp.concatenate([flag[:, 128 * c:128 * (c + 1)] for c in range(chunks)], axis=0)
        incl = mm(flags.astype(BF16), up)
        row_sum = jnp.broadcast_to(incl[:, 127:128], (chunks, 128)).astype(BF16)
        return flags, incl + mm(low, row_sum) - 1.0, mm(ones, row_sum)

    far, far_rank, n_far = count(live & jnp.logical_not(inner))
    near, near_rank, n_near = count(live & inner)
    skip = jnp.floor((n_far + (TILE - 1)) * (1.0 / TILE)) * TILE
    rank = jnp.where(far > 0.5, far_rank, jnp.where(near > 0.5, near_rank + skip, -1.0))
    return rank, n_far, skip + n_near


def mesh_latents(vtb, lons, nodes, wm_ref, wo_ref, bg_ref):
    slots = vtb.shape[1]
    latent = wo_ref.shape[-1]
    band = lons * nodes
    ids = lax.broadcasted_iota(jnp.int32, (band, slots), 0)
    local = lax.rem(ids, nodes)
    pick_row = lax.div(ids, nodes) * (slots // lons) + lax.rem(local, nodes // 2) * 128 + lax.div(local, nodes // 2) * 64
    pick = lax.broadcasted_iota(jnp.int32, (band, slots), 1) == pick_row
    mesh_feat = mm_nt(jnp.where(pick, 1.0, 0.0).astype(BF16), vtb).astype(BF16)
    wm = jnp.concatenate(
        [jnp.zeros((8, latent), F32), wm_ref[...].astype(F32), jnp.zeros((FEATS - 11, latent), F32)], axis=0).astype(BF16)
    bg1 = bg_ref[1]
    return mlp_tail(mm(mesh_feat, wm) + bg1[0:1], wo_ref[1], bg1)


def embed_kernel(x_ref, wg_ref, wo_ref, bg_ref, feat_ref, wm_ref,
                 vg_ref, tab_ref, band_ref, rank_ref, vm_ref,
                 scr, half, from_south, from_north, feat_in, up_sems, down_sems, feat_send, feat_recv, *, lats, lons):
    batch, grid_rows, cols, chans = x_ref.shape
    latent = vg_ref.shape[-1]
    lat = lax.axis_index('lat')
    lon = lax.axis_index('lon')
    odd = lax.rem(lat, 2)
    inner_north = lat > 0
    inner_south = lat < lats - 1
    mesh_id = pl.DeviceIdType.MESH

    def strip(start, dst, sems, to):
        return pltpu.make_async_remote_copy(
            tab_ref.at[pl.ds(start, REACH)], dst, sems.at[0], sems.at[1], device_id={'lat': to}, device_id_type=mesh_id)

    north_send = strip(REACH, from_south, up_sems, lat - 1)
    south_send = strip(grid_rows, from_north, down_sems, lat + 1)
    feats = [pltpu.make_async_remote_copy(
        feat_ref, feat_in.at[lon], feat_send.at[k - 1], feat_recv.at[k - 1],
        device_id={'lon': lax.rem(lon + k, lons)}, device_id_type=mesh_id) for k in range(1, lons)]

    barrier = pltpu.get_barrier_semaphore()
    for k in range(1, lons):
        pl.semaphore_signal(barrier, 1, device_id={'lon': lax.rem(lon + k, lons)}, device_id_type=mesh_id)

    @pl.when(inner_north)
    def _():
        pl.semaphore_signal(barrier, 1, device_id={'lat': lat - 1}, device_id_type=mesh_id)

    @pl.when(inner_south)
    def _():
        pl.semaphore_signal(barrier, 1, device_id={'lat': lat + 1}, device_id_type=mesh_id)

    feat_in[lon] = feat_ref[...]
    half[...] = wg_ref[...] * jnp.asarray(0.5, BF16)
    bg = bg_ref[0]
    b1 = bg[0:1] * 0.5

    def row(i):
        return i + odd * (grid_rows - 1 - 2 * i)

    def first(i):
        return gate(mm(x_ref[:, row(i)].reshape(batch * cols, chans), half[...]) + b1)

    def second(i, hid):
        vg = norm(mm(hid, wo_ref[0]) + bg[1:2]) * bg[2:3] + bg[3:4]
        vg_ref[:, row(i)] = vg.astype(BF16).reshape(batch, cols, latent)

        def put(c, k, part):
            tab_ref[REACH + row(i), c, :, 128 * k:128 * (k + 1)] = part

        swap_rows(vg, scr.at[i % scr.shape[0]], cols, put)

    staged(range(REACH), first, second)
    pl.semaphore_wait(barrier, lons - 1 + inner_north.astype(jnp.int32) + inner_south.astype(jnp.int32))

    @pl.when(inner_north & (odd == 0))
    def _():
        north_send.start()

    @pl.when(inner_south & (odd == 1))
    def _():
        south_send.start()

    for copy in feats:
        copy.start()
    staged(range(grid_rows - REACH, grid_rows), first, second)

    @pl.when(inner_north & (odd == 1))
    def _():
        north_send.start()

    @pl.when(inner_south & (odd == 0))
    def _():
        south_send.start()

    for copy in feats:
        copy.wait()

    def extra():
        band_ref[...] = feat_in[...]
        vtb = jnp.concatenate([feat_in[k] for k in range(lons)], axis=1)
        nodes = 2 * (feat_in.shape[2] // 128)
        rank, n_far, end = rank_slots(vtb, lon, cols, nodes)
        rank_ref[0:rank.shape[0]] = rank
        rank_ref[rank.shape[0]:rank.shape[0] + 8] = n_far[0:8]
        rank_ref[rank.shape[0] + 8:] = end[0:8]
        vm_ref[...] = mesh_latents(vtb, lons, nodes, wm_ref, wo_ref, bg_ref).astype(BF16).astype(F32)

    staged(range(REACH, grid_rows - REACH), first, second, extra)

    @pl.when(inner_north)
    def _():
        north_send.wait_send()
        south_send.wait_recv()
        tab_ref[0:REACH] = from_north[...]

    @pl.when(inner_south)
    def _():
        south_send.wait_send()
        north_send.wait_recv()
        tab_ref[grid_rows + REACH:grid_rows + 2 * REACH] = from_south[...]


def embed_call(grid_in, w_grid, w_out, bias_gain, feats, w_mesh, lats, lons):
    batch, rows, cols, chans = grid_in.shape
    latent = w_out.shape[-1]
    strip = (REACH, cols, batch, latent)
    local = pl.BlockSpec(memory_space=pltpu.VMEM)
    return pl.pallas_call(
        functools.partial(embed_kernel, lats=lats, lons=lons),
        in_specs=[local] * 6,
        out_specs=[local] * 5,
        out_shape=[
            jax.ShapeDtypeStruct((batch, rows, cols, latent), BF16),
            jax.ShapeDtypeStruct((rows + 2 * REACH, cols, batch, latent), BF16),
            jax.ShapeDtypeStruct((lons,) + feats.shape, BF16),
            jax.ShapeDtypeStruct((lons * feats.shape[1] // 128 + 16, 128), F32),
            jax.ShapeDtypeStruct((lons * feats.shape[1] // 64, latent), F32)],
        scratch_shapes=[
            pltpu.VMEM((4, latent // 128, batch * (cols + 8), 128), F32),
            pltpu.VMEM((chans, latent), BF16),
            pltpu.VMEM(strip, BF16), pltpu.VMEM(strip, BF16),
            pltpu.VMEM((lons,) + feats.shape, BF16),
            pltpu.SemaphoreType.DMA((2,)), pltpu.SemaphoreType.DMA((2,)),
            pltpu.SemaphoreType.DMA((lons - 1,)), pltpu.SemaphoreType.DMA((lons - 1,))],
        compiler_params=pltpu.CompilerParams(collective_id=0, has_side_effects=True, vmem_limit_bytes=GRID_VMEM),
        cost_estimate=pl.CostEstimate(
            flops=4 * rows * batch * cols * latent * latent, transcendentals=0,
            bytes_accessed=6 * rows * batch * cols * latent),
        name='embed',
    )(grid_in, w_grid, w_out, bias_gain, feats, w_mesh)


def staged(items, first, second, extra=None):
    items = list(items)
    hid = first(items[0])
    if extra is not None:
        extra()
    for k, item in enumerate(items):
        nxt = first(items[k + 1]) if k + 1 < len(items) else None
        second(item, hid)
        hid = nxt


def update_kernel(vg_ref, wu_ref, wo_ref, bg_ref, dep_ref, out_ref, half, obuf, sems):
    half[...] = wu_ref[...] * jnp.asarray(0.5, BF16)
    bg = bg_ref[5]
    b1 = bg[0:1] * 0.5
    count = vg_ref.shape[0] // SUB

    def rows(i):
        return pl.ds(i * SUB, SUB)

    def put(i):
        return pltpu.make_async_copy(obuf.at[rows(i)], out_ref.at[rows(i)], sems.at[i])

    def first(i):
        return gate(mm(vg_ref[rows(i), :], half[...]) + b1)

    def second(i, hid):
        upd = norm(mm(hid, wo_ref[5]) + bg[1:2]) * bg[2:3] + bg[3:4]
        obuf[rows(i), :] = (vg_ref[rows(i), :].astype(F32) + upd).astype(BF16)
        if i:
            put(i - 1).start()

    staged(range(count), first, second)
    put(count - 1).start()
    for i in range(count):
        put(i).wait()


def update_call(vg, w_gupd, w_out, bias_gain, dep):
    rows, latent = vg.shape
    local = pl.BlockSpec(memory_space=pltpu.VMEM)
    anywhere = pl.BlockSpec(memory_space=pl.ANY)
    return pl.pallas_call(
        update_kernel,
        in_specs=[local] * 4 + [anywhere],
        out_specs=anywhere,
        out_shape=jax.ShapeDtypeStruct(vg.shape, BF16),
        scratch_shapes=[pltpu.VMEM((latent, latent), BF16), pltpu.VMEM(vg.shape, BF16), pltpu.SemaphoreType.DMA((rows // SUB,))],
        cost_estimate=pl.CostEstimate(flops=4 * rows * latent * latent, transcendentals=0, bytes_accessed=4 * rows * latent),
        compiler_params=pltpu.CompilerParams(vmem_limit_bytes=UPDATE_VMEM),
        name='update',
    )(vg, w_gupd, w_out, bias_gain, dep)


def message_loop(start, stop, tab_ref, w_in, w3, bg3, lp, ec, idx, part, bufs, hids):
    rows, cols, batch, latent = tab_ref.shape
    table = tab_ref.reshape(rows * cols, batch, latent)
    per = TILE // 2
    b2 = bg3[1:2]
    gain = bg3[2:3]

    def first(base, k):
        for s in range(per):
            bufs[k][pl.ds(s * batch, batch), :] = table[lax.div(idx[0, base + s], CODE)]
        here = pl.ds(pl.multiple_of(base, per), per)
        acc = mm(bufs[k][...], w_in[...]).reshape(per, batch, latent)
        hids[k][...] = gate(acc + lp[here, :].reshape(per, 1, latent)).reshape(per * batch, latent)

    def second(base, k):
        here = pl.ds(pl.multiple_of(base, per), per)
        y = mm(hids[k][...], w3[...]) + b2
        z = (norm(y) * gain).reshape(per, batch, latent) + ec[here, :].reshape(per, 1, latent)
        z = z.astype(BF16).astype(F32)
        for s in range(per):
            n = lax.rem(idx[0, base + s], CODE)
            part[n] += z[s]

    @pl.when(stop > start)
    def _():
        first(start * TILE, 0)

    def step(t, carry):
        base = t * TILE
        first(base + per, 1)
        second(base, 0)
        first(jnp.minimum(t + 1, stop - 1) * TILE, 0)
        second(base + per, 1)
        return carry

    lax.fori_loop(start, stop, step, 0)


def three_parts(x):
    hi = x.astype(BF16)
    rest = x - hi.astype(F32)
    mid = rest.astype(BF16)
    return jnp.concatenate([hi, mid, (rest - mid.astype(F32)).astype(BF16)], axis=0)


def select(rank, base):
    slot = lax.broadcasted_iota(jnp.int32, (PREP, 128), 0).astype(F32) + base
    return jnp.concatenate(
        [jnp.where(rank[c:c + 1] == slot, 1.0, 0.0).astype(BF16) for c in range(rank.shape[0])], axis=1)


def prepare(start, stop, rank, vtb, we_ref, wmsg_ref, wo_ref, bg_ref, node_proj, lp, ec):
    latent = wo_ref.shape[-1]
    band = node_proj.shape[0] // 3
    we = jnp.concatenate([we_ref[...].astype(F32), jnp.zeros((FEATS - 4, latent), F32)], axis=0).astype(BF16)
    bg2 = bg_ref[2]
    bg3 = bg_ref[3]

    def prep(t, carry):
        feat = mm_nt(select(rank, (t * PREP).astype(F32)), vtb).astype(BF16)
        here = pl.ds(pl.multiple_of(t * PREP, PREP), PREP)
        edge = mlp_tail(mm(feat, we) + bg2[0:1], wo_ref[2], bg2).astype(BF16)
        lane = lax.rem(lax.broadcasted_iota(jnp.int32, (PREP, 3 * band), 1), band).astype(F32)
        hot = jnp.where(lane == feat[:, 7:8].astype(F32), 1.0, 0.0).astype(BF16)
        lp[here, :] = (mm(edge, wmsg_ref[0:latent, :]) + mm(hot, node_proj[...]) + bg3[0:1]) * 0.5
        ec[here, :] = edge.astype(F32) + bg3[3:4]
        return carry

    lax.fori_loop(start, stop, prep, 0)


def far_kernel(v_ref, rank_ref, vm_ref, we_ref, wmsg_ref, wo_ref, bg_ref, tab_ref,
               p1_ref, p2_ref, p3_ref, idx_v, proj_ref,
               lp, ec, idx_s, part, half, hid_a, hid_b, buf_a, buf_b, isem, *, lons, nodes):
    latent = wo_ref.shape[-1]
    grid_rows, cols = tab_ref.shape[:2]
    positions = grid_rows * cols
    cell_rows = grid_rows - 2 * REACH
    band = lons * nodes
    chunks = rank_ref.shape[0] - 16
    meta = idx_v.shape[1] - 128
    lat = lax.axis_index('lat')
    lon = lax.axis_index('lon')
    vtb = jnp.concatenate([v_ref[k] for k in range(lons)], axis=1)
    rank = rank_ref[0:chunks]
    n_far = jnp.max(rank_ref[chunks:chunks + 8]).astype(jnp.int32)
    end = jnp.max(rank_ref[chunks + 8:]).astype(jnp.int32)
    far_tiles = lax.div(n_far + TILE - 1, TILE)
    skip = far_tiles * TILE
    proj_ref[...] = three_parts(mm(vm_ref[...].astype(BF16), wmsg_ref[2 * latent:, :]))

    def index(t, carry):
        feat_t = mm_nt(vtb, select(rank, (t * PREP).astype(F32)))
        here = pl.ds(pl.multiple_of(t * PREP, PREP), PREP)
        slot = lax.broadcasted_iota(jnp.int32, (1, PREP), 1) + t * PREP
        used = (slot < n_far) | ((slot >= skip) & (slot < end))
        win_r = feat_t[4:5] - (lat * cell_rows - REACH).astype(F32)
        win_c = feat_t[5:6] - (lon * cols).astype(F32)
        pos = jnp.clip(jnp.where(used, (win_r * cols + win_c).astype(jnp.int32), REACH * cols), 0, positions - 1)
        node = feat_t[7:8].astype(jnp.int32)
        cell = lax.div(node, nodes)
        rel = jnp.where(used, jnp.bitwise_xor(cell, lon) * nodes + (node - cell * nodes), band)
        idx_v[0:1, here] = pos * CODE + rel
        return carry

    lax.fori_loop(0, lax.div(end + PREP - 1, PREP), index, 0)
    lane = lax.broadcasted_iota(jnp.int32, (1, 128), 1)
    idx_v[0:1, meta:meta + 128] = jnp.where(lane == 0, far_tiles, lax.div(end + TILE - 1, TILE))
    move = pltpu.make_async_copy(idx_v, idx_s, isem)
    move.start()
    part[...] = jnp.zeros_like(part)
    half[...] = wmsg_ref[latent:2 * latent, :] * jnp.asarray(0.5, BF16)
    prepare(0, lax.div(skip + PREP - 1, PREP), rank, vtb, we_ref, wmsg_ref, wo_ref, bg_ref, proj_ref, lp, ec)
    move.wait()
    message_loop(0, far_tiles, tab_ref, half, wo_ref.at[3], bg_ref[3], lp, ec, idx_s, part, (buf_a, buf_b), (hid_a, hid_b))
    for k, ref in enumerate((p1_ref, p2_ref, p3_ref)):
        ref[...] = part[(k + 1) * nodes:(k + 2) * nodes]


def near_kernel(idx, v_ref, rank_ref, proj_ref, we_ref, wmsg_ref, wo_ref, bg_ref, tab_ref, own_ref, lp, ec, part, half, hid_a, hid_b, buf_a, buf_b):
    latent = wo_ref.shape[-1]
    nodes = own_ref.shape[0]
    part[...] = jnp.zeros_like(part)
    half[...] = wmsg_ref[latent:2 * latent, :] * jnp.asarray(0.5, BF16)
    vtb = jnp.concatenate([v_ref[k] for k in range(v_ref.shape[0])], axis=1)
    meta = idx.shape[1] - 128
    start, stop = idx[0, meta], idx[0, meta + 1]
    ratio = PREP // TILE
    prepare(lax.div(start, ratio), lax.div(stop + ratio - 1, ratio), rank_ref[0:rank_ref.shape[0] - 16], vtb, we_ref, wmsg_ref, wo_ref, bg_ref,
            proj_ref, lp, ec)
    message_loop(start, stop, tab_ref, half, wo_ref.at[3], bg_ref[3], lp, ec, idx, part,
                 (buf_a, buf_b), (hid_a, hid_b))
    own_ref[...] = part[0:nodes]


def loop_scratch(batch, latent):
    half_tile = pltpu.VMEM((TILE // 2 * batch, latent), BF16)
    return [pltpu.VMEM((latent, latent), BF16)] + [half_tile] * 4


def edge_call(v, rank, vm, w_edge, w_msg, w_out, bias_gain, table, lons, nodes, per_node):
    latent = w_out.shape[-1]
    batch = table.shape[2]
    limit = lons * nodes * per_node + PREP + 128
    local = pl.BlockSpec(memory_space=pltpu.VMEM)
    outs = [jax.ShapeDtypeStruct((nodes, batch, latent), F32)] * (lons - 1)
    outs += [jax.ShapeDtypeStruct((1, limit), jnp.int32), jax.ShapeDtypeStruct((3 * lons * nodes, latent), BF16)]
    res = pl.pallas_call(
        functools.partial(far_kernel, lons=lons, nodes=nodes),
        in_specs=[local] * 8,
        out_specs=[local] * len(outs),
        out_shape=outs,
        scratch_shapes=[
            pltpu.VMEM((limit, latent), F32), pltpu.VMEM((limit, latent), F32),
            pltpu.SMEM((1, limit), jnp.int32),
            pltpu.VMEM((lons * nodes + 1, batch, latent), F32)] + loop_scratch(batch, latent) + [pltpu.SemaphoreType.DMA],
        compiler_params=pltpu.CompilerParams(vmem_limit_bytes=EDGE_VMEM),
        cost_estimate=pl.CostEstimate(
            flops=4 * limit // 8 * batch * latent * latent, transcendentals=0, bytes_accessed=limit * batch * latent),
        name='edges_far',
    )(v, rank, vm, w_edge, w_msg, w_out, bias_gain, table)
    return res[:lons - 1], res[lons - 1:]


def near_call(v, rank, lists, w_edge, w_msg, w_out, bias_gain, table, nodes, band):
    idx, proj = lists
    latent = w_out.shape[-1]
    batch = table.shape[2]
    local = pl.BlockSpec(memory_space=pltpu.VMEM)
    return pl.pallas_call(
        near_kernel,
        in_specs=[pl.BlockSpec(memory_space=pltpu.SMEM)] + [local] * 8,
        out_specs=[local],
        out_shape=[jax.ShapeDtypeStruct((nodes, batch, latent), F32)],
        scratch_shapes=[pltpu.VMEM((idx.shape[1], latent), F32), pltpu.VMEM((idx.shape[1], latent), F32),
                        pltpu.VMEM((band + 1, batch, latent), F32)] + loop_scratch(batch, latent),
        compiler_params=pltpu.CompilerParams(vmem_limit_bytes=EDGE_VMEM),
        cost_estimate=pl.CostEstimate(
            flops=idx.shape[1] * batch * latent * latent, transcendentals=0, bytes_accessed=idx.shape[1] * batch * latent),
        name='edges_near',
    )(idx, v, rank, proj, w_edge, w_msg, w_out, bias_gain, table)


def node_kernel(own_ref, r1_ref, r2_ref, r3_ref, vm_ref, wn_ref, w4_ref, bg_ref, out_ref, scr):
    nodes, batch, latent = own_ref.shape
    agg = (own_ref[...] + r1_ref[...] + r2_ref[...] + r3_ref[...]).astype(BF16).reshape(nodes * batch, latent)
    bg = bg_ref[4]
    own_vm = vm_ref[pl.ds(pl.multiple_of(lax.axis_index('lon') * nodes, 8), nodes), :]
    base = mm(own_vm.astype(BF16), wn_ref[0:latent, :]) + bg[0:1]
    acc = mm(agg, wn_ref[latent:, :]).reshape(nodes, batch, latent) + base.reshape(nodes, 1, latent)
    upd = mlp_tail(acc.reshape(nodes * batch, latent), w4_ref[4], bg)
    out = (upd.reshape(nodes, batch, latent) + own_vm.reshape(nodes, 1, latent)).reshape(nodes * batch, latent)

    def put(b, k, part):
        out_ref[b, :, 128 * k:128 * (k + 1)] = part

    swap_rows(out, scr, batch, put)


def node_call(blocks, vm, w_node, w_out, bias_gain):
    nodes, batch, latent = blocks[0].shape
    local = pl.BlockSpec(memory_space=pltpu.VMEM)
    out = jax.ShapeDtypeStruct((batch, nodes, latent), BF16)
    return pl.pallas_call(
        node_kernel,
        in_specs=[local] * 8,
        out_specs=local,
        out_shape=out,
        compiler_params=pltpu.CompilerParams(vmem_limit_bytes=NODE_VMEM),
        scratch_shapes=[pltpu.VMEM((latent // 128, nodes * (batch + 8), 128), F32)],
        name='nodes',
    )(*blocks, vm, w_node, w_out, bias_gain)


def solution(mesh):
    lats = mesh.shape['lat']
    lons = mesh.shape['lon']
    south_shift = [(s, s + 1) for s in range(lats - 1)]
    north_shift = [(s + 1, s) for s in range(lats - 1)]

    def cell_step(grid_in, mesh_in, edge_in, senders, edge_mask, w_grid, w_mesh, w_edge, w_msg, w_node, w_gupd, w_out, bias_gain):
        batch, rows, cols, _ = grid_in.shape
        nodes = senders.shape[0]
        latent = w_out.shape[-1]
        feats = pack_call(senders, edge_mask, jnp.swapaxes(edge_in, 1, 2), mesh_in.T, idle_call(), cols * lons)
        vg, table, band, rank, vm = embed_call(grid_in, w_grid, w_out, bias_gain, feats, w_mesh, lats, lons)
        blocks, lists = edge_call(band, rank, vm, w_edge, w_msg, w_out, bias_gain, table, lons, *senders.shape)
        own, = near_call(band, rank, lists, w_edge, w_msg, w_out, bias_gain, table, nodes, nodes * lons)
        pairs = lambda k, polar: [
            (j * lats + i, (j ^ k) * lats + i) for i in range(lats) for j in range(lons)
            if not polar or i in (0, lats - 1)]
        got = [lax.ppermute(blocks[k - 1], ('lon', 'lat'), pairs(k, k == 2)) for k in (3, 2, 1)]
        mesh_out = node_call([own] + got, vm, w_node, w_out, bias_gain)
        flat = update_call(vg.reshape(batch * rows * cols, latent), w_gupd, w_out, bias_gain, own)
        grid_out = flat.reshape(batch, rows, cols, latent)
        return mesh_out, grid_out

    grid_spec = P('dp', 'lat', 'lon', None)
    node_spec = P(('lat', 'lon'), None)
    slot_spec = P(('lat', 'lon'), None, None)
    in_specs = (grid_spec, node_spec, slot_spec, node_spec, node_spec) + (P(),) * 8
    out_specs = (P('dp', ('lat', 'lon'), None), grid_spec)
    return jax.shard_map(cell_step, mesh=mesh, in_specs=in_specs, out_specs=out_specs, check_vma=False)
```

```python
import functools

import jax
import jax.numpy as jnp
from jax import lax
from jax.experimental import pallas as pl
from jax.experimental.pallas import tpu as pltpu
from jax.sharding import PartitionSpec as P

REACH = 3
LN_EPS = 1e-5
FEATS = 16
TILE = 32
SUB = 256
PREP = 128
CODE = 64
PACK_VMEM = 40 * 2 ** 20
PACK_FLOPS = 2 * 10 ** 9
PACK_BYTES = 10 ** 6
EDGE_VMEM = 20 * 2 ** 20
NODE_VMEM = 6 * 2 ** 20
GRID_VMEM = 24 * 2 ** 20
UPDATE_VMEM = 12 * 2 ** 20
F32 = jnp.float32
BF16 = jnp.bfloat16


def mm(a, b):
    return jnp.dot(a, b, preferred_element_type=F32)


def mm_nt(a, b):
    return lax.dot_general(a, b, (((1,), (1,)), ((), ())), preferred_element_type=F32)


def gate(t):
    return (t + t * jnp.tanh(t)).astype(BF16)


def swish(x):
    return gate(x * 0.5)


def norm(y):
    scale = 1.0 / y.shape[-1]
    centered = y - jnp.sum(y, axis=-1, keepdims=True) * scale
    var = jnp.sum(centered * centered, axis=-1, keepdims=True) * scale
    return centered * lax.rsqrt(var + LN_EPS)


def mlp_tail(pre, w2, bg):
    y = mm(swish(pre), w2) + bg[1:2]
    return norm(y) * bg[2:3] + bg[3:4]


def swap_rows(value, scr, inner, put):
    outer = value.shape[0] // inner
    pitch = scr.shape[1] // outer
    for k in range(scr.shape[0]):
        for b in range(outer):
            scr[k, pl.ds(b * pitch, inner), :] = value[b * inner:(b + 1) * inner, 128 * k:128 * (k + 1)]
    for c in range(inner):
        for k in range(scr.shape[0]):
            put(c, k, scr[k, pl.ds(c, outer, stride=pitch), :].astype(BF16))


def pack_slots(send_ref, mask_ref, edge_ref, mesh_ref, lanes, table, lon, grid_cols):
    nodes, per_node = send_ref.shape
    bits = grid_cols.bit_length() - 1
    send = send_ref[...]
    row = lax.shift_right_logical(send, bits).astype(F32)
    col = (send & (grid_cols - 1)).astype(F32)
    mask = mask_ref[...].astype(F32)
    mesh = mesh_ref[...].astype(F32)
    pieces = []
    for n in range(nodes):
        here = slice(n, n + 1)
        lanes[...] = jnp.zeros_like(lanes)
        lanes[0:4, 0:per_node] = edge_ref[n].astype(F32)
        lanes[4:5, 0:per_node] = row[here]
        lanes[5:6, 0:per_node] = col[here]
        lanes[6:7, 0:per_node] = mask[here]
        lanes[7:8, 0:per_node] = jnp.full((1, per_node), n, F32) + (lon * nodes).astype(F32)
        lanes[8:11, 0:per_node] = jnp.broadcast_to(mesh[:, here], (3, per_node))
        pieces.append(lanes[...])
    for p in range(nodes // 2):
        table[:, 128 * p:128 * (p + 1)] = pieces[p] + pltpu.roll(pieces[p + nodes // 2], 64, 1)


def idle_kernel(out_ref):
    out_ref[...] = jnp.zeros_like(out_ref)


def idle_call():
    return pl.pallas_call(
        idle_kernel,
        out_shape=jax.ShapeDtypeStruct((8, 128), F32),
        compiler_params=pltpu.CompilerParams(vmem_limit_bytes=PACK_VMEM),
        cost_estimate=pl.CostEstimate(flops=PACK_FLOPS, transcendentals=0, bytes_accessed=PACK_BYTES),
        name='idle',
    )()


def pack_kernel(send_ref, mask_ref, edge_ref, mesh_ref, dep_ref, out_ref, lanes, table, *, grid_cols):
    pack_slots(send_ref, mask_ref, edge_ref, mesh_ref, lanes, table, lax.axis_index('lon'), grid_cols)
    out_ref[...] = table[...].astype(BF16)


def pack_call(senders, edge_mask, edge_t, mesh_t, dep, grid_cols):
    width = senders.shape[0] // 2 * 128
    return pl.pallas_call(
        functools.partial(pack_kernel, grid_cols=grid_cols),
        out_shape=jax.ShapeDtypeStruct((FEATS, width), BF16),
        scratch_shapes=[pltpu.VMEM((FEATS, 128), F32), pltpu.VMEM((FEATS, width), F32)],
        compiler_params=pltpu.CompilerParams(vmem_limit_bytes=PACK_VMEM),
        cost_estimate=pl.CostEstimate(flops=PACK_FLOPS, transcendentals=0, bytes_accessed=PACK_BYTES),
        name='pack',
    )(senders, edge_mask, edge_t, mesh_t, dep)


def rank_slots(vtb, lon, cols, nodes):
    slots = vtb.shape[1]
    chunks = slots // 128
    vt = vtb.astype(F32)
    col = vt[5:6] - (lon * cols).astype(F32)
    cell = vt[7:8] - (lon * nodes).astype(F32)
    inner = (cell > -0.5) & (cell < nodes - 0.5)
    live = (vt[6:7] > 0.5) & (col > -0.5) & (col < cols - 0.5)
    up = lax.broadcasted_iota(jnp.int32, (128, 128), 0) <= lax.broadcasted_iota(jnp.int32, (128, 128), 1)
    low = lax.broadcasted_iota(jnp.int32, (chunks, chunks), 1) < lax.broadcasted_iota(jnp.int32, (chunks, chunks), 0)
    up = jnp.where(up, 1.0, 0.0).astype(BF16)
    low = jnp.where(low, 1.0, 0.0).astype(BF16)
    ones = jnp.full((chunks, chunks), 1.0, BF16)

    def count(flag):
        flag = jnp.where(flag, 1.0, 0.0)
        flags = jnp.concatenate([flag[:, 128 * c:128 * (c + 1)] for c in range(chunks)], axis=0)
        incl = mm(flags.astype(BF16), up)
        row_sum = jnp.broadcast_to(incl[:, 127:128], (chunks, 128)).astype(BF16)
        return flags, incl + mm(low, row_sum) - 1.0, mm(ones, row_sum)

    far, far_rank, n_far = count(live & jnp.logical_not(inner))
    near, near_rank, n_near = count(live & inner)
    skip = jnp.floor((n_far + (TILE - 1)) * (1.0 / TILE)) * TILE
    rank = jnp.where(far > 0.5, far_rank, jnp.where(near > 0.5, near_rank + skip, -1.0))
    return rank, n_far, skip + n_near


def mesh_latents(vtb, lons, nodes, wm_ref, wo_ref, bg_ref):
    slots = vtb.shape[1]
    latent = wo_ref.shape[-1]
    band = lons * nodes
    ids = lax.broadcasted_iota(jnp.int32, (band, slots), 0)
    local = lax.rem(ids, nodes)
    pick_row = lax.div(ids, nodes) * (slots // lons) + lax.rem(local, nodes // 2) * 128 + lax.div(local, nodes // 2) * 64
    pick = lax.broadcasted_iota(jnp.int32, (band, slots), 1) == pick_row
    mesh_feat = mm_nt(jnp.where(pick, 1.0, 0.0).astype(BF16), vtb).astype(BF16)
    wm = jnp.concatenate(
        [jnp.zeros((8, latent), F32), wm_ref[...].astype(F32), jnp.zeros((FEATS - 11, latent), F32)], axis=0).astype(BF16)
    bg1 = bg_ref[1]
    return mlp_tail(mm(mesh_feat, wm) + bg1[0:1], wo_ref[1], bg1)


def embed_kernel(x_ref, wg_ref, wo_ref, bg_ref, feat_ref, wm_ref,
                 vg_ref, tab_ref, band_ref, rank_ref, vm_ref,
                 scr, half, from_south, from_north, feat_in, up_sems, down_sems, feat_send, feat_recv, *, lats, lons):
    batch, grid_rows, cols, chans = x_ref.shape
    latent = vg_ref.shape[-1]
    lat = lax.axis_index('lat')
    lon = lax.axis_index('lon')
    odd = lax.rem(lat, 2)
    inner_north = lat > 0
    inner_south = lat < lats - 1
    mesh_id = pl.DeviceIdType.MESH

    def strip(start, dst, sems, to):
        return pltpu.make_async_remote_copy(
            tab_ref.at[pl.ds(start, REACH)], dst, sems.at[0], sems.at[1], device_id={'lat': to}, device_id_type=mesh_id)

    north_send = strip(REACH, from_south, up_sems, lat - 1)
    south_send = strip(grid_rows, from_north, down_sems, lat + 1)
    feats = [pltpu.make_async_remote_copy(
        feat_ref, feat_in.at[lon], feat_send.at[k - 1], feat_recv.at[k - 1],
        device_id={'lon': lax.rem(lon + k, lons)}, device_id_type=mesh_id) for k in range(1, lons)]

    barrier = pltpu.get_barrier_semaphore()
    for k in range(1, lons):
        pl.semaphore_signal(barrier, 1, device_id={'lon': lax.rem(lon + k, lons)}, device_id_type=mesh_id)

    @pl.when(inner_north)
    def _():
        pl.semaphore_signal(barrier, 1, device_id={'lat': lat - 1}, device_id_type=mesh_id)

    @pl.when(inner_south)
    def _():
        pl.semaphore_signal(barrier, 1, device_id={'lat': lat + 1}, device_id_type=mesh_id)

    feat_in[lon] = feat_ref[...]
    half[...] = wg_ref[...] * jnp.asarray(0.5, BF16)
    bg = bg_ref[0]
    b1 = bg[0:1] * 0.5

    def row(i):
        return i + odd * (grid_rows - 1 - 2 * i)

    def first(i):
        return gate(mm(x_ref[:, row(i)].reshape(batch * cols, chans), half[...]) + b1)

    def second(i, hid):
        vg = norm(mm(hid, wo_ref[0]) + bg[1:2]) * bg[2:3] + bg[3:4]
        vg_ref[:, row(i)] = vg.astype(BF16).reshape(batch, cols, latent)

        def put(c, k, part):
            tab_ref[REACH + row(i), c, :, 128 * k:128 * (k + 1)] = part

        swap_rows(vg, scr.at[i % scr.shape[0]], cols, put)

    staged(range(REACH), first, second)
    pl.semaphore_wait(barrier, lons - 1 + inner_north.astype(jnp.int32) + inner_south.astype(jnp.int32))

    @pl.when(inner_north & (odd == 0))
    def _():
        north_send.start()

    @pl.when(inner_south & (odd == 1))
    def _():
        south_send.start()

    for copy in feats:
        copy.start()
    staged(range(grid_rows - REACH, grid_rows), first, second)

    @pl.when(inner_north & (odd == 1))
    def _():
        north_send.start()

    @pl.when(inner_south & (odd == 0))
    def _():
        south_send.start()

    def extra():
        band_ref[...] = feat_in[...]
        vtb = jnp.concatenate([feat_in[k] for k in range(lons)], axis=1)
        nodes = 2 * (feat_in.shape[2] // 128)
        rank, n_far, end = rank_slots(vtb, lon, cols, nodes)
        rank_ref[0:rank.shape[0]] = rank
        rank_ref[rank.shape[0]:rank.shape[0] + 8] = n_far[0:8]
        rank_ref[rank.shape[0] + 8:] = end[0:8]
        vm_ref[...] = mesh_latents(vtb, lons, nodes, wm_ref, wo_ref, bg_ref).astype(BF16).astype(F32)

    middle = grid_rows // 2 + 2
    staged(range(REACH, middle), first, second)
    for copy in feats:
        copy.wait()
    staged(range(middle, grid_rows - REACH), first, second, extra)

    @pl.when(inner_north)
    def _():
        north_send.wait_send()
        south_send.wait_recv()
        tab_ref[0:REACH] = from_north[...]

    @pl.when(inner_south)
    def _():
        south_send.wait_send()
        north_send.wait_recv()
        tab_ref[grid_rows + REACH:grid_rows + 2 * REACH] = from_south[...]


def embed_call(grid_in, w_grid, w_out, bias_gain, feats, w_mesh, lats, lons):
    batch, rows, cols, chans = grid_in.shape
    latent = w_out.shape[-1]
    strip = (REACH, cols, batch, latent)
    local = pl.BlockSpec(memory_space=pltpu.VMEM)
    return pl.pallas_call(
        functools.partial(embed_kernel, lats=lats, lons=lons),
        in_specs=[local] * 6,
        out_specs=[local] * 5,
        out_shape=[
            jax.ShapeDtypeStruct((batch, rows, cols, latent), BF16),
            jax.ShapeDtypeStruct((rows + 2 * REACH, cols, batch, latent), BF16),
            jax.ShapeDtypeStruct((lons,) + feats.shape, BF16),
            jax.ShapeDtypeStruct((lons * feats.shape[1] // 128 + 16, 128), F32),
            jax.ShapeDtypeStruct((lons * feats.shape[1] // 64, latent), F32)],
        scratch_shapes=[
            pltpu.VMEM((4, latent // 128, batch * (cols + 8), 128), F32),
            pltpu.VMEM((chans, latent), BF16),
            pltpu.VMEM(strip, BF16), pltpu.VMEM(strip, BF16),
            pltpu.VMEM((lons,) + feats.shape, BF16),
            pltpu.SemaphoreType.DMA((2,)), pltpu.SemaphoreType.DMA((2,)),
            pltpu.SemaphoreType.DMA((lons - 1,)), pltpu.SemaphoreType.DMA((lons - 1,))],
        compiler_params=pltpu.CompilerParams(collective_id=0, has_side_effects=True, vmem_limit_bytes=GRID_VMEM),
        cost_estimate=pl.CostEstimate(
            flops=4 * rows * batch * cols * latent * latent, transcendentals=0,
            bytes_accessed=6 * rows * batch * cols * latent),
        name='embed',
    )(grid_in, w_grid, w_out, bias_gain, feats, w_mesh)


def staged(items, first, second, extra=None):
    items = list(items)
    hid = first(items[0])
    if extra is not None:
        extra()
    for k, item in enumerate(items):
        nxt = first(items[k + 1]) if k + 1 < len(items) else None
        second(item, hid)
        hid = nxt


def update_kernel(vg_ref, wu_ref, wo_ref, bg_ref, dep_ref, out_ref, half, obuf, sems):
    half[...] = wu_ref[...] * jnp.asarray(0.5, BF16)
    bg = bg_ref[5]
    b1 = bg[0:1] * 0.5
    count = vg_ref.shape[0] // SUB

    def rows(i):
        return pl.ds(i * SUB, SUB)

    def put(i):
        return pltpu.make_async_copy(obuf.at[rows(i)], out_ref.at[rows(i)], sems.at[i])

    def first(i):
        return gate(mm(vg_ref[rows(i), :], half[...]) + b1)

    def second(i, hid):
        upd = norm(mm(hid, wo_ref[5]) + bg[1:2]) * bg[2:3] + bg[3:4]
        obuf[rows(i), :] = (vg_ref[rows(i), :].astype(F32) + upd).astype(BF16)
        if i:
            put(i - 1).start()

    staged(range(count), first, second)
    put(count - 1).start()
    for i in range(count):
        put(i).wait()


def update_call(vg, w_gupd, w_out, bias_gain, dep):
    rows, latent = vg.shape
    local = pl.BlockSpec(memory_space=pltpu.VMEM)
    anywhere = pl.BlockSpec(memory_space=pl.ANY)
    return pl.pallas_call(
        update_kernel,
        in_specs=[local] * 4 + [anywhere],
        out_specs=anywhere,
        out_shape=jax.ShapeDtypeStruct(vg.shape, BF16),
        scratch_shapes=[pltpu.VMEM((latent, latent), BF16), pltpu.VMEM(vg.shape, BF16), pltpu.SemaphoreType.DMA((rows // SUB,))],
        cost_estimate=pl.CostEstimate(flops=4 * rows * latent * latent, transcendentals=0, bytes_accessed=4 * rows * latent),
        compiler_params=pltpu.CompilerParams(vmem_limit_bytes=UPDATE_VMEM),
        name='update',
    )(vg, w_gupd, w_out, bias_gain, dep)


def spread(ref, base, count, reps):
    rows = []
    for s in range(count):
        row = jnp.concatenate([ref[k, pl.ds(base + s, 8, stride=0), :] for k in range(ref.shape[0])], axis=1)
        rows += [row] * reps
    return jnp.concatenate(rows, axis=0)


def put_lanes(ref, rows, value):
    for k in range(ref.shape[0]):
        ref[k, rows, :] = value[:, 128 * k:128 * (k + 1)]


def message_loop(start, stop, tab_ref, w_in, w3, bg3, lp, ec, idx, part, bufs, hids):
    rows, cols, batch, latent = tab_ref.shape
    table = tab_ref.reshape(rows * cols, batch, latent)
    per = TILE // 2
    b2 = bg3[1:2]
    gain = bg3[2:3]

    def first(base, k):
        for s in range(per):
            bufs[k % 2][pl.ds(s * batch, batch), :] = table[lax.div(idx[0, base + s], CODE)]
        acc = mm(bufs[k % 2][...], w_in[...])
        hids[k][...] = gate(acc + spread(lp, base, per, batch // 8))

    def second(base, k):
        y = mm(hids[k][...], w3[...]) + b2
        z = norm(y) * gain + spread(ec, base, per, batch // 8)
        z = z.astype(BF16).astype(F32).reshape(per, batch, latent)
        for s in range(per):
            n = lax.rem(idx[0, base + s], CODE)
            part[n] += z[s]

    def both(t, k, stage):
        for j in range(2):
            stage(t * TILE + j * per, 2 * k + j)

    def mixed(t1, k1, t2, k2):
        for j in range(2):
            first(t1 * TILE + j * per, 2 * k1 + j)
            second(t2 * TILE + j * per, 2 * k2 + j)

    @pl.when(stop > start)
    def _():
        both(start, 0, first)

    def step(m, carry):
        t = start + 2 * m
        mixed(t + 1, 1, t, 0)
        mixed(jnp.minimum(t + 2, stop - 1), 0, t + 1, 1)
        return carry

    lax.fori_loop(0, lax.div(stop - start, 2), step, 0)

    @pl.when(lax.rem(stop - start, 2) == 1)
    def _():
        both(stop - 1, 0, second)


def three_parts(x):
    hi = x.astype(BF16)
    rest = x - hi.astype(F32)
    mid = rest.astype(BF16)
    return jnp.concatenate([hi, mid, (rest - mid.astype(F32)).astype(BF16)], axis=0)


def select(rank, base):
    slot = lax.broadcasted_iota(jnp.int32, (PREP, 128), 0).astype(F32) + base
    return jnp.concatenate(
        [jnp.where(rank[c:c + 1] == slot, 1.0, 0.0).astype(BF16) for c in range(rank.shape[0])], axis=1)


def prepare(start, stop, rank, vtb, we_ref, wmsg_ref, wo_ref, bg_ref, node_proj, lp, ec):
    latent = wo_ref.shape[-1]
    band = node_proj.shape[0] // 3
    we = jnp.concatenate([we_ref[...].astype(F32), jnp.zeros((FEATS - 4, latent), F32)], axis=0).astype(BF16)
    bg2 = bg_ref[2]
    bg3 = bg_ref[3]

    def prep(t, carry):
        feat = mm_nt(select(rank, (t * PREP).astype(F32)), vtb).astype(BF16)
        here = pl.ds(pl.multiple_of(t * PREP, PREP), PREP)
        edge = mlp_tail(mm(feat, we) + bg2[0:1], wo_ref[2], bg2).astype(BF16)
        lane = lax.rem(lax.broadcasted_iota(jnp.int32, (PREP, 3 * band), 1), band).astype(F32)
        hot = jnp.where(lane == feat[:, 7:8].astype(F32), 1.0, 0.0).astype(BF16)
        put_lanes(lp, here, (mm(edge, wmsg_ref[0:latent, :]) + mm(hot, node_proj[...]) + bg3[0:1]) * 0.5)
        put_lanes(ec, here, edge.astype(F32) + bg3[3:4])
        return carry

    lax.fori_loop(start, stop, prep, 0)


def far_kernel(v_ref, rank_ref, vm_ref, we_ref, wmsg_ref, wo_ref, bg_ref, tab_ref,
               p1_ref, p2_ref, p3_ref, idx_v, proj_ref,
               lp, ec, idx_s, part, half, hid_a, hid_b, hid_c, hid_d, buf_a, buf_b, isem, *, lons, nodes):
    latent = wo_ref.shape[-1]
    grid_rows, cols = tab_ref.shape[:2]
    positions = grid_rows * cols
    cell_rows = grid_rows - 2 * REACH
    band = lons * nodes
    chunks = rank_ref.shape[0] - 16
    meta = idx_v.shape[1] - 128
    lat = lax.axis_index('lat')
    lon = lax.axis_index('lon')
    vtb = jnp.concatenate([v_ref[k] for k in range(lons)], axis=1)
    rank = rank_ref[0:chunks]
    n_far = jnp.max(rank_ref[chunks:chunks + 8]).astype(jnp.int32)
    end = jnp.max(rank_ref[chunks + 8:]).astype(jnp.int32)
    far_tiles = lax.div(n_far + TILE - 1, TILE)
    skip = far_tiles * TILE
    proj_ref[...] = three_parts(mm(vm_ref[...].astype(BF16), wmsg_ref[2 * latent:, :]))

    def index(t, carry):
        feat_t = mm_nt(vtb, select(rank, (t * PREP).astype(F32)))
        here = pl.ds(pl.multiple_of(t * PREP, PREP), PREP)
        slot = lax.broadcasted_iota(jnp.int32, (1, PREP), 1) + t * PREP
        used = (slot < n_far) | ((slot >= skip) & (slot < end))
        win_r = feat_t[4:5] - (lat * cell_rows - REACH).astype(F32)
        win_c = feat_t[5:6] - (lon * cols).astype(F32)
        pos = jnp.clip(jnp.where(used, (win_r * cols + win_c).astype(jnp.int32), REACH * cols), 0, positions - 1)
        node = feat_t[7:8].astype(jnp.int32)
        cell = lax.div(node, nodes)
        rel = jnp.where(used, jnp.bitwise_xor(cell, lon) * nodes + (node - cell * nodes), band)
        idx_v[0:1, here] = pos * CODE + rel
        return carry

    lax.fori_loop(0, lax.div(end + PREP - 1, PREP), index, 0)
    lane = lax.broadcasted_iota(jnp.int32, (1, 128), 1)
    idx_v[0:1, meta:meta + 128] = jnp.where(lane == 0, far_tiles, lax.div(end + TILE - 1, TILE))
    move = pltpu.make_async_copy(idx_v, idx_s, isem)
    move.start()
    part[...] = jnp.zeros_like(part)
    half[...] = wmsg_ref[latent:2 * latent, :] * jnp.asarray(0.5, BF16)
    prepare(0, lax.div(skip + PREP - 1, PREP), rank, vtb, we_ref, wmsg_ref, wo_ref, bg_ref, proj_ref, lp, ec)
    move.wait()
    message_loop(0, far_tiles, tab_ref, half, wo_ref.at[3], bg_ref[3], lp, ec, idx_s, part, (buf_a, buf_b), (hid_a, hid_b, hid_c, hid_d))
    for k, ref in enumerate((p1_ref, p2_ref, p3_ref)):
        ref[...] = part[(k + 1) * nodes:(k + 2) * nodes]


def near_kernel(idx, v_ref, rank_ref, proj_ref, we_ref, wmsg_ref, wo_ref, bg_ref, tab_ref, own_ref, lp, ec, part, half, hid_a, hid_b, hid_c, hid_d, buf_a, buf_b):
    latent = wo_ref.shape[-1]
    nodes = own_ref.shape[0]
    part[...] = jnp.zeros_like(part)
    half[...] = wmsg_ref[latent:2 * latent, :] * jnp.asarray(0.5, BF16)
    vtb = jnp.concatenate([v_ref[k] for k in range(v_ref.shape[0])], axis=1)
    meta = idx.shape[1] - 128
    start, stop = idx[0, meta], idx[0, meta + 1]
    ratio = PREP // TILE
    prepare(lax.div(start, ratio), lax.div(stop + ratio - 1, ratio), rank_ref[0:rank_ref.shape[0] - 16], vtb, we_ref, wmsg_ref, wo_ref, bg_ref,
            proj_ref, lp, ec)
    message_loop(start, stop, tab_ref, half, wo_ref.at[3], bg_ref[3], lp, ec, idx, part,
                 (buf_a, buf_b), (hid_a, hid_b, hid_c, hid_d))
    own_ref[...] = part[0:nodes]


def loop_scratch(batch, latent):
    half_tile = pltpu.VMEM((TILE // 2 * batch, latent), BF16)
    return [pltpu.VMEM((latent, latent), BF16)] + [half_tile] * 6


def edge_call(v, rank, vm, w_edge, w_msg, w_out, bias_gain, table, lons, nodes, per_node):
    latent = w_out.shape[-1]
    batch = table.shape[2]
    limit = lons * nodes * per_node + PREP + 128
    local = pl.BlockSpec(memory_space=pltpu.VMEM)
    outs = [jax.ShapeDtypeStruct((nodes, batch, latent), F32)] * (lons - 1)
    outs += [jax.ShapeDtypeStruct((1, limit), jnp.int32), jax.ShapeDtypeStruct((3 * lons * nodes, latent), BF16)]
    res = pl.pallas_call(
        functools.partial(far_kernel, lons=lons, nodes=nodes),
        in_specs=[local] * 8,
        out_specs=[local] * len(outs),
        out_shape=outs,
        scratch_shapes=[
            pltpu.VMEM((latent // 128, limit, 128), F32), pltpu.VMEM((latent // 128, limit, 128), F32),
            pltpu.SMEM((1, limit), jnp.int32),
            pltpu.VMEM((lons * nodes + 1, batch, latent), F32)] + loop_scratch(batch, latent) + [pltpu.SemaphoreType.DMA],
        compiler_params=pltpu.CompilerParams(vmem_limit_bytes=EDGE_VMEM),
        cost_estimate=pl.CostEstimate(
            flops=4 * limit // 8 * batch * latent * latent, transcendentals=0, bytes_accessed=limit * batch * latent),
        name='edges_far',
    )(v, rank, vm, w_edge, w_msg, w_out, bias_gain, table)
    return res[:lons - 1], res[lons - 1:]


def near_call(v, rank, lists, w_edge, w_msg, w_out, bias_gain, table, nodes, band):
    idx, proj = lists
    latent = w_out.shape[-1]
    batch = table.shape[2]
    local = pl.BlockSpec(memory_space=pltpu.VMEM)
    return pl.pallas_call(
        near_kernel,
        in_specs=[pl.BlockSpec(memory_space=pltpu.SMEM)] + [local] * 8,
        out_specs=[local],
        out_shape=[jax.ShapeDtypeStruct((nodes, batch, latent), F32)],
        scratch_shapes=[pltpu.VMEM((latent // 128, idx.shape[1], 128), F32), pltpu.VMEM((latent // 128, idx.shape[1], 128), F32),
                        pltpu.VMEM((band + 1, batch, latent), F32)] + loop_scratch(batch, latent),
        compiler_params=pltpu.CompilerParams(vmem_limit_bytes=EDGE_VMEM),
        cost_estimate=pl.CostEstimate(
            flops=idx.shape[1] * batch * latent * latent, transcendentals=0, bytes_accessed=idx.shape[1] * batch * latent),
        name='edges_near',
    )(idx, v, rank, proj, w_edge, w_msg, w_out, bias_gain, table)


def node_kernel(own_ref, r1_ref, r2_ref, r3_ref, vm_ref, wn_ref, w4_ref, bg_ref, out_ref, scr):
    nodes, batch, latent = own_ref.shape
    agg = (own_ref[...] + r1_ref[...] + r2_ref[...] + r3_ref[...]).astype(BF16).reshape(nodes * batch, latent)
    bg = bg_ref[4]
    own_vm = vm_ref[pl.ds(pl.multiple_of(lax.axis_index('lon') * nodes, 8), nodes), :]
    base = mm(own_vm.astype(BF16), wn_ref[0:latent, :]) + bg[0:1]
    acc = mm(agg, wn_ref[latent:, :]).reshape(nodes, batch, latent) + base.reshape(nodes, 1, latent)
    upd = mlp_tail(acc.reshape(nodes * batch, latent), w4_ref[4], bg)
    out = (upd.reshape(nodes, batch, latent) + own_vm.reshape(nodes, 1, latent)).reshape(nodes * batch, latent)

    def put(b, k, part):
        out_ref[b, :, 128 * k:128 * (k + 1)] = part

    swap_rows(out, scr, batch, put)


def node_call(blocks, vm, w_node, w_out, bias_gain):
    nodes, batch, latent = blocks[0].shape
    local = pl.BlockSpec(memory_space=pltpu.VMEM)
    out = jax.ShapeDtypeStruct((batch, nodes, latent), BF16)
    return pl.pallas_call(
        node_kernel,
        in_specs=[local] * 8,
        out_specs=local,
        out_shape=out,
        compiler_params=pltpu.CompilerParams(vmem_limit_bytes=NODE_VMEM),
        scratch_shapes=[pltpu.VMEM((latent // 128, nodes * (batch + 8), 128), F32)],
        name='nodes',
    )(*blocks, vm, w_node, w_out, bias_gain)


def solution(mesh):
    lats = mesh.shape['lat']
    lons = mesh.shape['lon']
    south_shift = [(s, s + 1) for s in range(lats - 1)]
    north_shift = [(s + 1, s) for s in range(lats - 1)]

    def cell_step(grid_in, mesh_in, edge_in, senders, edge_mask, w_grid, w_mesh, w_edge, w_msg, w_node, w_gupd, w_out, bias_gain):
        batch, rows, cols, _ = grid_in.shape
        nodes = senders.shape[0]
        latent = w_out.shape[-1]
        feats = pack_call(senders, edge_mask, jnp.swapaxes(edge_in, 1, 2), mesh_in.T, idle_call(), cols * lons)
        vg, table, band, rank, vm = embed_call(grid_in, w_grid, w_out, bias_gain, feats, w_mesh, lats, lons)
        blocks, lists = edge_call(band, rank, vm, w_edge, w_msg, w_out, bias_gain, table, lons, *senders.shape)
        own, = near_call(band, rank, lists, w_edge, w_msg, w_out, bias_gain, table, nodes, nodes * lons)
        pairs = lambda k, polar: [
            (j * lats + i, (j ^ k) * lats + i) for i in range(lats) for j in range(lons)
            if not polar or i in (0, lats - 1)]
        got = [lax.ppermute(blocks[k - 1], ('lon', 'lat'), pairs(k, k == 2)) for k in (3, 2, 1)]
        mesh_out = node_call([own] + got, vm, w_node, w_out, bias_gain)
        flat = update_call(vg.reshape(batch * rows * cols, latent), w_gupd, w_out, bias_gain, own)
        grid_out = flat.reshape(batch, rows, cols, latent)
        return mesh_out, grid_out

    grid_spec = P('dp', 'lat', 'lon', None)
    node_spec = P(('lat', 'lon'), None)
    slot_spec = P(('lat', 'lon'), None, None)
    in_specs = (grid_spec, node_spec, slot_spec, node_spec, node_spec) + (P(),) * 8
    out_specs = (P('dp', ('lat', 'lon'), None), grid_spec)
    return jax.shard_map(cell_step, mesh=mesh, in_specs=in_specs, out_specs=out_specs, check_vma=False)
```

```python
import functools

import jax
import jax.numpy as jnp
from jax import lax
from jax.experimental import pallas as pl
from jax.experimental.pallas import tpu as pltpu
from jax.sharding import PartitionSpec as P

REACH = 3
LN_EPS = 1e-5
FEATS = 16
TILE = 32
SUB = 512
PREP = 128
CODE = 64
PACK_VMEM = 40 * 2 ** 20
PACK_FLOPS = 2 * 10 ** 9
PACK_BYTES = 10 ** 6
EDGE_VMEM = 20 * 2 ** 20
NODE_VMEM = 6 * 2 ** 20
GRID_VMEM = 24 * 2 ** 20
UPDATE_VMEM = 12 * 2 ** 20
F32 = jnp.float32
BF16 = jnp.bfloat16


def mm(a, b):
    return jnp.dot(a, b, preferred_element_type=F32)


def mm_nt(a, b):
    return lax.dot_general(a, b, (((1,), (1,)), ((), ())), preferred_element_type=F32)


def gate(t):
    return (t + t * jnp.tanh(t)).astype(BF16)


def swish(x):
    return gate(x * 0.5)


def norm(y):
    scale = 1.0 / y.shape[-1]
    centered = y - jnp.sum(y, axis=-1, keepdims=True) * scale
    var = jnp.sum(centered * centered, axis=-1, keepdims=True) * scale
    return centered * lax.rsqrt(var + LN_EPS)


def mlp_tail(pre, w2, bg):
    y = mm(swish(pre), w2) + bg[1:2]
    return norm(y) * bg[2:3] + bg[3:4]


def swap_rows(value, scr, inner, put):
    outer = value.shape[0] // inner
    pitch = scr.shape[1] // outer
    for k in range(scr.shape[0]):
        for b in range(outer):
            scr[k, pl.ds(b * pitch, inner), :] = value[b * inner:(b + 1) * inner, 128 * k:128 * (k + 1)]
    for c in range(inner):
        for k in range(scr.shape[0]):
            put(c, k, scr[k, pl.ds(c, outer, stride=pitch), :].astype(BF16))


def pack_slots(send_ref, mask_ref, edge_ref, mesh_ref, lanes, table, lon, grid_cols):
    nodes, per_node = send_ref.shape
    bits = grid_cols.bit_length() - 1
    send = send_ref[...]
    row = lax.shift_right_logical(send, bits).astype(F32)
    col = (send & (grid_cols - 1)).astype(F32)
    mask = mask_ref[...].astype(F32)
    mesh = mesh_ref[...].astype(F32)
    pieces = []
    for n in range(nodes):
        here = slice(n, n + 1)
        lanes[...] = jnp.zeros_like(lanes)
        lanes[0:4, 0:per_node] = edge_ref[n].astype(F32)
        lanes[4:5, 0:per_node] = row[here]
        lanes[5:6, 0:per_node] = col[here]
        lanes[6:7, 0:per_node] = mask[here]
        lanes[7:8, 0:per_node] = jnp.full((1, per_node), n, F32) + (lon * nodes).astype(F32)
        lanes[8:11, 0:per_node] = jnp.broadcast_to(mesh[:, here], (3, per_node))
        pieces.append(lanes[...])
    for p in range(nodes // 2):
        table[:, 128 * p:128 * (p + 1)] = pieces[p] + pltpu.roll(pieces[p + nodes // 2], 64, 1)


def idle_kernel(out_ref):
    out_ref[...] = jnp.zeros_like(out_ref)


def idle_call():
    return pl.pallas_call(
        idle_kernel,
        out_shape=jax.ShapeDtypeStruct((8, 128), F32),
        compiler_params=pltpu.CompilerParams(vmem_limit_bytes=PACK_VMEM),
        cost_estimate=pl.CostEstimate(flops=PACK_FLOPS, transcendentals=0, bytes_accessed=PACK_BYTES),
        name='idle',
    )()


def pack_kernel(send_ref, mask_ref, edge_ref, mesh_ref, dep_ref, wm_ref, wo_ref, bg_ref, out_ref, vm_ref, lanes, table, *, grid_cols):
    pack_slots(send_ref, mask_ref, edge_ref, mesh_ref, lanes, table, lax.axis_index('lon'), grid_cols)
    out_ref[...] = table[...].astype(BF16)
    latent = wo_ref.shape[-1]
    nodes = mesh_ref.shape[1]
    feat = jnp.concatenate([mesh_ref[...].astype(F32), jnp.zeros((nodes - 3, nodes), F32)], axis=0)
    weight = jnp.concatenate([wm_ref[...].astype(F32), jnp.zeros((nodes - 3, latent), F32)], axis=0)
    pre = lax.dot_general(
        feat.astype(BF16), weight.astype(BF16), (((0,), (0,)), ((), ())), preferred_element_type=F32)
    bg1 = bg_ref[1]
    vm_ref[...] = mlp_tail(pre + bg1[0:1], wo_ref[1], bg1).astype(BF16).astype(F32)


def pack_call(senders, edge_mask, edge_t, mesh_t, dep, w_mesh, w_out, bias_gain, grid_cols):
    width = senders.shape[0] // 2 * 128
    latent = w_out.shape[-1]
    return pl.pallas_call(
        functools.partial(pack_kernel, grid_cols=grid_cols),
        out_shape=[jax.ShapeDtypeStruct((FEATS, width), BF16), jax.ShapeDtypeStruct((senders.shape[0], latent), F32)],
        scratch_shapes=[pltpu.VMEM((FEATS, 128), F32), pltpu.VMEM((FEATS, width), F32)],
        compiler_params=pltpu.CompilerParams(vmem_limit_bytes=PACK_VMEM),
        cost_estimate=pl.CostEstimate(flops=PACK_FLOPS, transcendentals=0, bytes_accessed=PACK_BYTES),
        name='pack',
    )(senders, edge_mask, edge_t, mesh_t, dep, w_mesh, w_out, bias_gain)


def rank_slots(vtb, lon, cols, nodes):
    slots = vtb.shape[1]
    chunks = slots // 128
    vt = vtb.astype(F32)
    col = vt[5:6] - (lon * cols).astype(F32)
    cell = vt[7:8] - (lon * nodes).astype(F32)
    inner = (cell > -0.5) & (cell < nodes - 0.5)
    live = (vt[6:7] > 0.5) & (col > -0.5) & (col < cols - 0.5)
    up = lax.broadcasted_iota(jnp.int32, (128, 128), 0) <= lax.broadcasted_iota(jnp.int32, (128, 128), 1)
    low = lax.broadcasted_iota(jnp.int32, (chunks, chunks), 1) < lax.broadcasted_iota(jnp.int32, (chunks, chunks), 0)
    up = jnp.where(up, 1.0, 0.0).astype(BF16)
    low = jnp.where(low, 1.0, 0.0).astype(BF16)
    ones = jnp.full((chunks, chunks), 1.0, BF16)

    def count(flag):
        flag = jnp.where(flag, 1.0, 0.0)
        flags = jnp.concatenate([flag[:, 128 * c:128 * (c + 1)] for c in range(chunks)], axis=0)
        incl = mm(flags.astype(BF16), up)
        row_sum = jnp.broadcast_to(incl[:, 127:128], (chunks, 128)).astype(BF16)
        return flags, incl + mm(low, row_sum) - 1.0, mm(ones, row_sum)

    far, far_rank, n_far = count(live & jnp.logical_not(inner))
    near, near_rank, n_near = count(live & inner)
    skip = jnp.floor((n_far + (TILE - 1)) * (1.0 / TILE)) * TILE
    rank = jnp.where(far > 0.5, far_rank, jnp.where(near > 0.5, near_rank + skip, -1.0))
    return rank, n_far, skip + n_near


def embed_kernel(x_ref, wg_ref, wo_ref, bg_ref, feat_ref, own_vm_ref,
                 vg_ref, tab_ref, band_ref, rank_ref, vm_ref,
                 scr, half, from_south, from_north, feat_in, vm_in, up_sems, down_sems, feat_send, feat_recv, vm_send, vm_recv, *, lats, lons):
    batch, grid_rows, cols, chans = x_ref.shape
    latent = vg_ref.shape[-1]
    lat = lax.axis_index('lat')
    lon = lax.axis_index('lon')
    odd = lax.rem(lat, 2)
    inner_north = lat > 0
    inner_south = lat < lats - 1
    mesh_id = pl.DeviceIdType.MESH

    def strip(start, dst, sems, to):
        return pltpu.make_async_remote_copy(
            tab_ref.at[pl.ds(start, REACH)], dst, sems.at[0], sems.at[1], device_id={'lat': to}, device_id_type=mesh_id)

    north_send = strip(REACH, from_south, up_sems, lat - 1)
    south_send = strip(grid_rows, from_north, down_sems, lat + 1)
    feats = [pltpu.make_async_remote_copy(
        feat_ref, feat_in.at[lon], feat_send.at[k - 1], feat_recv.at[k - 1],
        device_id={'lon': lax.rem(lon + k, lons)}, device_id_type=mesh_id) for k in range(1, lons)]
    feats += [pltpu.make_async_remote_copy(
        own_vm_ref, vm_in.at[lon], vm_send.at[k - 1], vm_recv.at[k - 1],
        device_id={'lon': lax.rem(lon + k, lons)}, device_id_type=mesh_id) for k in range(1, lons)]

    barrier = pltpu.get_barrier_semaphore()
    for k in range(1, lons):
        pl.semaphore_signal(barrier, 1, device_id={'lon': lax.rem(lon + k, lons)}, device_id_type=mesh_id)

    @pl.when(inner_north)
    def _():
        pl.semaphore_signal(barrier, 1, device_id={'lat': lat - 1}, device_id_type=mesh_id)

    @pl.when(inner_south)
    def _():
        pl.semaphore_signal(barrier, 1, device_id={'lat': lat + 1}, device_id_type=mesh_id)

    feat_in[lon] = feat_ref[...]
    vm_in[lon] = own_vm_ref[...]
    half[...] = wg_ref[...] * jnp.asarray(0.5, BF16)
    bg = bg_ref[0]
    b1 = bg[0:1] * 0.5

    def row(i):
        return i + odd * (grid_rows - 1 - 2 * i)

    def first(i):
        return gate(mm(x_ref[:, row(i)].reshape(batch * cols, chans), half[...]) + b1)

    def second(i, hid):
        vg = norm(mm(hid, wo_ref[0]) + bg[1:2]) * bg[2:3] + bg[3:4]
        vg_ref[:, row(i)] = vg.astype(BF16).reshape(batch, cols, latent)

        def put(c, k, part):
            tab_ref[REACH + row(i), c, :, 128 * k:128 * (k + 1)] = part

        swap_rows(vg, scr.at[i % scr.shape[0]], cols, put)

    staged(range(REACH), first, second)
    pl.semaphore_wait(barrier, lons - 1 + inner_north.astype(jnp.int32) + inner_south.astype(jnp.int32))

    @pl.when(inner_north & (odd == 0))
    def _():
        north_send.start()

    @pl.when(inner_south & (odd == 1))
    def _():
        south_send.start()

    for copy in feats:
        copy.start()
    staged(range(grid_rows - REACH, grid_rows), first, second)

    @pl.when(inner_north & (odd == 1))
    def _():
        north_send.start()

    @pl.when(inner_south & (odd == 0))
    def _():
        south_send.start()

    def extra():
        band_ref[...] = feat_in[...]
        vtb = jnp.concatenate([feat_in[k] for k in range(lons)], axis=1)
        nodes = 2 * (feat_in.shape[2] // 128)
        rank, n_far, end = rank_slots(vtb, lon, cols, nodes)
        rank_ref[0:rank.shape[0]] = rank
        rank_ref[rank.shape[0]:rank.shape[0] + 8] = n_far[0:8]
        rank_ref[rank.shape[0] + 8:] = end[0:8]
        vm_ref[...] = vm_in[...].reshape(lons * nodes, latent)

    middle = grid_rows // 2 + 2
    staged(range(REACH, middle), first, second)
    for copy in feats:
        copy.wait()
    staged(range(middle, grid_rows - REACH), first, second, extra)

    @pl.when(inner_north)
    def _():
        north_send.wait_send()
        south_send.wait_recv()
        tab_ref[0:REACH] = from_north[...]

    @pl.when(inner_south)
    def _():
        south_send.wait_send()
        north_send.wait_recv()
        tab_ref[grid_rows + REACH:grid_rows + 2 * REACH] = from_south[...]


def embed_call(grid_in, w_grid, w_out, bias_gain, feats, own_vm, lats, lons):
    batch, rows, cols, chans = grid_in.shape
    latent = w_out.shape[-1]
    strip = (REACH, cols, batch, latent)
    local = pl.BlockSpec(memory_space=pltpu.VMEM)
    return pl.pallas_call(
        functools.partial(embed_kernel, lats=lats, lons=lons),
        in_specs=[local] * 6,
        out_specs=[local] * 5,
        out_shape=[
            jax.ShapeDtypeStruct((batch, rows, cols, latent), BF16),
            jax.ShapeDtypeStruct((rows + 2 * REACH, cols, batch, latent), BF16),
            jax.ShapeDtypeStruct((lons,) + feats.shape, BF16),
            jax.ShapeDtypeStruct((lons * feats.shape[1] // 128 + 16, 128), F32),
            jax.ShapeDtypeStruct((lons * feats.shape[1] // 64, latent), F32)],
        scratch_shapes=[
            pltpu.VMEM((4, latent // 128, batch * (cols + 8), 128), F32),
            pltpu.VMEM((chans, latent), BF16),
            pltpu.VMEM(strip, BF16), pltpu.VMEM(strip, BF16),
            pltpu.VMEM((lons,) + feats.shape, BF16), pltpu.VMEM((lons,) + own_vm.shape, F32),
            pltpu.SemaphoreType.DMA((2,)), pltpu.SemaphoreType.DMA((2,)),
            pltpu.SemaphoreType.DMA((lons - 1,)), pltpu.SemaphoreType.DMA((lons - 1,)),
            pltpu.SemaphoreType.DMA((lons - 1,)), pltpu.SemaphoreType.DMA((lons - 1,))],
        compiler_params=pltpu.CompilerParams(collective_id=0, has_side_effects=True, vmem_limit_bytes=GRID_VMEM),
        cost_estimate=pl.CostEstimate(
            flops=4 * rows * batch * cols * latent * latent, transcendentals=0,
            bytes_accessed=6 * rows * batch * cols * latent),
        name='embed',
    )(grid_in, w_grid, w_out, bias_gain, feats, own_vm)


def staged(items, first, second, extra=None):
    items = list(items)
    hid = first(items[0])
    if extra is not None:
        extra()
    for k, item in enumerate(items):
        nxt = first(items[k + 1]) if k + 1 < len(items) else None
        second(item, hid)
        hid = nxt


def update_kernel(vg_ref, wu_ref, wo_ref, bg_ref, dep_ref, out_ref, half, obuf, sems):
    half[...] = wu_ref[...] * jnp.asarray(0.5, BF16)
    bg = bg_ref[5]
    b1 = bg[0:1] * 0.5
    count = vg_ref.shape[0] // SUB

    def rows(i):
        return pl.ds(i * SUB, SUB)

    def put(i):
        return pltpu.make_async_copy(obuf.at[rows(i)], out_ref.at[rows(i)], sems.at[i])

    def first(i):
        return gate(mm(vg_ref[rows(i), :], half[...]) + b1)

    def second(i, hid):
        upd = norm(mm(hid, wo_ref[5]) + bg[1:2]) * bg[2:3] + bg[3:4]
        obuf[rows(i), :] = (vg_ref[rows(i), :].astype(F32) + upd).astype(BF16)
        if i:
            put(i - 1).start()

    staged(range(count), first, second)
    put(count - 1).start()
    for i in range(count):
        put(i).wait()


def update_call(vg, w_gupd, w_out, bias_gain, dep):
    rows, latent = vg.shape
    local = pl.BlockSpec(memory_space=pltpu.VMEM)
    anywhere = pl.BlockSpec(memory_space=pl.ANY)
    return pl.pallas_call(
        update_kernel,
        in_specs=[local] * 4 + [anywhere],
        out_specs=anywhere,
        out_shape=jax.ShapeDtypeStruct(vg.shape, BF16),
        scratch_shapes=[pltpu.VMEM((latent, latent), BF16), pltpu.VMEM(vg.shape, BF16), pltpu.SemaphoreType.DMA((rows // SUB,))],
        cost_estimate=pl.CostEstimate(flops=4 * rows * latent * latent, transcendentals=0, bytes_accessed=4 * rows * latent),
        compiler_params=pltpu.CompilerParams(vmem_limit_bytes=UPDATE_VMEM),
        name='update',
    )(vg, w_gupd, w_out, bias_gain, dep)


def spread(ref, base, count, reps):
    rows = []
    for s in range(count):
        row = jnp.concatenate([ref[k, pl.ds(base + s, 8, stride=0), :] for k in range(ref.shape[0])], axis=1)
        rows += [row] * reps
    return jnp.concatenate(rows, axis=0)


def put_lanes(ref, rows, value):
    for k in range(ref.shape[0]):
        ref[k, rows, :] = value[:, 128 * k:128 * (k + 1)]


def message_loop(start, stop, tab_ref, w_in, w3, bg3, lp, ec, idx, part, bufs, hids):
    rows, cols, batch, latent = tab_ref.shape
    table = tab_ref.reshape(rows * cols, batch, latent)
    per = TILE // 2
    b2 = bg3[1:2]
    gain = bg3[2:3]

    def first(base, k):
        for s in range(per):
            bufs[k % 2][pl.ds(s * batch, batch), :] = table[lax.div(idx[0, base + s], CODE)]
        acc = mm(bufs[k % 2][...], w_in[...])
        hids[k][...] = gate(acc + spread(lp, base, per, batch // 8))

    def second(base, k):
        y = mm(hids[k][...], w3[...]) + b2
        z = norm(y) * gain + spread(ec, base, per, batch // 8)
        z = z.astype(BF16).astype(F32).reshape(per, batch, latent)
        for s in range(per):
            n = lax.rem(idx[0, base + s], CODE)
            part[n] += z[s]

    def both(t, k, stage):
        for j in range(2):
            stage(t * TILE + j * per, 2 * k + j)

    def mixed(t1, k1, t2, k2):
        for j in range(2):
            first(t1 * TILE + j * per, 2 * k1 + j)
            second(t2 * TILE + j * per, 2 * k2 + j)

    @pl.when(stop > start)
    def _():
        both(start, 0, first)

    def step(m, carry):
        t = start + 2 * m
        mixed(t + 1, 1, t, 0)
        mixed(jnp.minimum(t + 2, stop - 1), 0, t + 1, 1)
        return carry

    lax.fori_loop(0, lax.div(stop - start, 2), step, 0)

    @pl.when(lax.rem(stop - start, 2) == 1)
    def _():
        both(stop - 1, 0, second)


def three_parts(x):
    hi = x.astype(BF16)
    rest = x - hi.astype(F32)
    mid = rest.astype(BF16)
    return jnp.concatenate([hi, mid, (rest - mid.astype(F32)).astype(BF16)], axis=0)


def select(rank, base):
    slot = lax.broadcasted_iota(jnp.int32, (PREP, 128), 0).astype(F32) + base
    return jnp.concatenate(
        [jnp.where(rank[c:c + 1] == slot, 1.0, 0.0).astype(BF16) for c in range(rank.shape[0])], axis=1)


def prepare(start, stop, rank, vtb, we_ref, wmsg_ref, wo_ref, bg_ref, node_proj, lp, ec):
    latent = wo_ref.shape[-1]
    band = node_proj.shape[0] // 3
    we = jnp.concatenate([we_ref[...].astype(F32), jnp.zeros((FEATS - 4, latent), F32)], axis=0).astype(BF16)
    bg2 = bg_ref[2]
    bg3 = bg_ref[3]

    def prep(t, carry):
        feat = mm_nt(select(rank, (t * PREP).astype(F32)), vtb).astype(BF16)
        here = pl.ds(pl.multiple_of(t * PREP, PREP), PREP)
        edge = mlp_tail(mm(feat, we) + bg2[0:1], wo_ref[2], bg2).astype(BF16)
        lane = lax.rem(lax.broadcasted_iota(jnp.int32, (PREP, 3 * band), 1), band).astype(F32)
        hot = jnp.where(lane == feat[:, 7:8].astype(F32), 1.0, 0.0).astype(BF16)
        put_lanes(lp, here, (mm(edge, wmsg_ref[0:latent, :]) + mm(hot, node_proj[...]) + bg3[0:1]) * 0.5)
        put_lanes(ec, here, edge.astype(F32) + bg3[3:4])
        return carry

    lax.fori_loop(start, stop, prep, 0)


def far_kernel(v_ref, rank_ref, vm_ref, we_ref, wmsg_ref, wo_ref, bg_ref, tab_ref,
               p1_ref, p2_ref, p3_ref, idx_v, proj_ref,
               lp, ec, idx_s, part, half, hid_a, hid_b, hid_c, hid_d, buf_a, buf_b, isem, *, lons, nodes):
    latent = wo_ref.shape[-1]
    grid_rows, cols = tab_ref.shape[:2]
    positions = grid_rows * cols
    cell_rows = grid_rows - 2 * REACH
    band = lons * nodes
    chunks = rank_ref.shape[0] - 16
    meta = idx_v.shape[1] - 128
    lat = lax.axis_index('lat')
    lon = lax.axis_index('lon')
    vtb = jnp.concatenate([v_ref[k] for k in range(lons)], axis=1)
    rank = rank_ref[0:chunks]
    n_far = jnp.max(rank_ref[chunks:chunks + 8]).astype(jnp.int32)
    end = jnp.max(rank_ref[chunks + 8:]).astype(jnp.int32)
    far_tiles = lax.div(n_far + TILE - 1, TILE)
    skip = far_tiles * TILE
    proj_ref[...] = three_parts(mm(vm_ref[...].astype(BF16), wmsg_ref[2 * latent:, :]))

    def index(t, carry):
        feat_t = mm_nt(vtb, select(rank, (t * PREP).astype(F32)))
        here = pl.ds(pl.multiple_of(t * PREP, PREP), PREP)
        slot = lax.broadcasted_iota(jnp.int32, (1, PREP), 1) + t * PREP
        used = (slot < n_far) | ((slot >= skip) & (slot < end))
        win_r = feat_t[4:5] - (lat * cell_rows - REACH).astype(F32)
        win_c = feat_t[5:6] - (lon * cols).astype(F32)
        pos = jnp.clip(jnp.where(used, (win_r * cols + win_c).astype(jnp.int32), REACH * cols), 0, positions - 1)
        node = feat_t[7:8].astype(jnp.int32)
        cell = lax.div(node, nodes)
        rel = jnp.where(used, jnp.bitwise_xor(cell, lon) * nodes + (node - cell * nodes), band)
        idx_v[0:1, here] = pos * CODE + rel
        return carry

    lax.fori_loop(0, lax.div(end + PREP - 1, PREP), index, 0)
    lane = lax.broadcasted_iota(jnp.int32, (1, 128), 1)
    idx_v[0:1, meta:meta + 128] = jnp.where(lane == 0, far_tiles, lax.div(end + TILE - 1, TILE))
    move = pltpu.make_async_copy(idx_v, idx_s, isem)
    move.start()
    part[...] = jnp.zeros_like(part)
    half[...] = wmsg_ref[latent:2 * latent, :] * jnp.asarray(0.5, BF16)
    prepare(0, lax.div(skip + PREP - 1, PREP), rank, vtb, we_ref, wmsg_ref, wo_ref, bg_ref, proj_ref, lp, ec)
    move.wait()
    message_loop(0, far_tiles, tab_ref, half, wo_ref.at[3], bg_ref[3], lp, ec, idx_s, part, (buf_a, buf_b), (hid_a, hid_b, hid_c, hid_d))
    for k, ref in enumerate((p1_ref, p2_ref, p3_ref)):
        ref[...] = part[(k + 1) * nodes:(k + 2) * nodes]


def near_kernel(idx, v_ref, rank_ref, proj_ref, we_ref, wmsg_ref, wo_ref, bg_ref, tab_ref, own_ref, lp, ec, part, half, hid_a, hid_b, hid_c, hid_d, buf_a, buf_b):
    latent = wo_ref.shape[-1]
    nodes = own_ref.shape[0]
    part[...] = jnp.zeros_like(part)
    half[...] = wmsg_ref[latent:2 * latent, :] * jnp.asarray(0.5, BF16)
    vtb = jnp.concatenate([v_ref[k] for k in range(v_ref.shape[0])], axis=1)
    meta = idx.shape[1] - 128
    start, stop = idx[0, meta], idx[0, meta + 1]
    ratio = PREP // TILE
    prepare(lax.div(start, ratio), lax.div(stop + ratio - 1, ratio), rank_ref[0:rank_ref.shape[0] - 16], vtb, we_ref, wmsg_ref, wo_ref, bg_ref,
            proj_ref, lp, ec)
    message_loop(start, stop, tab_ref, half, wo_ref.at[3], bg_ref[3], lp, ec, idx, part,
                 (buf_a, buf_b), (hid_a, hid_b, hid_c, hid_d))
    own_ref[...] = part[0:nodes]


def loop_scratch(batch, latent):
    half_tile = pltpu.VMEM((TILE // 2 * batch, latent), BF16)
    return [pltpu.VMEM((latent, latent), BF16)] + [half_tile] * 6


def edge_call(v, rank, vm, w_edge, w_msg, w_out, bias_gain, table, lons, nodes, per_node):
    latent = w_out.shape[-1]
    batch = table.shape[2]
    limit = lons * nodes * per_node + PREP + 128
    local = pl.BlockSpec(memory_space=pltpu.VMEM)
    outs = [jax.ShapeDtypeStruct((nodes, batch, latent), F32)] * (lons - 1)
    outs += [jax.ShapeDtypeStruct((1, limit), jnp.int32), jax.ShapeDtypeStruct((3 * lons * nodes, latent), BF16)]
    res = pl.pallas_call(
        functools.partial(far_kernel, lons=lons, nodes=nodes),
        in_specs=[local] * 8,
        out_specs=[local] * len(outs),
        out_shape=outs,
        scratch_shapes=[
            pltpu.VMEM((latent // 128, limit, 128), F32), pltpu.VMEM((latent // 128, limit, 128), F32),
            pltpu.SMEM((1, limit), jnp.int32),
            pltpu.VMEM((lons * nodes + 1, batch, latent), F32)] + loop_scratch(batch, latent) + [pltpu.SemaphoreType.DMA],
        compiler_params=pltpu.CompilerParams(vmem_limit_bytes=EDGE_VMEM),
        cost_estimate=pl.CostEstimate(
            flops=4 * limit // 8 * batch * latent * latent, transcendentals=0, bytes_accessed=limit * batch * latent),
        name='edges_far',
    )(v, rank, vm, w_edge, w_msg, w_out, bias_gain, table)
    return res[:lons - 1], res[lons - 1:]


def near_call(v, rank, lists, w_edge, w_msg, w_out, bias_gain, table, nodes, band):
    idx, proj = lists
    latent = w_out.shape[-1]
    batch = table.shape[2]
    local = pl.BlockSpec(memory_space=pltpu.VMEM)
    return pl.pallas_call(
        near_kernel,
        in_specs=[pl.BlockSpec(memory_space=pltpu.SMEM)] + [local] * 8,
        out_specs=[local],
        out_shape=[jax.ShapeDtypeStruct((nodes, batch, latent), F32)],
        scratch_shapes=[pltpu.VMEM((latent // 128, idx.shape[1], 128), F32), pltpu.VMEM((latent // 128, idx.shape[1], 128), F32),
                        pltpu.VMEM((band + 1, batch, latent), F32)] + loop_scratch(batch, latent),
        compiler_params=pltpu.CompilerParams(vmem_limit_bytes=EDGE_VMEM),
        cost_estimate=pl.CostEstimate(
            flops=idx.shape[1] * batch * latent * latent, transcendentals=0, bytes_accessed=idx.shape[1] * batch * latent),
        name='edges_near',
    )(idx, v, rank, proj, w_edge, w_msg, w_out, bias_gain, table)


def node_kernel(own_ref, r1_ref, r2_ref, r3_ref, vm_ref, wn_ref, w4_ref, bg_ref, out_ref, scr):
    nodes, batch, latent = own_ref.shape
    agg = (own_ref[...] + r1_ref[...] + r2_ref[...] + r3_ref[...]).astype(BF16).reshape(nodes * batch, latent)
    bg = bg_ref[4]
    own_vm = vm_ref[...]
    base = mm(own_vm.astype(BF16), wn_ref[0:latent, :]) + bg[0:1]
    acc = mm(agg, wn_ref[latent:, :]).reshape(nodes, batch, latent) + base.reshape(nodes, 1, latent)
    upd = mlp_tail(acc.reshape(nodes * batch, latent), w4_ref[4], bg)
    out = (upd.reshape(nodes, batch, latent) + own_vm.reshape(nodes, 1, latent)).reshape(nodes * batch, latent)

    def put(b, k, part):
        out_ref[b, :, 128 * k:128 * (k + 1)] = part

    swap_rows(out, scr, batch, put)


def node_call(blocks, vm, w_node, w_out, bias_gain):
    nodes, batch, latent = blocks[0].shape
    local = pl.BlockSpec(memory_space=pltpu.VMEM)
    out = jax.ShapeDtypeStruct((batch, nodes, latent), BF16)
    return pl.pallas_call(
        node_kernel,
        in_specs=[local] * 8,
        out_specs=local,
        out_shape=out,
        compiler_params=pltpu.CompilerParams(vmem_limit_bytes=NODE_VMEM),
        scratch_shapes=[pltpu.VMEM((latent // 128, nodes * (batch + 8), 128), F32)],
        name='nodes',
    )(*blocks, vm, w_node, w_out, bias_gain)


def solution(mesh):
    lats = mesh.shape['lat']
    lons = mesh.shape['lon']
    south_shift = [(s, s + 1) for s in range(lats - 1)]
    north_shift = [(s + 1, s) for s in range(lats - 1)]

    def cell_step(grid_in, mesh_in, edge_in, senders, edge_mask, w_grid, w_mesh, w_edge, w_msg, w_node, w_gupd, w_out, bias_gain):
        batch, rows, cols, _ = grid_in.shape
        nodes = senders.shape[0]
        latent = w_out.shape[-1]
        feats, own_vm = pack_call(
            senders, edge_mask, jnp.swapaxes(edge_in, 1, 2), mesh_in.T, idle_call(), w_mesh, w_out, bias_gain, cols * lons)
        vg, table, band, rank, vm = embed_call(grid_in, w_grid, w_out, bias_gain, feats, own_vm, lats, lons)
        blocks, lists = edge_call(band, rank, vm, w_edge, w_msg, w_out, bias_gain, table, lons, *senders.shape)
        own, = near_call(band, rank, lists, w_edge, w_msg, w_out, bias_gain, table, nodes, nodes * lons)
        pairs = lambda k, polar: [
            (j * lats + i, (j ^ k) * lats + i) for i in range(lats) for j in range(lons)
            if not polar or i in (0, lats - 1)]
        got = [lax.ppermute(blocks[k - 1], ('lon', 'lat'), pairs(k, k == 2)) for k in (3, 2, 1)]
        mesh_out = node_call([own] + got, own_vm, w_node, w_out, bias_gain)
        flat = update_call(vg.reshape(batch * rows * cols, latent), w_gupd, w_out, bias_gain, own)
        grid_out = flat.reshape(batch, rows, cols, latent)
        return mesh_out, grid_out

    grid_spec = P('dp', 'lat', 'lon', None)
    node_spec = P(('lat', 'lon'), None)
    slot_spec = P(('lat', 'lon'), None, None)
    in_specs = (grid_spec, node_spec, slot_spec, node_spec, node_spec) + (P(),) * 8
    out_specs = (P('dp', ('lat', 'lon'), None), grid_spec)
    return jax.shard_map(cell_step, mesh=mesh, in_specs=in_specs, out_specs=out_specs, check_vma=False)
```

```python
import functools

import jax
import jax.numpy as jnp
from jax import lax
from jax.experimental import pallas as pl
from jax.experimental.pallas import tpu as pltpu
from jax.sharding import PartitionSpec as P

REACH = 3
LN_EPS = 1e-5
FEATS = 16
TILE = 32
SUB = 256
LP = None
PREP = 128
CODE = 64
PACK_VMEM = 40 * 2 ** 20
PACK_FLOPS = 2 * 10 ** 9
PACK_BYTES = 10 ** 6
EDGE_VMEM = 20 * 2 ** 20
NODE_VMEM = 6 * 2 ** 20
GRID_VMEM = 24 * 2 ** 20
UPDATE_VMEM = 12 * 2 ** 20
F32 = jnp.float32
BF16 = jnp.bfloat16


def mm(a, b):
    return jnp.dot(a, b, preferred_element_type=F32)


def mm_nt(a, b):
    return lax.dot_general(a, b, (((1,), (1,)), ((), ())), preferred_element_type=F32)


def gate(t):
    return (t + t * jnp.tanh(t)).astype(BF16)


def swish(x):
    return gate(x * 0.5)


def norm(y):
    scale = 1.0 / y.shape[-1]
    centered = y - jnp.sum(y, axis=-1, keepdims=True) * scale
    var = jnp.sum(centered * centered, axis=-1, keepdims=True) * scale
    return centered * lax.rsqrt(var + LN_EPS)


def mlp_tail(pre, w2, bg):
    y = mm(swish(pre), w2) + bg[1:2]
    return norm(y) * bg[2:3] + bg[3:4]


def swap_rows(value, scr, inner, put):
    outer = value.shape[0] // inner
    pitch = scr.shape[1] // outer
    for k in range(scr.shape[0]):
        for b in range(outer):
            scr[k, pl.ds(b * pitch, inner), :] = value[b * inner:(b + 1) * inner, 128 * k:128 * (k + 1)]
    for c in range(inner):
        for k in range(scr.shape[0]):
            put(c, k, scr[k, pl.ds(c, outer, stride=pitch), :].astype(BF16))


def pack_slots(send_ref, mask_ref, edge_ref, mesh_ref, lanes, table, lon, grid_cols):
    nodes, per_node = send_ref.shape
    bits = grid_cols.bit_length() - 1
    send = send_ref[...]
    row = lax.shift_right_logical(send, bits).astype(F32)
    col = (send & (grid_cols - 1)).astype(F32)
    mask = mask_ref[...].astype(F32)
    mesh = mesh_ref[...].astype(F32)
    pieces = []
    for n in range(nodes):
        here = slice(n, n + 1)
        lanes[...] = jnp.zeros_like(lanes)
        lanes[0:4, 0:per_node] = edge_ref[n].astype(F32)
        lanes[4:5, 0:per_node] = row[here]
        lanes[5:6, 0:per_node] = col[here]
        lanes[6:7, 0:per_node] = mask[here]
        lanes[7:8, 0:per_node] = jnp.full((1, per_node), n, F32) + (lon * nodes).astype(F32)
        lanes[8:11, 0:per_node] = jnp.broadcast_to(mesh[:, here], (3, per_node))
        pieces.append(lanes[...])
    for p in range(nodes // 2):
        table[:, 128 * p:128 * (p + 1)] = pieces[p] + pltpu.roll(pieces[p + nodes // 2], 64, 1)


def idle_kernel(out_ref):
    out_ref[...] = jnp.zeros_like(out_ref)


def idle_call():
    return pl.pallas_call(
        idle_kernel,
        out_shape=jax.ShapeDtypeStruct((8, 128), F32),
        compiler_params=pltpu.CompilerParams(vmem_limit_bytes=PACK_VMEM),
        cost_estimate=pl.CostEstimate(flops=PACK_FLOPS, transcendentals=0, bytes_accessed=PACK_BYTES),
        name='idle',
    )()


def pack_kernel(send_ref, mask_ref, edge_ref, mesh_ref, dep_ref, wm_ref, wo_ref, bg_ref, out_ref, vm_ref, lanes, table, *, grid_cols):
    pack_slots(send_ref, mask_ref, edge_ref, mesh_ref, lanes, table, lax.axis_index('lon'), grid_cols)
    out_ref[...] = table[...].astype(BF16)
    latent = wo_ref.shape[-1]
    nodes = mesh_ref.shape[1]
    feat = jnp.concatenate([mesh_ref[...].astype(F32), jnp.zeros((nodes - 3, nodes), F32)], axis=0)
    weight = jnp.concatenate([wm_ref[...].astype(F32), jnp.zeros((nodes - 3, latent), F32)], axis=0)
    pre = lax.dot_general(
        feat.astype(BF16), weight.astype(BF16), (((0,), (0,)), ((), ())), preferred_element_type=F32)
    bg1 = bg_ref[1]
    vm_ref[...] = mlp_tail(pre + bg1[0:1], wo_ref[1], bg1).astype(BF16).astype(F32)


def pack_call(senders, edge_mask, edge_t, mesh_t, dep, w_mesh, w_out, bias_gain, grid_cols):
    width = senders.shape[0] // 2 * 128
    latent = w_out.shape[-1]
    return pl.pallas_call(
        functools.partial(pack_kernel, grid_cols=grid_cols),
        out_shape=[jax.ShapeDtypeStruct((FEATS, width), BF16), jax.ShapeDtypeStruct((senders.shape[0], latent), F32)],
        scratch_shapes=[pltpu.VMEM((FEATS, 128), F32), pltpu.VMEM((FEATS, width), F32)],
        compiler_params=pltpu.CompilerParams(vmem_limit_bytes=PACK_VMEM),
        cost_estimate=pl.CostEstimate(flops=PACK_FLOPS, transcendentals=0, bytes_accessed=PACK_BYTES),
        name='pack',
    )(senders, edge_mask, edge_t, mesh_t, dep, w_mesh, w_out, bias_gain)


def rank_slots(vtb, lon, cols, nodes):
    slots = vtb.shape[1]
    chunks = slots // 128
    vt = vtb.astype(F32)
    col = vt[5:6] - (lon * cols).astype(F32)
    cell = vt[7:8] - (lon * nodes).astype(F32)
    inner = (cell > -0.5) & (cell < nodes - 0.5)
    live = (vt[6:7] > 0.5) & (col > -0.5) & (col < cols - 0.5)
    up = lax.broadcasted_iota(jnp.int32, (128, 128), 0) <= lax.broadcasted_iota(jnp.int32, (128, 128), 1)
    low = lax.broadcasted_iota(jnp.int32, (chunks, chunks), 1) < lax.broadcasted_iota(jnp.int32, (chunks, chunks), 0)
    up = jnp.where(up, 1.0, 0.0).astype(BF16)
    low = jnp.where(low, 1.0, 0.0).astype(BF16)
    ones = jnp.full((chunks, chunks), 1.0, BF16)

    def count(flag):
        flag = jnp.where(flag, 1.0, 0.0)
        flags = jnp.concatenate([flag[:, 128 * c:128 * (c + 1)] for c in range(chunks)], axis=0)
        incl = mm(flags.astype(BF16), up)
        row_sum = jnp.broadcast_to(incl[:, 127:128], (chunks, 128)).astype(BF16)
        return flags, incl + mm(low, row_sum) - 1.0, mm(ones, row_sum)

    far, far_rank, n_far = count(live & jnp.logical_not(inner))
    near, near_rank, n_near = count(live & inner)
    skip = jnp.floor((n_far + (TILE - 1)) * (1.0 / TILE)) * TILE
    rank = jnp.where(far > 0.5, far_rank, jnp.where(near > 0.5, near_rank + skip, -1.0))
    return rank, n_far, skip + n_near


def embed_kernel(x_ref, wg_ref, wo_ref, bg_ref, feat_ref, own_vm_ref,
                 vg_ref, tab_ref, band_ref, rank_ref, vm_ref,
                 scr, half, from_south, from_north, feat_in, vm_in, up_sems, down_sems, feat_send, feat_recv, vm_send, vm_recv, *, lats, lons):
    batch, grid_rows, cols, chans = x_ref.shape
    latent = vg_ref.shape[-1]
    lat = lax.axis_index('lat')
    lon = lax.axis_index('lon')
    odd = lax.rem(lat, 2)
    inner_north = lat > 0
    inner_south = lat < lats - 1
    mesh_id = pl.DeviceIdType.MESH

    def strip(start, dst, sems, to):
        return pltpu.make_async_remote_copy(
            tab_ref.at[pl.ds(start, REACH)], dst, sems.at[0], sems.at[1], device_id={'lat': to}, device_id_type=mesh_id)

    north_send = strip(REACH, from_south, up_sems, lat - 1)
    south_send = strip(grid_rows, from_north, down_sems, lat + 1)
    feats = [pltpu.make_async_remote_copy(
        feat_ref, feat_in.at[lon], feat_send.at[k - 1], feat_recv.at[k - 1],
        device_id={'lon': lax.rem(lon + k, lons)}, device_id_type=mesh_id) for k in range(1, lons)]
    feats += [pltpu.make_async_remote_copy(
        own_vm_ref, vm_in.at[lon], vm_send.at[k - 1], vm_recv.at[k - 1],
        device_id={'lon': lax.rem(lon + k, lons)}, device_id_type=mesh_id) for k in range(1, lons)]

    barrier = pltpu.get_barrier_semaphore()
    for k in range(1, lons):
        pl.semaphore_signal(barrier, 1, device_id={'lon': lax.rem(lon + k, lons)}, device_id_type=mesh_id)

    @pl.when(inner_north)
    def _():
        pl.semaphore_signal(barrier, 1, device_id={'lat': lat - 1}, device_id_type=mesh_id)

    @pl.when(inner_south)
    def _():
        pl.semaphore_signal(barrier, 1, device_id={'lat': lat + 1}, device_id_type=mesh_id)

    feat_in[lon] = feat_ref[...]
    vm_in[lon] = own_vm_ref[...]
    half[...] = wg_ref[...] * jnp.asarray(0.5, BF16)
    bg = bg_ref[0]
    b1 = bg[0:1] * 0.5

    def row(i):
        return i + odd * (grid_rows - 1 - 2 * i)

    def first(i):
        return gate(mm(x_ref[:, row(i)].reshape(batch * cols, chans), half[...]) + b1)

    def second(i, hid):
        vg = norm(mm(hid, wo_ref[0]) + bg[1:2]) * bg[2:3] + bg[3:4]
        vg_ref[:, row(i)] = vg.astype(BF16).reshape(batch, cols, latent)

        def put(c, k, part):
            tab_ref[REACH + row(i), c, :, 128 * k:128 * (k + 1)] = part

        swap_rows(vg, scr.at[i % scr.shape[0]], cols, put)

    staged(range(REACH), first, second)
    pl.semaphore_wait(barrier, lons - 1 + inner_north.astype(jnp.int32) + inner_south.astype(jnp.int32))

    @pl.when(inner_north & (odd == 0))
    def _():
        north_send.start()

    @pl.when(inner_south & (odd == 1))
    def _():
        south_send.start()

    for copy in feats:
        copy.start()
    middle = grid_rows // 2
    staged(list(range(grid_rows - REACH, grid_rows)) + list(range(REACH, middle)), first, second)

    @pl.when(inner_north & (odd == 1))
    def _():
        north_send.start()

    @pl.when(inner_south & (odd == 0))
    def _():
        south_send.start()

    def extra():
        band_ref[...] = feat_in[...]
        vtb = jnp.concatenate([feat_in[k] for k in range(lons)], axis=1)
        nodes = 2 * (feat_in.shape[2] // 128)
        rank, n_far, end = rank_slots(vtb, lon, cols, nodes)
        rank_ref[0:rank.shape[0]] = rank
        rank_ref[rank.shape[0]:rank.shape[0] + 8] = n_far[0:8]
        rank_ref[rank.shape[0] + 8:] = end[0:8]
        vm_ref[...] = vm_in[...].reshape(lons * nodes, latent)

    for copy in feats:
        copy.wait()
    staged(range(middle, grid_rows - REACH), first, second, extra)

    @pl.when(inner_north)
    def _():
        north_send.wait_send()
        south_send.wait_recv()
        tab_ref[0:REACH] = from_north[...]

    @pl.when(inner_south)
    def _():
        south_send.wait_send()
        north_send.wait_recv()
        tab_ref[grid_rows + REACH:grid_rows + 2 * REACH] = from_south[...]


def embed_call(grid_in, w_grid, w_out, bias_gain, feats, own_vm, lats, lons):
    batch, rows, cols, chans = grid_in.shape
    latent = w_out.shape[-1]
    strip = (REACH, cols, batch, latent)
    local = pl.BlockSpec(memory_space=pltpu.VMEM)
    return pl.pallas_call(
        functools.partial(embed_kernel, lats=lats, lons=lons),
        in_specs=[local] * 6,
        out_specs=[local] * 5,
        out_shape=[
            jax.ShapeDtypeStruct((batch, rows, cols, latent), BF16),
            jax.ShapeDtypeStruct((rows + 2 * REACH, cols, batch, latent), BF16),
            jax.ShapeDtypeStruct((lons,) + feats.shape, BF16),
            jax.ShapeDtypeStruct((lons * feats.shape[1] // 128 + 16, 128), F32),
            jax.ShapeDtypeStruct((lons * feats.shape[1] // 64, latent), F32)],
        scratch_shapes=[
            pltpu.VMEM((4, latent // 128, batch * (cols + 8), 128), F32),
            pltpu.VMEM((chans, latent), BF16),
            pltpu.VMEM(strip, BF16), pltpu.VMEM(strip, BF16),
            pltpu.VMEM((lons,) + feats.shape, BF16), pltpu.VMEM((lons,) + own_vm.shape, F32),
            pltpu.SemaphoreType.DMA((2,)), pltpu.SemaphoreType.DMA((2,)),
            pltpu.SemaphoreType.DMA((lons - 1,)), pltpu.SemaphoreType.DMA((lons - 1,)),
            pltpu.SemaphoreType.DMA((lons - 1,)), pltpu.SemaphoreType.DMA((lons - 1,))],
        compiler_params=pltpu.CompilerParams(collective_id=0, has_side_effects=True, vmem_limit_bytes=GRID_VMEM),
        cost_estimate=pl.CostEstimate(
            flops=4 * rows * batch * cols * latent * latent, transcendentals=0,
            bytes_accessed=6 * rows * batch * cols * latent),
        name='embed',
    )(grid_in, w_grid, w_out, bias_gain, feats, own_vm)


def staged(items, first, second, extra=None):
    items = list(items)
    hid = first(items[0])
    if extra is not None:
        extra()
    for k, item in enumerate(items):
        nxt = first(items[k + 1]) if k + 1 < len(items) else None
        second(item, hid)
        hid = nxt


def update_kernel(vg_ref, wu_ref, wo_ref, bg_ref, dep_ref, out_ref, half, obuf, sems):
    half[...] = wu_ref[...] * jnp.asarray(0.5, BF16)
    bg = bg_ref[5]
    b1 = bg[0:1] * 0.5
    count = vg_ref.shape[0] // SUB

    def rows(i):
        return pl.ds(i * SUB, SUB)

    def put(i):
        return pltpu.make_async_copy(obuf.at[rows(i)], out_ref.at[rows(i)], sems.at[i])

    def first(i):
        return gate(mm(vg_ref[rows(i), :], half[...]) + b1)

    def second(i, hid):
        upd = norm(mm(hid, wo_ref[5]) + bg[1:2]) * bg[2:3] + bg[3:4]
        obuf[rows(i), :] = (vg_ref[rows(i), :].astype(F32) + upd).astype(BF16)
        if i:
            put(i - 1).start()

    staged(range(count), first, second)
    put(count - 1).start()
    for i in range(count):
        put(i).wait()


def update_call(vg, w_gupd, w_out, bias_gain, dep):
    rows, latent = vg.shape
    local = pl.BlockSpec(memory_space=pltpu.VMEM)
    anywhere = pl.BlockSpec(memory_space=pl.ANY)
    return pl.pallas_call(
        update_kernel,
        in_specs=[local] * 4 + [anywhere],
        out_specs=anywhere,
        out_shape=jax.ShapeDtypeStruct(vg.shape, BF16),
        scratch_shapes=[pltpu.VMEM((latent, latent), BF16), pltpu.VMEM(vg.shape, BF16), pltpu.SemaphoreType.DMA((rows // SUB,))],
        cost_estimate=pl.CostEstimate(flops=4 * rows * latent * latent, transcendentals=0, bytes_accessed=4 * rows * latent),
        compiler_params=pltpu.CompilerParams(vmem_limit_bytes=UPDATE_VMEM),
        name='update',
    )(vg, w_gupd, w_out, bias_gain, dep)


def spread(ref, base, count, reps):
    rows = []
    for s in range(count):
        row = jnp.concatenate([ref[k, pl.ds(base + s, 8, stride=0), :] for k in range(ref.shape[0])], axis=1)
        rows += [row] * reps
    return jnp.concatenate(rows, axis=0)


def put_lanes(ref, rows, value):
    for k in range(ref.shape[0]):
        ref[k, rows, :] = value[:, 128 * k:128 * (k + 1)]


def message_loop(start, stop, tab_ref, w_in, w3, bg3, lp, ec, idx, part, bufs, hids):
    rows, cols, batch, latent = tab_ref.shape
    table = tab_ref.reshape(rows * cols, batch, latent)
    per = TILE // 2
    b2 = bg3[1:2]
    gain = bg3[2:3]

    def first(base, k):
        for s in range(per):
            bufs[k % 2][pl.ds(s * batch, batch), :] = table[lax.div(idx[0, base + s], CODE)]
        acc = mm(bufs[k % 2][...], w_in[...])
        hids[k][...] = gate(acc + spread(lp, base, per, batch // 8))

    def second(base, k):
        y = mm(hids[k][...], w3[...]) + b2
        z = norm(y) * gain + spread(ec, base, per, batch // 8)
        z = z.astype(BF16).astype(F32).reshape(per, batch, latent)
        for s in range(per):
            n = lax.rem(idx[0, base + s], CODE)
            part[n] += z[s]

    def both(t, k, stage):
        for j in range(2):
            stage(t * TILE + j * per, 2 * k + j)

    def mixed(t1, k1, t2, k2):
        for j in range(2):
            first(t1 * TILE + j * per, 2 * k1 + j)
            second(t2 * TILE + j * per, 2 * k2 + j)

    @pl.when(stop > start)
    def _():
        both(start, 0, first)

    def step(m, carry):
        t = start + 2 * m
        mixed(t + 1, 1, t, 0)
        mixed(jnp.minimum(t + 2, stop - 1), 0, t + 1, 1)
        return carry

    lax.fori_loop(0, lax.div(stop - start, 2), step, 0)

    @pl.when(lax.rem(stop - start, 2) == 1)
    def _():
        both(stop - 1, 0, second)


def three_parts(x):
    hi = x.astype(BF16)
    rest = x - hi.astype(F32)
    mid = rest.astype(BF16)
    return jnp.concatenate([hi, mid, (rest - mid.astype(F32)).astype(BF16)], axis=0)


def select(rank, base):
    slot = lax.broadcasted_iota(jnp.int32, (PREP, 128), 0).astype(F32) + base
    return jnp.concatenate(
        [jnp.where(rank[c:c + 1] == slot, 1.0, 0.0).astype(BF16) for c in range(rank.shape[0])], axis=1)


def prepare(start, stop, rank, vtb, we_ref, wmsg_ref, wo_ref, bg_ref, node_proj, lp, ec):
    latent = wo_ref.shape[-1]
    band = node_proj.shape[0] // 3
    we = jnp.concatenate([we_ref[...].astype(F32), jnp.zeros((FEATS - 4, latent), F32)], axis=0).astype(BF16)
    bg2 = bg_ref[2]
    bg3 = bg_ref[3]

    def prep(t, carry):
        feat = mm_nt(select(rank, (t * PREP).astype(F32)), vtb).astype(BF16)
        here = pl.ds(pl.multiple_of(t * PREP, PREP), PREP)
        edge = mlp_tail(mm(feat, we) + bg2[0:1], wo_ref[2], bg2).astype(BF16)
        lane = lax.rem(lax.broadcasted_iota(jnp.int32, (PREP, 3 * band), 1), band).astype(F32)
        hot = jnp.where(lane == feat[:, 7:8].astype(F32), 1.0, 0.0).astype(BF16)
        put_lanes(lp, here, (mm(edge, wmsg_ref[0:latent, :]) + mm(hot, node_proj[...]) + bg3[0:1]) * 0.5)
        put_lanes(ec, here, edge.astype(F32) + bg3[3:4])
        return carry

    lax.fori_loop(start, stop, prep, 0)


def far_kernel(v_ref, rank_ref, vm_ref, we_ref, wmsg_ref, wo_ref, bg_ref, tab_ref,
               p1_ref, p2_ref, p3_ref, idx_v, proj_ref,
               lp, ec, idx_s, part, half, hid_a, hid_b, hid_c, hid_d, buf_a, buf_b, isem, *, lons, nodes):
    latent = wo_ref.shape[-1]
    grid_rows, cols = tab_ref.shape[:2]
    positions = grid_rows * cols
    cell_rows = grid_rows - 2 * REACH
    band = lons * nodes
    chunks = rank_ref.shape[0] - 16
    meta = idx_v.shape[1] - 128
    lat = lax.axis_index('lat')
    lon = lax.axis_index('lon')
    vtb = jnp.concatenate([v_ref[k] for k in range(lons)], axis=1)
    rank = rank_ref[0:chunks]
    n_far = jnp.max(rank_ref[chunks:chunks + 8]).astype(jnp.int32)
    end = jnp.max(rank_ref[chunks + 8:]).astype(jnp.int32)
    far_tiles = lax.div(n_far + TILE - 1, TILE)
    skip = far_tiles * TILE
    proj_ref[...] = three_parts(mm(vm_ref[...].astype(BF16), wmsg_ref[2 * latent:, :]))

    def index(t, carry):
        feat_t = mm_nt(vtb, select(rank, (t * PREP).astype(F32)))
        here = pl.ds(pl.multiple_of(t * PREP, PREP), PREP)
        slot = lax.broadcasted_iota(jnp.int32, (1, PREP), 1) + t * PREP
        used = (slot < n_far) | ((slot >= skip) & (slot < end))
        win_r = feat_t[4:5] - (lat * cell_rows - REACH).astype(F32)
        win_c = feat_t[5:6] - (lon * cols).astype(F32)
        pos = jnp.clip(jnp.where(used, (win_r * cols + win_c).astype(jnp.int32), REACH * cols), 0, positions - 1)
        node = feat_t[7:8].astype(jnp.int32)
        cell = lax.div(node, nodes)
        rel = jnp.where(used, jnp.bitwise_xor(cell, lon) * nodes + (node - cell * nodes), band)
        idx_v[0:1, here] = pos * CODE + rel
        return carry

    lax.fori_loop(0, lax.div(end + PREP - 1, PREP), index, 0)
    lane = lax.broadcasted_iota(jnp.int32, (1, 128), 1)
    idx_v[0:1, meta:meta + 128] = jnp.where(lane == 0, far_tiles, lax.div(end + TILE - 1, TILE))
    move = pltpu.make_async_copy(idx_v, idx_s, isem)
    move.start()
    part[...] = jnp.zeros_like(part)
    half[...] = wmsg_ref[latent:2 * latent, :] * jnp.asarray(0.5, BF16)
    prepare(0, lax.div(skip + PREP - 1, PREP), rank, vtb, we_ref, wmsg_ref, wo_ref, bg_ref, proj_ref, lp, ec)
    move.wait()
    message_loop(0, far_tiles, tab_ref, half, wo_ref.at[3], bg_ref[3], lp, ec, idx_s, part, (buf_a, buf_b), (hid_a, hid_b, hid_c, hid_d))
    for k, ref in enumerate((p1_ref, p2_ref, p3_ref)):
        ref[...] = part[(k + 1) * nodes:(k + 2) * nodes]


def near_kernel(idx, v_ref, rank_ref, proj_ref, we_ref, wmsg_ref, wo_ref, bg_ref, tab_ref, own_ref, lp, ec, part, half, hid_a, hid_b, hid_c, hid_d, buf_a, buf_b):
    latent = wo_ref.shape[-1]
    nodes = own_ref.shape[0]
    part[...] = jnp.zeros_like(part)
    half[...] = wmsg_ref[latent:2 * latent, :] * jnp.asarray(0.5, BF16)
    vtb = jnp.concatenate([v_ref[k] for k in range(v_ref.shape[0])], axis=1)
    meta = idx.shape[1] - 128
    start, stop = idx[0, meta], idx[0, meta + 1]
    ratio = PREP // TILE
    prepare(lax.div(start, ratio), lax.div(stop + ratio - 1, ratio), rank_ref[0:rank_ref.shape[0] - 16], vtb, we_ref, wmsg_ref, wo_ref, bg_ref,
            proj_ref, lp, ec)
    message_loop(start, stop, tab_ref, half, wo_ref.at[3], bg_ref[3], lp, ec, idx, part,
                 (buf_a, buf_b), (hid_a, hid_b, hid_c, hid_d))
    own_ref[...] = part[0:nodes]


def loop_scratch(batch, latent):
    half_tile = pltpu.VMEM((TILE // 2 * batch, latent), BF16)
    return [pltpu.VMEM((latent, latent), BF16)] + [half_tile] * 6


def edge_call(v, rank, vm, w_edge, w_msg, w_out, bias_gain, table, lons, nodes, per_node):
    latent = w_out.shape[-1]
    batch = table.shape[2]
    limit = lons * nodes * per_node + PREP + 128
    local = pl.BlockSpec(memory_space=pltpu.VMEM)
    outs = [jax.ShapeDtypeStruct((nodes, batch, latent), F32)] * (lons - 1)
    outs += [jax.ShapeDtypeStruct((1, limit), jnp.int32), jax.ShapeDtypeStruct((3 * lons * nodes, latent), BF16)]
    res = pl.pallas_call(
        functools.partial(far_kernel, lons=lons, nodes=nodes),
        in_specs=[local] * 8,
        out_specs=[local] * len(outs),
        out_shape=outs,
        scratch_shapes=[
            pltpu.VMEM((latent // 128, limit, 128), F32), pltpu.VMEM((latent // 128, limit, 128), F32),
            pltpu.SMEM((1, limit), jnp.int32),
            pltpu.VMEM((lons * nodes + 1, batch, latent), F32)] + loop_scratch(batch, latent) + [pltpu.SemaphoreType.DMA],
        compiler_params=pltpu.CompilerParams(vmem_limit_bytes=EDGE_VMEM),
        cost_estimate=pl.CostEstimate(
            flops=4 * limit // 8 * batch * latent * latent, transcendentals=0, bytes_accessed=limit * batch * latent),
        name='edges_far',
    )(v, rank, vm, w_edge, w_msg, w_out, bias_gain, table)
    return res[:lons - 1], res[lons - 1:]


def near_call(v, rank, lists, w_edge, w_msg, w_out, bias_gain, table, nodes, band):
    idx, proj = lists
    latent = w_out.shape[-1]
    batch = table.shape[2]
    local = pl.BlockSpec(memory_space=pltpu.VMEM)
    return pl.pallas_call(
        near_kernel,
        in_specs=[pl.BlockSpec(memory_space=pltpu.SMEM)] + [local] * 8,
        out_specs=[local],
        out_shape=[jax.ShapeDtypeStruct((nodes, batch, latent), F32)],
        scratch_shapes=[pltpu.VMEM((latent // 128, idx.shape[1], 128), F32), pltpu.VMEM((latent // 128, idx.shape[1], 128), F32),
                        pltpu.VMEM((band + 1, batch, latent), F32)] + loop_scratch(batch, latent),
        compiler_params=pltpu.CompilerParams(vmem_limit_bytes=EDGE_VMEM),
        cost_estimate=pl.CostEstimate(
            flops=idx.shape[1] * batch * latent * latent, transcendentals=0, bytes_accessed=idx.shape[1] * batch * latent),
        name='edges_near',
    )(idx, v, rank, proj, w_edge, w_msg, w_out, bias_gain, table)


def node_kernel(own_ref, r1_ref, r2_ref, r3_ref, vm_ref, wn_ref, w4_ref, bg_ref, out_ref, scr):
    nodes, batch, latent = own_ref.shape
    agg = (own_ref[...] + r1_ref[...] + r2_ref[...] + r3_ref[...]).astype(BF16).reshape(nodes * batch, latent)
    bg = bg_ref[4]
    own_vm = vm_ref[...]
    base = mm(own_vm.astype(BF16), wn_ref[0:latent, :]) + bg[0:1]
    acc = mm(agg, wn_ref[latent:, :]).reshape(nodes, batch, latent) + base.reshape(nodes, 1, latent)
    upd = mlp_tail(acc.reshape(nodes * batch, latent), w4_ref[4], bg)
    out = (upd.reshape(nodes, batch, latent) + own_vm.reshape(nodes, 1, latent)).reshape(nodes * batch, latent)

    def put(b, k, part):
        out_ref[b, :, 128 * k:128 * (k + 1)] = part

    swap_rows(out, scr, batch, put)


def node_call(blocks, vm, w_node, w_out, bias_gain):
    nodes, batch, latent = blocks[0].shape
    local = pl.BlockSpec(memory_space=pltpu.VMEM)
    out = jax.ShapeDtypeStruct((batch, nodes, latent), BF16)
    return pl.pallas_call(
        node_kernel,
        in_specs=[local] * 8,
        out_specs=local,
        out_shape=out,
        compiler_params=pltpu.CompilerParams(vmem_limit_bytes=NODE_VMEM),
        scratch_shapes=[pltpu.VMEM((latent // 128, nodes * (batch + 8), 128), F32)],
        name='nodes',
    )(*blocks, vm, w_node, w_out, bias_gain)


def solution(mesh):
    lats = mesh.shape['lat']
    lons = mesh.shape['lon']
    south_shift = [(s, s + 1) for s in range(lats - 1)]
    north_shift = [(s + 1, s) for s in range(lats - 1)]

    def cell_step(grid_in, mesh_in, edge_in, senders, edge_mask, w_grid, w_mesh, w_edge, w_msg, w_node, w_gupd, w_out, bias_gain):
        batch, rows, cols, _ = grid_in.shape
        nodes = senders.shape[0]
        latent = w_out.shape[-1]
        feats, own_vm = pack_call(
            senders, edge_mask, jnp.swapaxes(edge_in, 1, 2), mesh_in.T, idle_call(), w_mesh, w_out, bias_gain, cols * lons)
        vg, table, band, rank, vm = embed_call(grid_in, w_grid, w_out, bias_gain, feats, own_vm, lats, lons)
        blocks, lists = edge_call(band, rank, vm, w_edge, w_msg, w_out, bias_gain, table, lons, *senders.shape)
        own, = near_call(band, rank, lists, w_edge, w_msg, w_out, bias_gain, table, nodes, nodes * lons)
        pairs = lambda k, polar: [
            (j * lats + i, (j ^ k) * lats + i) for i in range(lats) for j in range(lons)
            if not polar or i in (0, lats - 1)]
        got = [lax.ppermute(blocks[k - 1], ('lon', 'lat'), pairs(k, k == 2)) for k in (3, 2, 1)]
        mesh_out = node_call([own] + got, own_vm, w_node, w_out, bias_gain)
        flat = update_call(vg.reshape(batch * rows * cols, latent), w_gupd, w_out, bias_gain, own)
        grid_out = flat.reshape(batch, rows, cols, latent)
        return mesh_out, grid_out

    grid_spec = P('dp', 'lat', 'lon', None)
    node_spec = P(('lat', 'lon'), None)
    slot_spec = P(('lat', 'lon'), None, None)
    in_specs = (grid_spec, node_spec, slot_spec, node_spec, node_spec) + (P(),) * 8
    out_specs = (P('dp', ('lat', 'lon'), None), grid_spec)
    return jax.shard_map(cell_step, mesh=mesh, in_specs=in_specs, out_specs=out_specs, check_vma=False)
```

```python
import functools

import jax
import jax.numpy as jnp
from jax import lax
from jax.experimental import pallas as pl
from jax.experimental.pallas import tpu as pltpu
from jax.sharding import PartitionSpec as P

REACH = 3
LN_EPS = 1e-5
FEATS = 16
TILE = 32
SUB = 256
LP = None
PREP = 128
CODE = 64
PACK_VMEM = 40 * 2 ** 20
PACK_FLOPS = 2 * 10 ** 9
PACK_BYTES = 10 ** 6
EDGE_VMEM = 20 * 2 ** 20
NODE_VMEM = 6 * 2 ** 20
GRID_VMEM = 24 * 2 ** 20
UPDATE_VMEM = 12 * 2 ** 20
F32 = jnp.float32
BF16 = jnp.bfloat16


def mm(a, b):
    return jnp.dot(a, b, preferred_element_type=F32)


def mm_nt(a, b):
    return lax.dot_general(a, b, (((1,), (1,)), ((), ())), preferred_element_type=F32)


def gate(t):
    return (t + t * jnp.tanh(t)).astype(BF16)


def swish(x):
    return gate(x * 0.5)


def norm(y):
    scale = 1.0 / y.shape[-1]
    centered = y - jnp.sum(y, axis=-1, keepdims=True) * scale
    var = jnp.sum(centered * centered, axis=-1, keepdims=True) * scale
    return centered * lax.rsqrt(var + LN_EPS)


def mlp_tail(pre, w2, bg):
    y = mm(swish(pre), w2) + bg[1:2]
    return norm(y) * bg[2:3] + bg[3:4]


def swap_rows(value, scr, inner, put):
    outer = value.shape[0] // inner
    pitch = scr.shape[1] // outer
    for k in range(scr.shape[0]):
        for b in range(outer):
            scr[k, pl.ds(b * pitch, inner), :] = value[b * inner:(b + 1) * inner, 128 * k:128 * (k + 1)]
    for c in range(inner):
        for k in range(scr.shape[0]):
            put(c, k, scr[k, pl.ds(c, outer, stride=pitch), :].astype(BF16))


def pack_slots(send_ref, mask_ref, edge_ref, mesh_ref, lanes, table, lon, grid_cols):
    nodes, per_node = send_ref.shape
    bits = grid_cols.bit_length() - 1
    send = send_ref[...]
    row = lax.shift_right_logical(send, bits).astype(F32)
    col = (send & (grid_cols - 1)).astype(F32)
    mask = mask_ref[...].astype(F32)
    mesh = mesh_ref[...].astype(F32)
    pieces = []
    for n in range(nodes):
        here = slice(n, n + 1)
        lanes[...] = jnp.zeros_like(lanes)
        lanes[0:4, 0:per_node] = edge_ref[n].astype(F32)
        lanes[4:5, 0:per_node] = row[here]
        lanes[5:6, 0:per_node] = col[here]
        lanes[6:7, 0:per_node] = mask[here]
        lanes[7:8, 0:per_node] = jnp.full((1, per_node), n, F32) + (lon * nodes).astype(F32)
        lanes[8:11, 0:per_node] = jnp.broadcast_to(mesh[:, here], (3, per_node))
        pieces.append(lanes[...])
    for p in range(nodes // 2):
        table[:, 128 * p:128 * (p + 1)] = pieces[p] + pltpu.roll(pieces[p + nodes // 2], 64, 1)


def idle_kernel(out_ref):
    out_ref[...] = jnp.zeros_like(out_ref)


def idle_call():
    return pl.pallas_call(
        idle_kernel,
        out_shape=jax.ShapeDtypeStruct((8, 128), F32),
        compiler_params=pltpu.CompilerParams(vmem_limit_bytes=PACK_VMEM),
        cost_estimate=pl.CostEstimate(flops=PACK_FLOPS, transcendentals=0, bytes_accessed=PACK_BYTES),
        name='idle',
    )()


def pack_kernel(send_ref, mask_ref, edge_ref, mesh_ref, dep_ref, wm_ref, wo_ref, bg_ref, out_ref, vm_ref, lanes, table, *, grid_cols):
    pack_slots(send_ref, mask_ref, edge_ref, mesh_ref, lanes, table, lax.axis_index('lon'), grid_cols)
    out_ref[...] = table[...].astype(BF16)
    latent = wo_ref.shape[-1]
    nodes = mesh_ref.shape[1]
    feat = jnp.concatenate([mesh_ref[...].astype(F32), jnp.zeros((nodes - 3, nodes), F32)], axis=0)
    weight = jnp.concatenate([wm_ref[...].astype(F32), jnp.zeros((nodes - 3, latent), F32)], axis=0)
    pre = lax.dot_general(
        feat.astype(BF16), weight.astype(BF16), (((0,), (0,)), ((), ())), preferred_element_type=F32)
    bg1 = bg_ref[1]
    vm_ref[...] = mlp_tail(pre + bg1[0:1], wo_ref[1], bg1).astype(BF16).astype(F32)


def pack_call(senders, edge_mask, edge_t, mesh_t, dep, w_mesh, w_out, bias_gain, grid_cols):
    width = senders.shape[0] // 2 * 128
    latent = w_out.shape[-1]
    return pl.pallas_call(
        functools.partial(pack_kernel, grid_cols=grid_cols),
        out_shape=[jax.ShapeDtypeStruct((FEATS, width), BF16), jax.ShapeDtypeStruct((senders.shape[0], latent), F32)],
        scratch_shapes=[pltpu.VMEM((FEATS, 128), F32), pltpu.VMEM((FEATS, width), F32)],
        compiler_params=pltpu.CompilerParams(vmem_limit_bytes=PACK_VMEM),
        cost_estimate=pl.CostEstimate(flops=PACK_FLOPS, transcendentals=0, bytes_accessed=PACK_BYTES),
        name='pack',
    )(senders, edge_mask, edge_t, mesh_t, dep, w_mesh, w_out, bias_gain)


def rank_slots(vtb, lon, cols, nodes):
    slots = vtb.shape[1]
    chunks = slots // 128
    vt = vtb.astype(F32)
    col = vt[5:6] - (lon * cols).astype(F32)
    cell = vt[7:8] - (lon * nodes).astype(F32)
    inner = (cell > -0.5) & (cell < nodes - 0.5)
    live = (vt[6:7] > 0.5) & (col > -0.5) & (col < cols - 0.5)
    up = lax.broadcasted_iota(jnp.int32, (128, 128), 0) <= lax.broadcasted_iota(jnp.int32, (128, 128), 1)
    low = lax.broadcasted_iota(jnp.int32, (chunks, chunks), 1) < lax.broadcasted_iota(jnp.int32, (chunks, chunks), 0)
    up = jnp.where(up, 1.0, 0.0).astype(BF16)
    low = jnp.where(low, 1.0, 0.0).astype(BF16)
    ones = jnp.full((chunks, chunks), 1.0, BF16)

    def count(flag):
        flag = jnp.where(flag, 1.0, 0.0)
        flags = jnp.concatenate([flag[:, 128 * c:128 * (c + 1)] for c in range(chunks)], axis=0)
        incl = mm(flags.astype(BF16), up)
        row_sum = jnp.broadcast_to(incl[:, 127:128], (chunks, 128)).astype(BF16)
        return flags, incl + mm(low, row_sum) - 1.0, mm(ones, row_sum)

    far, far_rank, n_far = count(live & jnp.logical_not(inner))
    near, near_rank, n_near = count(live & inner)
    skip = jnp.floor((n_far + (TILE - 1)) * (1.0 / TILE)) * TILE
    rank = jnp.where(far > 0.5, far_rank, jnp.where(near > 0.5, near_rank + skip, -1.0))
    return rank, n_far, skip + n_near


def embed_kernel(x_ref, wg_ref, wo_ref, bg_ref, feat_ref, own_vm_ref,
                 vg_ref, tab_ref, band_ref, rank_ref, vm_ref,
                 scr, half, from_south, from_north, feat_in, vm_in, up_sems, down_sems, feat_send, feat_recv, vm_send, vm_recv, *, lats, lons):
    batch, grid_rows, cols, chans = x_ref.shape
    latent = vg_ref.shape[-1]
    lat = lax.axis_index('lat')
    lon = lax.axis_index('lon')
    odd = lax.rem(lat, 2)
    inner_north = lat > 0
    inner_south = lat < lats - 1
    mesh_id = pl.DeviceIdType.MESH

    def strip(start, dst, sems, to):
        return pltpu.make_async_remote_copy(
            tab_ref.at[pl.ds(start, REACH)], dst, sems.at[0], sems.at[1], device_id={'lat': to}, device_id_type=mesh_id)

    north_send = strip(REACH, from_south, up_sems, lat - 1)
    south_send = strip(grid_rows, from_north, down_sems, lat + 1)
    feats = [pltpu.make_async_remote_copy(
        feat_ref, feat_in.at[lon], feat_send.at[k - 1], feat_recv.at[k - 1],
        device_id={'lon': lax.rem(lon + k, lons)}, device_id_type=mesh_id) for k in range(1, lons)]
    feats += [pltpu.make_async_remote_copy(
        own_vm_ref, vm_in.at[lon], vm_send.at[k - 1], vm_recv.at[k - 1],
        device_id={'lon': lax.rem(lon + k, lons)}, device_id_type=mesh_id) for k in range(1, lons)]

    barrier = pltpu.get_barrier_semaphore()
    for k in range(1, lons):
        pl.semaphore_signal(barrier, 1, device_id={'lon': lax.rem(lon + k, lons)}, device_id_type=mesh_id)

    @pl.when(inner_north)
    def _():
        pl.semaphore_signal(barrier, 1, device_id={'lat': lat - 1}, device_id_type=mesh_id)

    @pl.when(inner_south)
    def _():
        pl.semaphore_signal(barrier, 1, device_id={'lat': lat + 1}, device_id_type=mesh_id)

    feat_in[lon] = feat_ref[...]
    vm_in[lon] = own_vm_ref[...]
    half[...] = wg_ref[...] * jnp.asarray(0.5, BF16)
    bg = bg_ref[0]
    b1 = bg[0:1] * 0.5

    def row(i):
        return i + odd * (grid_rows - 1 - 2 * i)

    def first(i):
        return gate(mm(x_ref[:, row(i)].reshape(batch * cols, chans), half[...]) + b1)

    def second(i, hid):
        vg = norm(mm(hid, wo_ref[0]) + bg[1:2]) * bg[2:3] + bg[3:4]
        vg_ref[:, row(i)] = vg.astype(BF16).reshape(batch, cols, latent)

        def put(c, k, part):
            tab_ref[REACH + row(i), c, :, 128 * k:128 * (k + 1)] = part

        swap_rows(vg, scr.at[i % scr.shape[0]], cols, put)

    staged(range(REACH), first, second)
    pl.semaphore_wait(barrier, lons - 1 + inner_north.astype(jnp.int32) + inner_south.astype(jnp.int32))

    @pl.when(inner_north & (odd == 0))
    def _():
        north_send.start()

    @pl.when(inner_south & (odd == 1))
    def _():
        south_send.start()

    for copy in feats:
        copy.start()
    middle = grid_rows // 2
    staged(list(range(grid_rows - REACH, grid_rows)) + list(range(REACH, middle)), first, second)

    @pl.when(inner_north & (odd == 1))
    def _():
        north_send.start()

    @pl.when(inner_south & (odd == 0))
    def _():
        south_send.start()

    def extra():
        band_ref[...] = feat_in[...]
        vtb = jnp.concatenate([feat_in[k] for k in range(lons)], axis=1)
        nodes = 2 * (feat_in.shape[2] // 128)
        rank, n_far, end = rank_slots(vtb, lon, cols, nodes)
        rank_ref[0:rank.shape[0]] = rank
        rank_ref[rank.shape[0]:rank.shape[0] + 8] = n_far[0:8]
        rank_ref[rank.shape[0] + 8:] = end[0:8]
        vm_ref[...] = vm_in[...].reshape(lons * nodes, latent)

    for copy in feats:
        copy.wait()
    staged(range(middle, grid_rows - REACH), first, second, extra)

    @pl.when(inner_north)
    def _():
        north_send.wait_send()
        south_send.wait_recv()
        tab_ref[0:REACH] = from_north[...]

    @pl.when(inner_south)
    def _():
        south_send.wait_send()
        north_send.wait_recv()
        tab_ref[grid_rows + REACH:grid_rows + 2 * REACH] = from_south[...]


def embed_call(grid_in, w_grid, w_out, bias_gain, feats, own_vm, lats, lons):
    batch, rows, cols, chans = grid_in.shape
    latent = w_out.shape[-1]
    strip = (REACH, cols, batch, latent)
    local = pl.BlockSpec(memory_space=pltpu.VMEM)
    return pl.pallas_call(
        functools.partial(embed_kernel, lats=lats, lons=lons),
        in_specs=[local] * 6,
        out_specs=[local] * 5,
        out_shape=[
            jax.ShapeDtypeStruct((batch, rows, cols, latent), BF16),
            jax.ShapeDtypeStruct((rows + 2 * REACH, cols, batch, latent), BF16),
            jax.ShapeDtypeStruct((lons,) + feats.shape, BF16),
            jax.ShapeDtypeStruct((lons * feats.shape[1] // 128 + 16, 128), F32),
            jax.ShapeDtypeStruct((lons * feats.shape[1] // 64, latent), F32)],
        scratch_shapes=[
            pltpu.VMEM((4, latent // 128, batch * (cols + 8), 128), F32),
            pltpu.VMEM((chans, latent), BF16),
            pltpu.VMEM(strip, BF16), pltpu.VMEM(strip, BF16),
            pltpu.VMEM((lons,) + feats.shape, BF16), pltpu.VMEM((lons,) + own_vm.shape, F32),
            pltpu.SemaphoreType.DMA((2,)), pltpu.SemaphoreType.DMA((2,)),
            pltpu.SemaphoreType.DMA((lons - 1,)), pltpu.SemaphoreType.DMA((lons - 1,)),
            pltpu.SemaphoreType.DMA((lons - 1,)), pltpu.SemaphoreType.DMA((lons - 1,))],
        compiler_params=pltpu.CompilerParams(collective_id=0, has_side_effects=True, vmem_limit_bytes=GRID_VMEM),
        cost_estimate=pl.CostEstimate(
            flops=4 * rows * batch * cols * latent * latent, transcendentals=0,
            bytes_accessed=6 * rows * batch * cols * latent),
        name='embed',
    )(grid_in, w_grid, w_out, bias_gain, feats, own_vm)


def staged(items, first, second, extra=None):
    items = list(items)
    hid = first(items[0])
    if extra is not None:
        extra()
    for k, item in enumerate(items):
        nxt = first(items[k + 1]) if k + 1 < len(items) else None
        second(item, hid)
        hid = nxt


def update_kernel(vg_ref, wu_ref, wo_ref, bg_ref, dep_ref, out_ref, half, obuf, sems):
    half[...] = wu_ref[...] * jnp.asarray(0.5, BF16)
    bg = bg_ref[5]
    b1 = bg[0:1] * 0.5
    count = vg_ref.shape[0] // SUB

    def rows(i):
        return pl.ds(i * SUB, SUB)

    def put(i):
        return pltpu.make_async_copy(obuf.at[rows(i)], out_ref.at[rows(i)], sems.at[i])

    def first(i):
        return gate(mm(vg_ref[rows(i), :], half[...]) + b1)

    def second(i, hid):
        upd = norm(mm(hid, wo_ref[5]) + bg[1:2]) * bg[2:3] + bg[3:4]
        obuf[rows(i), :] = (vg_ref[rows(i), :].astype(F32) + upd).astype(BF16)
        if i:
            put(i - 1).start()

    staged(range(count), first, second)
    put(count - 1).start()
    for i in range(count):
        put(i).wait()


def update_call(vg, w_gupd, w_out, bias_gain, dep):
    rows, latent = vg.shape
    local = pl.BlockSpec(memory_space=pltpu.VMEM)
    anywhere = pl.BlockSpec(memory_space=pl.ANY)
    return pl.pallas_call(
        update_kernel,
        in_specs=[local] * 4 + [anywhere],
        out_specs=anywhere,
        out_shape=jax.ShapeDtypeStruct(vg.shape, BF16),
        scratch_shapes=[pltpu.VMEM((latent, latent), BF16), pltpu.VMEM(vg.shape, BF16), pltpu.SemaphoreType.DMA((rows // SUB,))],
        cost_estimate=pl.CostEstimate(flops=4 * rows * latent * latent, transcendentals=0, bytes_accessed=4 * rows * latent),
        compiler_params=pltpu.CompilerParams(vmem_limit_bytes=UPDATE_VMEM),
        name='update',
    )(vg, w_gupd, w_out, bias_gain, dep)


def spread(ref, base, count, reps):
    rows = []
    for s in range(count):
        row = jnp.concatenate([ref[k, pl.ds(base + s, 8, stride=0), :] for k in range(ref.shape[0])], axis=1)
        rows += [row] * reps
    return jnp.concatenate(rows, axis=0)


def put_lanes(ref, rows, value):
    for k in range(ref.shape[0]):
        ref[k, rows, :] = value[:, 128 * k:128 * (k + 1)]


def message_loop(start, stop, tab_ref, w_in, w3, bg3, lp, ec, idx, part, bufs, hids):
    rows, cols, batch, latent = tab_ref.shape
    table = tab_ref.reshape(rows * cols, batch, latent)
    per = TILE // 2
    b2 = bg3[1:2]
    gain = bg3[2:3]

    def first(base, k):
        for s in range(per):
            bufs[k % 2][pl.ds(s * batch, batch), :] = table[lax.div(idx[0, base + s], CODE)]
        acc = mm(bufs[k % 2][...], w_in[...])
        hids[k][...] = gate(acc + spread(lp, base, per, batch // 8))

    def second(base, k):
        y = mm(hids[k][...], w3[...]) + b2
        z = norm(y) * gain + spread(ec, base, per, batch // 8)
        z = z.astype(BF16).astype(F32).reshape(per, batch, latent)
        for s in range(per):
            n = lax.rem(idx[0, base + s], CODE)
            part[n] += z[s]

    def both(t, k, stage):
        for j in range(2):
            stage(t * TILE + j * per, 2 * k + j)

    def mixed(t1, k1, t2, k2):
        for j in range(2):
            first(t1 * TILE + j * per, 2 * k1 + j)
            second(t2 * TILE + j * per, 2 * k2 + j)

    @pl.when(stop > start)
    def _():
        both(start, 0, first)

    def step(m, carry):
        t = start + 2 * m
        mixed(t + 1, 1, t, 0)
        mixed(jnp.minimum(t + 2, stop - 1), 0, t + 1, 1)
        return carry

    lax.fori_loop(0, lax.div(stop - start, 2), step, 0)

    @pl.when(lax.rem(stop - start, 2) == 1)
    def _():
        both(stop - 1, 0, second)


def three_parts(x):
    hi = x.astype(BF16)
    rest = x - hi.astype(F32)
    mid = rest.astype(BF16)
    return jnp.concatenate([hi, mid, (rest - mid.astype(F32)).astype(BF16)], axis=0)


def select(rank, base):
    slot = lax.broadcasted_iota(jnp.int32, (PREP, 128), 0).astype(F32) + base
    return jnp.concatenate(
        [jnp.where(rank[c:c + 1] == slot, 1.0, 0.0).astype(BF16) for c in range(rank.shape[0])], axis=1)


def prepare(start, stop, rank, vtb, we_ref, wmsg_ref, wo_ref, bg_ref, node_proj, lp, ec):
    latent = wo_ref.shape[-1]
    band = node_proj.shape[0] // 3
    we = jnp.concatenate([we_ref[...].astype(F32), jnp.zeros((FEATS - 4, latent), F32)], axis=0).astype(BF16)
    bg2 = bg_ref[2]
    bg3 = bg_ref[3]

    def prep(t, carry):
        feat = mm_nt(select(rank, (t * PREP).astype(F32)), vtb).astype(BF16)
        here = pl.ds(pl.multiple_of(t * PREP, PREP), PREP)
        edge = mlp_tail(mm(feat, we) + bg2[0:1], wo_ref[2], bg2).astype(BF16)
        lane = lax.rem(lax.broadcasted_iota(jnp.int32, (PREP, 3 * band), 1), band).astype(F32)
        hot = jnp.where(lane == feat[:, 7:8].astype(F32), 1.0, 0.0).astype(BF16)
        put_lanes(lp, here, (mm(edge, wmsg_ref[0:latent, :]) + mm(hot, node_proj[...]) + bg3[0:1]) * 0.5)
        put_lanes(ec, here, edge.astype(F32) + bg3[3:4])
        return carry

    lax.fori_loop(start, stop, prep, 0)


def far_kernel(v_ref, rank_ref, vm_ref, we_ref, wmsg_ref, wo_ref, bg_ref, tab_ref,
               p1_ref, p2_ref, p3_ref, idx_v, proj_ref,
               lp, ec, idx_s, part, half, hid_a, hid_b, hid_c, hid_d, buf_a, buf_b, isem, *, lons, nodes):
    latent = wo_ref.shape[-1]
    grid_rows, cols = tab_ref.shape[:2]
    positions = grid_rows * cols
    cell_rows = grid_rows - 2 * REACH
    band = lons * nodes
    chunks = rank_ref.shape[0] - 16
    meta = idx_v.shape[1] - 128
    lat = lax.axis_index('lat')
    lon = lax.axis_index('lon')
    vtb = jnp.concatenate([v_ref[k] for k in range(lons)], axis=1)
    rank = rank_ref[0:chunks]
    n_far = jnp.max(rank_ref[chunks:chunks + 8]).astype(jnp.int32)
    end = jnp.max(rank_ref[chunks + 8:]).astype(jnp.int32)
    far_tiles = lax.div(n_far + TILE - 1, TILE)
    skip = far_tiles * TILE
    proj_ref[...] = three_parts(mm(vm_ref[...].astype(BF16), wmsg_ref[2 * latent:, :]))

    def index(t, carry):
        feat_t = mm_nt(vtb, select(rank, (t * PREP).astype(F32)))
        here = pl.ds(pl.multiple_of(t * PREP, PREP), PREP)
        slot = lax.broadcasted_iota(jnp.int32, (1, PREP), 1) + t * PREP
        used = (slot < n_far) | ((slot >= skip) & (slot < end))
        win_r = feat_t[4:5] - (lat * cell_rows - REACH).astype(F32)
        win_c = feat_t[5:6] - (lon * cols).astype(F32)
        pos = jnp.clip(jnp.where(used, (win_r * cols + win_c).astype(jnp.int32), REACH * cols), 0, positions - 1)
        node = feat_t[7:8].astype(jnp.int32)
        cell = lax.div(node, nodes)
        rel = jnp.where(used, jnp.bitwise_xor(cell, lon) * nodes + (node - cell * nodes), band)
        idx_v[0:1, here] = pos * CODE + rel
        return carry

    lax.fori_loop(0, lax.div(end + PREP - 1, PREP), index, 0)
    lane = lax.broadcasted_iota(jnp.int32, (1, 128), 1)
    idx_v[0:1, meta:meta + 128] = jnp.where(lane == 0, far_tiles, lax.div(end + TILE - 1, TILE))
    move = pltpu.make_async_copy(idx_v, idx_s, isem)
    move.start()
    part[...] = jnp.zeros_like(part)
    half[...] = wmsg_ref[latent:2 * latent, :] * jnp.asarray(0.5, BF16)
    prepare(0, lax.div(skip + PREP - 1, PREP), rank, vtb, we_ref, wmsg_ref, wo_ref, bg_ref, proj_ref, lp, ec)
    move.wait()
    message_loop(0, far_tiles, tab_ref, half, wo_ref.at[3], bg_ref[3], lp, ec, idx_s, part, (buf_a, buf_b), (hid_a, hid_b, hid_c, hid_d))
    for k, ref in enumerate((p1_ref, p2_ref, p3_ref)):
        ref[...] = part[(k + 1) * nodes:(k + 2) * nodes]


def near_kernel(idx, v_ref, rank_ref, proj_ref, we_ref, wmsg_ref, wo_ref, bg_ref, tab_ref, own_ref, lp, ec, part, half, hid_a, hid_b, hid_c, hid_d, buf_a, buf_b):
    latent = wo_ref.shape[-1]
    nodes = own_ref.shape[0]
    part[...] = jnp.zeros_like(part)
    half[...] = wmsg_ref[latent:2 * latent, :] * jnp.asarray(0.5, BF16)
    vtb = jnp.concatenate([v_ref[k] for k in range(v_ref.shape[0])], axis=1)
    meta = idx.shape[1] - 128
    start, stop = idx[0, meta], idx[0, meta + 1]
    ratio = PREP // TILE
    prepare(lax.div(start, ratio), lax.div(stop + ratio - 1, ratio), rank_ref[0:rank_ref.shape[0] - 16], vtb, we_ref, wmsg_ref, wo_ref, bg_ref,
            proj_ref, lp, ec)
    message_loop(start, stop, tab_ref, half, wo_ref.at[3], bg_ref[3], lp, ec, idx, part,
                 (buf_a, buf_b), (hid_a, hid_b, hid_c, hid_d))
    own_ref[...] = part[0:nodes]


def loop_scratch(batch, latent):
    half_tile = pltpu.VMEM((TILE // 2 * batch, latent), BF16)
    return [pltpu.VMEM((latent, latent), BF16)] + [half_tile] * 6


def edge_call(v, rank, vm, w_edge, w_msg, w_out, bias_gain, table, lons, nodes, per_node):
    latent = w_out.shape[-1]
    batch = table.shape[2]
    limit = lons * nodes * per_node + PREP + 128
    local = pl.BlockSpec(memory_space=pltpu.VMEM)
    outs = [jax.ShapeDtypeStruct((nodes, batch, latent), F32)] * (lons - 1)
    outs += [jax.ShapeDtypeStruct((1, limit), jnp.int32), jax.ShapeDtypeStruct((3 * lons * nodes, latent), BF16)]
    res = pl.pallas_call(
        functools.partial(far_kernel, lons=lons, nodes=nodes),
        in_specs=[local] * 8,
        out_specs=[local] * len(outs),
        out_shape=outs,
        scratch_shapes=[
            pltpu.VMEM((latent // 128, limit, 128), F32), pltpu.VMEM((latent // 128, limit, 128), F32),
            pltpu.SMEM((1, limit), jnp.int32),
            pltpu.VMEM((lons * nodes + 1, batch, latent), F32)] + loop_scratch(batch, latent) + [pltpu.SemaphoreType.DMA],
        compiler_params=pltpu.CompilerParams(vmem_limit_bytes=EDGE_VMEM),
        cost_estimate=pl.CostEstimate(
            flops=4 * limit // 8 * batch * latent * latent, transcendentals=0, bytes_accessed=limit * batch * latent),
        name='edges_far',
    )(v, rank, vm, w_edge, w_msg, w_out, bias_gain, table)
    return res[:lons - 1], res[lons - 1:]


def near_call(v, rank, lists, w_edge, w_msg, w_out, bias_gain, table, nodes, band):
    idx, proj = lists
    latent = w_out.shape[-1]
    batch = table.shape[2]
    local = pl.BlockSpec(memory_space=pltpu.VMEM)
    return pl.pallas_call(
        near_kernel,
        in_specs=[pl.BlockSpec(memory_space=pltpu.SMEM)] + [local] * 8,
        out_specs=[local],
        out_shape=[jax.ShapeDtypeStruct((nodes, batch, latent), F32)],
        scratch_shapes=[pltpu.VMEM((latent // 128, idx.shape[1], 128), F32), pltpu.VMEM((latent // 128, idx.shape[1], 128), F32),
                        pltpu.VMEM((band + 1, batch, latent), F32)] + loop_scratch(batch, latent),
        compiler_params=pltpu.CompilerParams(vmem_limit_bytes=EDGE_VMEM),
        cost_estimate=pl.CostEstimate(
            flops=idx.shape[1] * batch * latent * latent, transcendentals=0, bytes_accessed=idx.shape[1] * batch * latent),
        name='edges_near',
    )(idx, v, rank, proj, w_edge, w_msg, w_out, bias_gain, table)


def node_kernel(own_ref, r1_ref, r2_ref, r3_ref, vm_ref, wn_ref, w4_ref, bg_ref, out_ref, scr):
    nodes, batch, latent = own_ref.shape
    agg = (own_ref[...] + r1_ref[...] + r2_ref[...] + r3_ref[...]).astype(BF16).reshape(nodes * batch, latent)
    bg = bg_ref[4]
    own_vm = vm_ref[...]
    base = mm(own_vm.astype(BF16), wn_ref[0:latent, :]) + bg[0:1]
    acc = mm(agg, wn_ref[latent:, :]).reshape(nodes, batch, latent) + base.reshape(nodes, 1, latent)
    upd = mlp_tail(acc.reshape(nodes * batch, latent), w4_ref[4], bg)
    out = (upd.reshape(nodes, batch, latent) + own_vm.reshape(nodes, 1, latent)).reshape(nodes * batch, latent)

    def put(b, k, part):
        out_ref[b, :, 128 * k:128 * (k + 1)] = part

    swap_rows(out, scr, batch, put)


def node_call(blocks, vm, w_node, w_out, bias_gain):
    nodes, batch, latent = blocks[0].shape
    local = pl.BlockSpec(memory_space=pltpu.VMEM)
    out = jax.ShapeDtypeStruct((batch, nodes, latent), BF16)
    return pl.pallas_call(
        node_kernel,
        in_specs=[local] * 8,
        out_specs=local,
        out_shape=out,
        compiler_params=pltpu.CompilerParams(vmem_limit_bytes=NODE_VMEM),
        scratch_shapes=[pltpu.VMEM((latent // 128, nodes * (batch + 8), 128), F32)],
        name='nodes',
    )(*blocks, vm, w_node, w_out, bias_gain)


def solution(mesh):
    lats = mesh.shape['lat']
    lons = mesh.shape['lon']
    south_shift = [(s, s + 1) for s in range(lats - 1)]
    north_shift = [(s + 1, s) for s in range(lats - 1)]

    def cell_step(grid_in, mesh_in, edge_in, senders, edge_mask, w_grid, w_mesh, w_edge, w_msg, w_node, w_gupd, w_out, bias_gain):
        batch, rows, cols, _ = grid_in.shape
        nodes = senders.shape[0]
        latent = w_out.shape[-1]
        feats, own_vm = pack_call(
            senders, edge_mask, jnp.swapaxes(edge_in, 1, 2), mesh_in.T, idle_call(), w_mesh, w_out, bias_gain, cols * lons)
        vg, table, band, rank, vm = embed_call(grid_in, w_grid, w_out, bias_gain, feats, own_vm, lats, lons)
        blocks, lists = edge_call(band, rank, vm, w_edge, w_msg, w_out, bias_gain, table, lons, *senders.shape)
        own, = near_call(band, rank, lists, w_edge, w_msg, w_out, bias_gain, table, nodes, nodes * lons)
        pairs = lambda k, polar: [
            (j * lats + i, (j ^ k) * lats + i) for i in range(lats) for j in range(lons)
            if not polar or i in (0, lats - 1)]
        last_block, own = lax.optimization_barrier((blocks[0], own))
        sends = ((3, blocks[2]), (2, blocks[1]), (1, last_block))
        got = [lax.ppermute(block, ('lon', 'lat'), pairs(k, k == 2)) for k, block in sends]
        mesh_out = node_call([own] + got, own_vm, w_node, w_out, bias_gain)
        flat = update_call(vg.reshape(batch * rows * cols, latent), w_gupd, w_out, bias_gain, own)
        grid_out = flat.reshape(batch, rows, cols, latent)
        return mesh_out, grid_out

    grid_spec = P('dp', 'lat', 'lon', None)
    node_spec = P(('lat', 'lon'), None)
    slot_spec = P(('lat', 'lon'), None, None)
    in_specs = (grid_spec, node_spec, slot_spec, node_spec, node_spec) + (P(),) * 8
    out_specs = (P('dp', ('lat', 'lon'), None), grid_spec)
    return jax.shard_map(cell_step, mesh=mesh, in_specs=in_specs, out_specs=out_specs, check_vma=False)
```
